32 devices in a mesh: scan: 8 (over z, y), grp: 4 (over x, core).
Axes of the slice: x: 2, y: 2, z: 4, core: 2. Of those that a mesh axis runs over, the one named last changes fastest.
Arguments:
- samples: float32 [128, 64, 6, 128], P('scan', 'grp'), may hold values from -6 to 6
- point_count: int32 [128], P('scan'), may hold values from 4096 to 8192
- corr_scan: int32 [128, 64], P('scan', 'grp'), may hold values from 0 to 127, as said below
- corr_tile: int32 [128, 64], P('scan', 'grp'), may hold values from 0 to 63
- corr_src: int32 [128, 64, 128], P('scan', 'grp'), may hold values from 0 to 2047
Outputs:
- hessian: float32 [128, 6, 6, 128], P('scan', None, None, 'grp')
- gradient: float32 [128, 6], P(('scan', 'grp'))
The draws below stay inside these ranges and needn't reach their ends.
Inputs may be any that keep to these rules, and one draw needn't show every extreme that they name: Never the scan of the entry's own row. A named tile is held by the device with scan index corr_scan // 16 and grp index corr_tile // 16; the 256 entries of one device name at most 16 tiles held by any one device, and in every draw some device is named exactly 16 times by every device.
All inputs are finite; a program needn't handle non-finite values.
Results may differ from the reference program's by a relative error of at most 0.00021.
Values sent between devices are 32-bit elements; how exact they have to be, the bound alone decides.
A program may use at most 64 MiB of HBM per device.

```python
import jax
import jax.numpy as jnp
from jax import lax

SCAN_LOC = 16
TILES_G = 16
CT = 16
SCANS = 128
TILES = 64
N_SCAN = 8
N_GRP = 4
DEVICES = 32


def pair_plan(key):
    half_count = DEVICES // 2
    slot_cap = 2 * SCAN_LOC * CT // DEVICES
    request_count = SCAN_LOC * CT
    hub_device = jax.random.randint(jax.random.fold_in(key, 1), (), 0, DEVICES)

    def one_device(device):
        dev_key = jax.random.fold_in(key, device + 100)

        def one_round(round_idx):
            round_key = jax.random.fold_in(dev_key, round_idx)
            shuffled = jax.random.permutation(round_key, DEVICES - 1) + 1
            offsets = jnp.concatenate([jnp.zeros((1,), jnp.int32), shuffled[:half_count - 1].astype(jnp.int32)])
            return (hub_device + offsets) % DEVICES
        destination = jax.vmap(one_round)(jnp.arange(slot_cap)).reshape(request_count)
        own_index = device // N_GRP
        dest_index = destination // N_GRP
        dest_group = destination % N_GRP
        local_scan = jnp.arange(request_count) // CT
        chosen = jax.random.randint(jax.random.fold_in(dev_key, 5000), (request_count,), 0, SCAN_LOC)
        clashes = (dest_index == own_index) & (chosen == local_scan)
        chosen = jnp.where(clashes, (chosen + 1) % SCAN_LOC, chosen)
        target_scan = dest_index * SCAN_LOC + chosen
        tile_ids = dest_group * TILES_G + jax.random.randint(jax.random.fold_in(dev_key, 6000), (request_count,), 0, TILES_G)
        return (target_scan.astype(jnp.int32), tile_ids.astype(jnp.int32))
    targets, tile_ids = jax.vmap(one_device)(jnp.arange(DEVICES))
    grid_shape = (N_SCAN, N_GRP, SCAN_LOC, CT)
    targets = targets.reshape(grid_shape).transpose(0, 2, 1, 3).reshape(N_SCAN * SCAN_LOC, N_GRP * CT)
    tile_ids = tile_ids.reshape(grid_shape).transpose(0, 2, 1, 3).reshape(N_SCAN * SCAN_LOC, N_GRP * CT)
    return (targets, tile_ids)


def draw_corr_scan(key, part):
    return pair_plan(key)[0]


def draw_corr_tile(key, part):
    return pair_plan(key)[1]


def set_ends(result, stream_key, smallest, top_value):
    longest = result.shape.index(max(result.shape))
    spots = []
    for shift in (0, 1):
        where = [jax.random.randint(jax.random.fold_in(stream_key, axis), (), 0, length) for axis, length in enumerate(result.shape)]
        where[longest] = (where[longest] + shift) % result.shape[longest]
        spots.append(tuple(where))
    return result.at[spots[0]].set(smallest).at[spots[1]].set(top_value)


def steps_of(own_key, extent, pieces, low, high):
    level, own = 1.0, jax.random.fold_in(own_key, 6)
    for dim, blocks in pieces:
        draws = jnp.exp(jax.random.uniform(jax.random.fold_in(own, dim), (blocks,), jnp.float32, low / len(pieces), high / len(pieces)))
        level = level * jnp.repeat(draws, extent[dim] // blocks).reshape([-1 if axis == dim else 1 for axis in range(len(extent))])
    return level


def scatter_about(key, shape, scale, limit, split=(), held_as=jnp.bfloat16):
    array = scale * jax.random.normal(key, shape, jnp.float32)
    if split:
        array = array * steps_of(key, shape, split, -0.22, 0.18)
    return jnp.clip(array, -limit, limit).astype(held_as)


def setup_inputs(seed: int = 0) -> dict:
    seeds = jax.random.split(jax.random.key(seed), 6)
    samples = scatter_about(seeds[0], (SCANS, TILES, 6, 128), 1.0, 6.0, ((0, 8), (1, 4)), jnp.float32)
    point_count = set_ends(jax.random.randint(seeds[1], (SCANS,), TILES_G * N_GRP * 64, TILES_G * N_GRP * 128 + 1), jax.random.fold_in(seeds[1], 1), TILES_G * N_GRP * 64, TILES_G * N_GRP * 128).astype(jnp.int32)
    corr_scan = draw_corr_scan(jax.random.fold_in(seeds[5], 71), 0)
    corr_tile = draw_corr_tile(jax.random.fold_in(seeds[5], 71), 0)
    corr_src = set_ends(jax.random.randint(seeds[4], (SCANS, N_GRP * CT, 128), 0, TILES_G * 128), jax.random.fold_in(seeds[4], 1), 0, (TILES_G * 128) - 1).astype(jnp.int32)
    return {"samples": samples, "point_count": point_count, "corr_scan": corr_scan, "corr_tile": corr_tile, "corr_src": corr_src}


def pair_blocks(pos_x, pos_y, pos_z, source_mask, tile_data):
    diff_x = pos_x - tile_data[:, 0, :]
    diff_y = pos_y - tile_data[:, 1, :]
    diff_z = pos_z - tile_data[:, 2, :]
    normal_x = tile_data[:, 3, :]
    normal_y = tile_data[:, 4, :]
    normal_z = tile_data[:, 5, :]
    residual = normal_x * diff_x + normal_y * diff_y + normal_z * diff_z
    weight = source_mask / (1.0 + residual * residual)
    jacobian = jnp.stack([pos_y * normal_z - pos_z * normal_y, pos_z * normal_x - pos_x * normal_z, pos_x * normal_y - pos_y * normal_x, normal_x, normal_y, normal_z], axis=1)
    blocks = jnp.einsum("nik,njk->nij", jacobian * weight[:, None, :], jacobian, precision=lax.Precision.HIGHEST)
    vectors = jnp.einsum("nik,nk->ni", jacobian, weight * residual, precision=lax.Precision.HIGHEST)
    return blocks.reshape(-1, 36), vectors


def reference(samples, point_count, corr_scan, corr_tile, corr_src):
    scan_count = samples.shape[0]
    tile_count = samples.shape[1]
    column_count = corr_scan.shape[1]
    per_group = column_count // N_GRP
    group_points = (tile_count // N_GRP) * 128
    groups = (jnp.arange(column_count) // per_group).astype(jnp.int32)
    point_ids = groups[None, :, None] * group_points + corr_src
    flat_samples = samples.reshape(scan_count, tile_count * 768)
    offsets = ((point_ids // 128) * 768 + point_ids % 128).reshape(scan_count, column_count * 128)
    coords = [jnp.take_along_axis(flat_samples, offsets + axis_id * 128, axis=1).reshape(-1, 128) for axis_id in range(3)]
    source_mask = (point_ids < point_count[:, None, None]).astype(jnp.float32).reshape(-1, 128)
    target_scan = corr_scan.reshape(-1)
    target_tile = corr_tile.reshape(-1)
    tile_data = samples[target_scan, target_tile]
    row_ids = jnp.arange(128).astype(jnp.int32)
    target_mask = ((target_tile[:, None] * 128 + row_ids[None, :]) < point_count[target_scan][:, None]).astype(jnp.float32)
    tile_data = jnp.concatenate([tile_data[:, 0:3, :], tile_data[:, 3:6, :] * target_mask[:, None, :]], axis=1)
    blocks, vectors = pair_blocks(coords[0], coords[1], coords[2], source_mask, tile_data)
    source_scan = (jnp.arange(scan_count * column_count) // column_count).astype(jnp.int32)
    pairwise = jnp.zeros((scan_count, scan_count, 36), jnp.float32)
    pairwise = pairwise.at[source_scan, source_scan].add(blocks)
    pairwise = pairwise.at[target_scan, target_scan].add(blocks)
    pairwise = pairwise.at[source_scan, target_scan].add(-blocks)
    pairwise = pairwise.at[target_scan, source_scan].add(-blocks)
    hessian = pairwise.reshape(scan_count, scan_count, 6, 6).transpose(0, 2, 3, 1)
    gradient = jnp.zeros((scan_count, 6), jnp.float32)
    gradient = gradient.at[source_scan].add(vectors).at[target_scan].add(-vectors)
    return hessian, gradient
```

```python
import functools

import jax
import jax.numpy as jnp
from jax import lax
from jax.experimental import pallas as pl
from jax.experimental.pallas import tpu as pltpu
from jax.sharding import PartitionSpec as P

LANES = 128
VALUES = 32
LEAST_POINTS = 4096
PAIRS = [(i, j) for i in range(6) for j in range(i, 6)]
VMEM = pl.BlockSpec(memory_space=pltpu.VMEM)
SMEM = pl.BlockSpec(memory_space=pltpu.SMEM)


def halves(value, size):
    if size & (size - 1):
        return value // size, value % size
    return value >> (size.bit_length() - 1), value & (size - 1)


def lane_take(table, index):
    return jnp.take_along_axis(table, index, axis=1, mode="promise_in_bounds")


def pack_kernel(cap, n_grp, samples, count, corr_scan, corr_tile, corr_src, data, meta, used):
    scan_local, tiles_local = samples.shape[0], samples.shape[2]
    per_scan = corr_src.shape[1]
    devices = meta.shape[0]
    scan_index, group_index = lax.axis_index("scan"), lax.axis_index("grp")
    first_point = group_index * tiles_local * LANES

    def clear(d, _):
        used[d] = 0
        for j in range(cap):
            meta[d, 0, j] = -1
            meta[d, 0, cap + j] = 0
            meta[d, 0, 2 * cap + j] = -1
        data[pl.ds(pl.multiple_of(d * cap * 4, 8), cap * 4), :] = jnp.zeros((cap * 4, LANES), jnp.float32)
        return 0

    lax.fori_loop(0, devices, clear, 0)

    def one_scan(s, _):
        wanted = corr_src[s]
        tile, lane = wanted >> 7, wanted & (LANES - 1)
        picked = [jnp.zeros((per_scan, LANES), jnp.float32)] * 3
        for t in range(tiles_local):
            hit = tile == t
            for c in range(3):
                row = jnp.broadcast_to(samples[s, c, pl.ds(t, 1), :], (per_scan, LANES))
                picked[c] = jnp.where(hit, lane_take(row, lane), picked[c])
        mask = jnp.where(first_point + wanted < count[s], 1.0, 0.0).astype(jnp.float32)
        picked.append(mask)
        for k in range(per_scan):
            b, t = corr_scan[s, k], corr_tile[s, k]
            (b_dev, b_loc), (t_dev, t_loc) = halves(b, scan_local), halves(t, tiles_local)
            d = b_dev * n_grp + t_dev
            j = used[d]
            used[d] = j + 1
            meta[d, 0, j] = b_loc
            meta[d, 0, cap + j] = b_loc * tiles_local + t_loc
            meta[d, 0, 2 * cap + j] = scan_index * scan_local + s
            base = d * cap * 4 + j
            for c in range(4):
                data[pl.ds(base + c * cap, 1), :] = picked[c][k : k + 1, :]
        return 0

    lax.fori_loop(0, scan_local, one_scan, 0)


def meet_all(n_grp, devices, me):
    barrier = pltpu.get_barrier_semaphore()

    def hello(k, _):
        peer = lax.rem(me + k, devices)
        pl.semaphore_signal(
            barrier, inc=1, device_id=(peer // n_grp, peer % n_grp), device_id_type=pl.DeviceIdType.MESH
        )
        return 0

    lax.fori_loop(1, devices, hello, 0)
    pl.semaphore_wait(barrier, devices - 1)


def remote(src, dst, send, recv, peer, n_grp):
    return pltpu.make_async_remote_copy(
        src_ref=src, dst_ref=dst, send_sem=send, recv_sem=recv,
        device_id=(peer // n_grp, peer % n_grp), device_id_type=pl.DeviceIdType.MESH,
    )


def exclusive(a, b, size):
    if size & (size - 1):
        return lax.rem(a + b, size)
    total = 0
    for bit in range(size.bit_length() - 1):
        total = total + ((((a >> bit) + (b >> bit)) & 1) << bit)
    return total


def split(values):
    high = values.astype(jnp.bfloat16)
    return high, (values - high.astype(jnp.float32)).astype(jnp.bfloat16)


def contract(a, b):
    return lax.dot_general(a, b, (((1,), (1,)), ((), ())), preferred_element_type=jnp.float32)


def row_sum(products):
    return jnp.sum(products, axis=0, keepdims=True)


def exchange_kernel(
    cap, n_grp, samples, count, data, meta, by_source, by_partner, shares,
    data_in, meta_in, codes, tiles, comps, turned, ids, result, packed,
    send_data, recv_data, send_meta, recv_meta, send_src, recv_src, send_part, recv_part,
    send_share, recv_share, own,
):
    scan_local, tiles_local = samples.shape[0], samples.shape[2]
    n_scan = send_src.shape[0]
    devices = n_scan * n_grp
    rows = cap * 4
    width = n_grp * cap
    per_block = LANES // width
    blocks = n_scan // per_block
    sources = per_block * n_grp
    packed_rows = packed.shape[1]
    scan_index, group_index = lax.axis_index("scan"), lax.axis_index("grp")
    me = scan_index * n_grp + group_index
    home, home_row = scan_index // per_block, lax.rem(scan_index, per_block)
    full_groups = min(LEAST_POINTS // (tiles_local * LANES), n_grp) if 3 * cap % 8 == 0 else 0
    short = rows - cap

    def send_one(src, dst_index, send_index, recv_index, peer, size):
        return remote(
            data.at[pl.ds(pl.multiple_of(src * rows, 8), size)],
            data_in.at[pl.ds(pl.multiple_of(dst_index * rows, 8), size)],
            send_data.at[send_index], recv_data.at[recv_index], peer, n_grp,
        )

    def send_code(src, dst_index, send_index, recv_index, peer):
        return remote(
            meta.at[src], meta_in.at[dst_index], send_meta.at[send_index], recv_meta.at[recv_index], peer, n_grp
        )

    def to_source(row, holder, index):
        peer = row * n_grp + home
        return remote(packed.at[row], by_source.at[holder], send_src.at[row], recv_src.at[index], peer, n_grp)

    def to_partner(block, at):
        peer = scan_index * n_grp + block
        return remote(result.at[block], by_partner.at[at], send_part.at[block], recv_part.at[at], peer, n_grp)

    def to_share(g, at):
        peer = scan_index * n_grp + g
        return remote(shares.at[group_index], shares.at[at], send_share.at[g], recv_share.at[at], peer, n_grp)

    meet_all(n_grp, devices, me)

    def start_meta(k, _):
        peer = lax.rem(me + k, devices)
        send_code(peer, me, peer, me, peer).start()
        return 0

    def wait_meta(k, _):
        peer = lax.rem(me + k, devices)
        copy = send_code(peer, peer, peer, peer, peer)
        copy.wait_send()
        copy.wait_recv()
        return 0

    def start_data(k, _):
        row = exclusive(scan_index, n_scan - 1 - k, n_scan)
        for g in range(n_grp):
            peer = row * n_grp + g

            @pl.when((peer != me) & (group_index < full_groups))
            def _():
                send_one(peer, me, peer, me, peer, short).start()

            @pl.when((peer != me) & (group_index >= full_groups))
            def _():
                send_one(peer, me, peer, me, peer, rows).start()

        return 0

    lax.fori_loop(1, devices, start_meta, 0)
    lax.fori_loop(0, n_scan, start_data, 0)
    own_data = pltpu.make_async_copy(
        data.at[pl.ds(pl.multiple_of(me * rows, 8), rows)], data_in.at[pl.ds(pl.multiple_of(me * rows, 8), rows)], own.at[0]
    )
    own_meta = pltpu.make_async_copy(meta.at[me], meta_in.at[me], own.at[1])
    own_data.start()
    own_meta.start()
    own_data.wait()
    own_meta.wait()

    def no_mask(row, _):
        for g in range(full_groups):
            first = pl.multiple_of((row * n_grp + g) * rows + short, 8)
            data_in[pl.ds(first, cap), :] = jnp.ones((cap, LANES), jnp.float32)
        return 0

    lax.fori_loop(0, n_scan, no_mask, 0)
    shares[...] = jnp.zeros_like(shares)
    result[...] = jnp.zeros_like(result)

    point = lax.broadcasted_iota(jnp.int32, (tiles_local, LANES), 0) * LANES
    point = point + lax.broadcasted_iota(jnp.int32, (tiles_local, LANES), 1)

    tile_rows = tiles.reshape(scan_local * tiles_local * 8, LANES)

    def fill(b, _):
        valid = point < count[b] - group_index * tiles_local * LANES
        for c in range(6):
            values = samples[b, c]
            if c >= 3:
                values = jnp.where(valid, values, 0.0)
            tile_rows[pl.ds(b * tiles_local * 8 + c, tiles_local, stride=8), :] = values
        return 0

    lax.fori_loop(0, scan_local, fill, 0)
    lax.fori_loop(1, devices, wait_meta, 0)
    to_scalar = pltpu.make_async_copy(meta_in, codes, own.at[2])
    to_scalar.start()

    slot_lane = lax.broadcasted_iota(jnp.int32, (sources, LANES), 1) // cap
    slot_row = lax.broadcasted_iota(jnp.int32, (sources, LANES), 0)

    def decode(m, _):
        arrived = meta_in[pl.ds(m * sources, sources), 0, :]
        kinds = []
        for kind in (0, 2):
            moved = pltpu.roll(arrived, LANES - kind * cap, 1) if kind else arrived
            moved = pltpu.roll(moved, 0, 1, stride=cap, stride_axis=0)
            kinds.append(row_sum(jnp.where(slot_lane == slot_row, moved, 0)))
        partner, source = kinds
        ids[m, 0:1, :] = source.astype(jnp.float32)
        ids[m, 1:2, :] = jnp.where(partner < 0, -1, scan_index * scan_local + partner).astype(jnp.float32)
        return 0

    lax.fori_loop(0, blocks, decode, 0)
    to_scalar.wait()

    def one_block(k, _):
        m = exclusive(home, blocks - 1 - k, blocks)

        def gather(i, _):
            for j in range(cap):
                slot = i * cap + j
                row = codes[m * sources + i, 0, cap + j]
                comps[pl.ds(pl.multiple_of(slot * 8, 8), 8), :] = tiles[row]
            return 0

        lax.fori_loop(0, sources, gather, 0)
        for c in range(6):
            turned[4 + c] = comps[pl.ds(c, LANES, stride=8), :].T

        def arrive(i, _):
            source = m * sources + i
            group = lax.rem(i, n_grp)

            @pl.when((source != me) & (group < full_groups))
            def _():
                send_one(source, source, source, source, source, short).wait_recv()

            @pl.when((source != me) & (group >= full_groups))
            def _():
                send_one(source, source, source, source, source, rows).wait_recv()

            return 0

        lax.fori_loop(0, sources, arrive, 0)
        for c in range(4):
            pieces = [
                data_in[pl.ds((m * sources + i) * rows + c * cap, cap), :] for i in range(sources)
            ]
            turned[c] = jnp.concatenate(pieces, axis=0).T

        def step(kk, sums):
            at = pl.ds(pl.multiple_of(kk * 8, 8), 8)
            px, py, pz, mask, qx, qy, qz, nx, ny, nz = [turned[c, at, :] for c in range(10)]
            residual = nx * (px - qx) + ny * (py - qy) + nz * (pz - qz)
            weight = mask / (1.0 + residual * residual)
            jac = [py * nz - pz * ny, pz * nx - px * nz, px * ny - py * nx, nx, ny, nz]
            scaled = [weight * x for x in jac]
            products = [scaled[a] * jac[b] for a, b in PAIRS] + [x * residual for x in scaled]
            return tuple(s + p for s, p in zip(sums, products))

        zero = jnp.zeros((8, LANES), jnp.float32)
        sums = lax.fori_loop(0, LANES // 8, step, (zero,) * (len(PAIRS) + 6))
        for q, total in enumerate(sums):
            result[m, q : q + 1, :] = row_sum(total)
        result[m, 27:29, :] = ids[m, 0:2, :]
        values = result[m]
        lane = lax.broadcasted_iota(jnp.int32, (packed_rows, LANES), 1) // width
        chunks = [values[g * packed_rows : (g + 1) * packed_rows, :] for g in range(per_block)]
        for p in range(per_block):
            total = chunks[p]
            for g in range(per_block):
                if g != p:
                    total = jnp.where(lane == g, pltpu.roll(chunks[g], (g - p) * width % LANES, 1), total)
            row = m * per_block + p
            packed[row] = total
            holder = group_index * per_block + home_row

            @pl.when(row * n_grp + home == me)
            def _():
                by_source[holder] = total

            @pl.when(row * n_grp + home != me)
            def _():
                to_source(row, holder, holder).start()

        @pl.when(m == group_index)
        def _():
            by_partner[group_index] = values

        @pl.when(m != group_index)
        def _():
            to_partner(m, group_index).start()

        return 0

    lax.fori_loop(0, blocks, one_block, 0)

    for holder in range(sources):
        group, other = holder // per_block, holder % per_block
        peer = (group_index * per_block + other) * n_grp + group

        @pl.when(peer != me)
        def _():
            to_source(0, holder, holder).wait_recv()

    for g in range(n_grp):

        @pl.when(g != group_index)
        def _():
            to_partner(0, g).wait_recv()

    span = lax.broadcasted_iota(jnp.int32, (2 * scan_local, LANES), 0)
    values, chosen = [], []
    for g in range(n_grp):
        parts = [by_source[g * per_block + p] for p in range(per_block)]
        block = jnp.concatenate(regroup(parts, width), axis=0)
        values.append(block)
        at = block[27:28, :].astype(jnp.int32) - scan_index * scan_local
        chosen.append(jnp.where(span == at, 1.0, 0.0))
    for g in range(n_grp):
        block = by_partner[g]
        values.append(block)
        at = block[28:29, :].astype(jnp.int32) - scan_index * scan_local
        chosen.append(jnp.where((at >= 0) & (span - scan_local == at), 1.0, 0.0))
    high, low = split(jnp.concatenate(values, axis=1))
    matrix = jnp.concatenate(chosen, axis=1).astype(jnp.bfloat16)
    shares[group_index, :, 0 : 2 * scan_local] = contract(high, matrix) + contract(low, matrix)
    for g in range(n_grp):

        @pl.when(g != group_index)
        def _():
            to_share(g, group_index).start()

    def finish(k, _):
        peer = lax.rem(me + k, devices)

        @pl.when(group_index < full_groups)
        def _():
            send_one(peer, peer, peer, peer, peer, short).wait_send()

        @pl.when(group_index >= full_groups)
        def _():
            send_one(peer, peer, peer, peer, peer, rows).wait_send()

        return 0

    lax.fori_loop(1, devices, finish, 0)

    def finish_source(row, _):
        @pl.when(row * n_grp + home != me)
        def _():
            to_source(row, 0, 0).wait_send()

        return 0

    lax.fori_loop(0, n_scan, finish_source, 0)
    for g in range(n_grp):

        @pl.when(g != group_index)
        def _():
            to_partner(g, 0).wait_send()
            copy = to_share(g, g)
            copy.wait_send()
            copy.wait_recv()


def regroup(parts, width):
    groups = len(parts)
    lane = lax.broadcasted_iota(jnp.int32, parts[0].shape, 1) // width
    out = []
    for b in range(groups):
        total = parts[b]
        for g in range(groups):
            if g != b:
                total = jnp.where(lane == g, pltpu.roll(parts[g], (g - b) * width % LANES, 1), total)
        out.append(total)
    return out


def assemble_kernel(n_grp, width, by_source, by_partner, shares, hessian, gradient, spare):
    rows, columns = hessian.shape[2], hessian.shape[3]
    grad_rows = gradient.shape[0]
    per_block = LANES // width
    scan_index, group_index = lax.axis_index("scan"), lax.axis_index("grp")
    home, home_row = scan_index // per_block, lax.rem(scan_index, per_block)
    first_row, first_column = scan_index * rows, group_index * columns
    count = len(PAIRS)

    share = shares[0]
    for g in range(1, n_grp):
        share = share + shares[g]
    other = pltpu.roll(share, LANES - rows, 1)
    spare[...] = (share - other).T
    gradient[...] = spare[pl.ds(group_index * grad_rows, grad_rows), 21:27]

    pieces = []
    for g in range(n_grp):
        parts = [by_source[g * per_block + p] for p in range(per_block)]
        block = jnp.concatenate(regroup(parts, width), axis=0)
        source, partner = block[27:28, :].astype(jnp.int32), block[28:29, :].astype(jnp.int32)
        pieces.append((block, source - first_row, partner - first_column))
    for g in range(n_grp):
        block = by_partner[g]
        source, partner = block[27:28, :].astype(jnp.int32), block[28:29, :].astype(jnp.int32)
        pieces.append((block, partner - first_row, source - first_column))
    lane = lax.broadcasted_iota(jnp.int32, (1, LANES), 1)
    diagonal = jnp.where((lane < rows) & (group_index == home), lane, -1)
    pieces.append((share + other, diagonal, jnp.where(diagonal < 0, -1, lane + home_row * rows)))

    left, right = [], []
    row = lax.broadcasted_iota(jnp.int32, (rows, LANES), 0)
    column = lax.broadcasted_iota(jnp.int32, (columns, LANES), 0)
    for index, (block, at, to) in enumerate(pieces):
        hit = row == at
        left.append(jnp.concatenate([jnp.where(hit, block[q : q + 1, :], 0.0) for q in range(count)], axis=0))
        right.append(jnp.where(column == to, 1.0 if index == 2 * n_grp else -1.0, 0.0))
    matrix = jnp.concatenate(right, axis=1).astype(jnp.bfloat16)
    high, low = split(jnp.concatenate(left, axis=1))
    total = contract(high, matrix) + contract(low, matrix)
    where = {pair: q for q, pair in enumerate(PAIRS)}
    for i in range(6):
        for j in range(6):
            q = where[min(i, j), max(i, j)]
            hessian[i, j] = total[q * rows : (q + 1) * rows, :]


def local(samples, point_count, corr_scan, corr_tile, corr_src):
    f32, i32 = jnp.float32, jnp.int32
    scan_local, tiles_local = samples.shape[0], samples.shape[1]
    request_count = scan_local * corr_scan.shape[1]
    n_scan, n_grp = lax.axis_size("scan"), lax.axis_size("grp")
    devices = n_scan * n_grp
    cap = 2 * request_count // devices
    width = n_grp * cap
    packed_rows = VALUES * width // LANES
    per_block = LANES // width
    blocks = n_scan // per_block
    columns = scan_local * n_scan // n_grp
    grad_rows = scan_local // n_grp
    assert blocks == n_grp and blocks * per_block == n_scan and 2 * scan_local <= LANES
    shape = jax.ShapeDtypeStruct
    dma = pltpu.SemaphoreType.DMA

    tiles = samples.transpose(0, 2, 1, 3)
    data, meta = pl.pallas_call(
        functools.partial(pack_kernel, cap, n_grp),
        out_shape=(shape((devices * cap * 4, LANES), f32), shape((devices, 1, LANES), i32)),
        in_specs=[VMEM, SMEM, SMEM, SMEM, VMEM],
        out_specs=(VMEM, SMEM),
        scratch_shapes=[pltpu.SMEM((devices,), i32)],
    )(tiles, point_count, corr_scan, corr_tile, corr_src)

    by_source, by_partner, shares = pl.pallas_call(
        functools.partial(exchange_kernel, cap, n_grp),
        out_shape=(
            shape((n_grp * per_block, packed_rows, LANES), f32),
            shape((n_grp, VALUES, LANES), f32),
            shape((n_grp, VALUES, LANES), f32),
        ),
        in_specs=[VMEM, SMEM, VMEM, VMEM],
        out_specs=(VMEM, VMEM, VMEM),
        scratch_shapes=[
            pltpu.VMEM(data.shape, f32),
            pltpu.VMEM(meta.shape, i32),
            pltpu.SMEM(meta.shape, i32),
            pltpu.VMEM((scan_local * tiles_local, 8, LANES), f32),
            pltpu.VMEM((LANES * 8, LANES), f32),
            pltpu.VMEM((10, LANES, LANES), f32),
            pltpu.VMEM((blocks, 8, LANES), f32),
            pltpu.VMEM((blocks, VALUES, LANES), f32),
            pltpu.VMEM((n_scan, packed_rows, LANES), f32),
        ]
        + [dma((devices,))] * 4
        + [dma((n_scan,)), dma((n_grp * per_block,))]
        + [dma((n_grp,))] * 4
        + [dma((3,))],
        compiler_params=pltpu.CompilerParams(collective_id=0, has_side_effects=True),
    )(tiles, point_count, data, meta)

    hessian, gradient = pl.pallas_call(
        functools.partial(assemble_kernel, n_grp, width),
        out_shape=(shape((6, 6, scan_local, columns), f32), shape((grad_rows, 6), f32)),
        in_specs=[VMEM, VMEM, VMEM],
        out_specs=(VMEM, VMEM),
        scratch_shapes=[pltpu.VMEM((LANES, VALUES), f32)],
    )(by_source, by_partner, shares)
    return hessian.transpose(2, 0, 1, 3), gradient


def solution(mesh):
    placed = (
        P("scan", "grp", None, None),
        P("scan"),
        P("scan", "grp"),
        P("scan", "grp"),
        P("scan", "grp", None),
    )
    return jax.shard_map(
        local,
        mesh=mesh,
        in_specs=placed,
        out_specs=(P("scan", None, None, "grp"), P(("scan", "grp"), None)),
        check_vma=False,
    )
```

```python
import functools

import jax
import jax.numpy as jnp
from jax import lax
from jax.experimental import pallas as pl
from jax.experimental.pallas import tpu as pltpu
from jax.sharding import PartitionSpec as P

LANES = 128
VALUES = 32
LEAST_POINTS = 4096
PAIRS = [(i, j) for i in range(6) for j in range(i, 6)]
VMEM = pl.BlockSpec(memory_space=pltpu.VMEM)
SMEM = pl.BlockSpec(memory_space=pltpu.SMEM)
ANY = pl.BlockSpec(memory_space=pl.ANY)


def halves(value, size):
    if size & (size - 1):
        return value // size, value % size
    return value >> (size.bit_length() - 1), value & (size - 1)


def lane_take(table, index):
    return jnp.take_along_axis(table, index, axis=1, mode="promise_in_bounds")


def route_kernel(cap, n_grp, scan_local, tiles_local, corr_scan, corr_tile, slots, meta, wide):
    per_scan = corr_scan.shape[1]
    scan_index = lax.axis_index("scan")
    requests = scan_local * per_scan
    chunks, together = requests // LANES, LANES // per_scan
    f32 = jnp.float32

    def flat(ref):
        wide[...] = jnp.zeros_like(wide)
        wide[:, 0:per_scan] = ref[...]
        out = []
        for h in range(chunks):
            moved = pltpu.roll(wide[h * together : (h + 1) * together, :], 0, 1, stride=per_scan, stride_axis=0)
            out.append(row_sum(moved))
        return out

    def column(row):
        return jnp.broadcast_to(row, (LANES, LANES)).T

    scans, tiles = flat(corr_scan), flat(corr_tile)
    sublane = lax.broadcasted_iota(jnp.int32, (LANES, LANES), 0)
    lane = lax.broadcasted_iota(jnp.int32, (LANES, LANES), 1)
    targets, locals_, flats = [], [], []
    for b, t in zip(scans, tiles):
        (b_dev, b_loc), (t_dev, t_loc) = halves(b, scan_local), halves(t, tiles_local)
        targets.append((b_dev * n_grp + t_dev).astype(f32))
        locals_.append(b_loc.astype(f32))
        flats.append((b_loc * tiles_local + t_loc).astype(f32))
    target_columns = [column(x) for x in targets]
    places = []
    for h in range(chunks):
        rank = jnp.zeros((1, LANES), f32)
        for e in range(h + 1):
            same = target_columns[e] == targets[h]
            if e == h:
                same = same & (sublane < lane)
            rank = rank + row_sum(jnp.where(same, 1.0, 0.0))
        places.append(column(targets[h] * cap + rank))
    blank = jnp.zeros((4, LANES), f32)
    one = jnp.ones((1, LANES), f32)
    index = lax.broadcasted_iota(jnp.int32, (1, LANES), 1).astype(f32)
    left = jnp.concatenate(
        [
            jnp.concatenate([one, index + h * LANES, locals_[h], flats[h], blank], axis=0) for h in range(chunks)
        ],
        axis=1,
    ).astype(jnp.bfloat16)
    served = LANES // cap
    for a in range(slots.shape[0]):
        hits = [jnp.where(places[h] == (lane + a * LANES).astype(f32), 1.0, 0.0) for h in range(chunks)]
        table = lax.dot_general(
            left, jnp.concatenate(hits, axis=0).astype(jnp.bfloat16), (((1,), (0,)), ((), ())),
            preferred_element_type=f32,
        ).astype(jnp.int32)
        used, request = table[0:1, :] > 0, table[1:2, :]
        slots[a : a + 1, :] = request
        source = scan_index * scan_local + halves(request, per_scan)[0]
        kinds = [jnp.where(used, table[2:3, :], -1), table[3:4, :], jnp.where(used, source, -1)]
        total = jnp.zeros((served, LANES), jnp.int32)
        part = lax.broadcasted_iota(jnp.int32, (served, LANES), 1) // cap
        for kind, row in enumerate(kinds):
            moved = pltpu.roll(jnp.broadcast_to(row, (served, LANES)), cap, 1, stride=cap, stride_axis=0)
            if kind:
                moved = pltpu.roll(moved, kind * cap, 1)
            total = jnp.where(part == kind, moved, total)
        for i in range(served):
            meta[a * served + i] = total[served - 1 - i : served - i, :]


def greet_all(n_grp, devices, me):
    barrier = pltpu.get_barrier_semaphore()

    def hello(k, _):
        peer = lax.rem(me + k, devices)
        pl.semaphore_signal(
            barrier, inc=1, device_id=(peer // n_grp, peer % n_grp), device_id_type=pl.DeviceIdType.MESH
        )
        return 0

    lax.fori_loop(1, devices, hello, 0)


def await_all(devices):
    pl.semaphore_wait(pltpu.get_barrier_semaphore(), devices - 1)


def remote(src, dst, send, recv, peer, n_grp):
    return pltpu.make_async_remote_copy(
        src_ref=src, dst_ref=dst, send_sem=send, recv_sem=recv,
        device_id=(peer // n_grp, peer % n_grp), device_id_type=pl.DeviceIdType.MESH,
    )


def exclusive(a, b, size):
    if size & (size - 1):
        return lax.rem(a + b, size)
    total = 0
    for bit in range(size.bit_length() - 1):
        total = total + ((((a >> bit) + (b >> bit)) & 1) << bit)
    return total


def split(values):
    high = values.astype(jnp.bfloat16)
    return high, (values - high.astype(jnp.float32)).astype(jnp.bfloat16)


def contract(a, b):
    return lax.dot_general(a, b, (((1,), (1,)), ((), ())), preferred_element_type=jnp.float32)


def row_sum(products):
    return jnp.sum(products, axis=0, keepdims=True)


def exchange_kernel(
    cap, n_grp, samples_hbm, count_hbm, wanted_hbm, slots_hbm, meta, by_source, by_partner, shares,
    samples, count, wanted, slots, picks, data, data_in, meta_in, codes, tiles, comps, turned, ids, result, packed,
    send_data, recv_data, send_meta, recv_meta, send_src, recv_src, send_part, recv_part,
    send_share, recv_share, own,
):
    scan_local, tiles_local = samples.shape[0], samples.shape[2]
    per_scan = wanted.shape[1]
    n_scan = send_src.shape[0]
    devices = n_scan * n_grp
    rows = cap * 4
    width = n_grp * cap
    per_block = LANES // width
    blocks = n_scan // per_block
    sources = per_block * n_grp
    packed_rows = packed.shape[1]
    scan_index, group_index = lax.axis_index("scan"), lax.axis_index("grp")
    me = scan_index * n_grp + group_index
    home, home_row = scan_index // per_block, lax.rem(scan_index, per_block)
    full_groups = min(LEAST_POINTS // (tiles_local * LANES), n_grp) if 3 * cap % 8 == 0 else 0
    short = rows - cap

    def send_one(src, dst_index, send_index, recv_index, peer, size):
        return remote(
            data.at[pl.ds(pl.multiple_of(src * rows, 8), size)],
            data_in.at[pl.ds(pl.multiple_of(dst_index * rows, 8), size)],
            send_data.at[send_index], recv_data.at[recv_index], peer, n_grp,
        )

    def send_code(src, dst_index, send_index, recv_index, peer):
        return remote(
            meta.at[src], meta_in.at[dst_index], send_meta.at[send_index], recv_meta.at[recv_index], peer, n_grp
        )

    def to_source(row, holder, index):
        peer = row * n_grp + home
        return remote(packed.at[row], by_source.at[holder], send_src.at[row], recv_src.at[index], peer, n_grp)

    def to_partner(block, at):
        peer = scan_index * n_grp + block
        return remote(result.at[block], by_partner.at[at], send_part.at[block], recv_part.at[at], peer, n_grp)

    def to_share(g, at):
        peer = scan_index * n_grp + g
        return remote(shares.at[group_index], shares.at[at], send_share.at[g], recv_share.at[at], peer, n_grp)

    greet_all(n_grp, devices, me)
    fetch = pltpu.make_async_copy(samples_hbm, samples, own.at[3])
    fetch_count = pltpu.make_async_copy(count_hbm, count, own.at[4])
    fetch_wanted = pltpu.make_async_copy(wanted_hbm, wanted, own.at[0])
    fetch_slots = pltpu.make_async_copy(slots_hbm, slots, own.at[2])
    fetch_count.start()
    fetch_slots.start()
    fetch_wanted.start()
    fetch.start()
    fetch_count.wait()
    fetch_wanted.wait()
    fetch.wait()
    pick_rows = picks.reshape(scan_local * per_scan * 8, LANES)
    first_point = group_index * tiles_local * LANES

    def pick(s, _):
        point = wanted[s]
        tile, place = point >> 7, point & (LANES - 1)
        picked = [jnp.zeros((per_scan, LANES), jnp.float32)] * 3
        for t in range(tiles_local):
            hit = tile == t
            for c in range(3):
                row = jnp.broadcast_to(samples[s, c, pl.ds(t, 1), :], (per_scan, LANES))
                picked[c] = jnp.where(hit, lane_take(row, place), picked[c])
        picked.append(jnp.where(first_point + point < count[s], 1.0, 0.0).astype(jnp.float32))
        for c in range(4):
            pick_rows[pl.ds(s * per_scan * 8 + c, per_scan, stride=8), :] = picked[c]
        return 0

    lax.fori_loop(0, scan_local, pick, 0)
    fetch_slots.wait()

    def collect(peer, into):
        first = lax.rem(peer, LANES // cap) * cap
        for j in range(cap):
            request = slots[peer // (LANES // cap), first + j]
            into[pl.ds(peer * rows + j, 4, stride=cap), :] = picks[request, 0:4, :]

    await_all(devices)

    def start_meta(k, _):
        peer = lax.rem(me + k, devices)
        send_code(peer, me, peer, me, peer).start()
        return 0

    def wait_meta(k, _):
        peer = lax.rem(me + k, devices)
        copy = send_code(peer, peer, peer, peer, peer)
        copy.wait_send()
        copy.wait_recv()
        return 0

    def start_data(k, _):
        row = exclusive(scan_index, n_scan - 1 - k, n_scan)
        for g in range(n_grp):
            collect(row * n_grp + exclusive(group_index, g, n_grp), data)
        for g in range(n_grp):
            peer = row * n_grp + exclusive(group_index, g, n_grp)

            @pl.when((peer != me) & (group_index < full_groups))
            def _():
                send_one(peer, me, peer, me, peer, short).start()

            @pl.when((peer != me) & (group_index >= full_groups))
            def _():
                send_one(peer, me, peer, me, peer, rows).start()

        return 0

    lax.fori_loop(1, devices, start_meta, 0)
    lax.fori_loop(0, n_scan, start_data, 0)
    own_meta = pltpu.make_async_copy(meta.at[me], meta_in.at[me], own.at[1])
    own_meta.start()
    collect(me, data_in)
    own_meta.wait()

    def no_mask(row, _):
        for g in range(full_groups):
            first = pl.multiple_of((row * n_grp + g) * rows + short, 8)
            data_in[pl.ds(first, cap), :] = jnp.ones((cap, LANES), jnp.float32)
        return 0

    lax.fori_loop(0, n_scan, no_mask, 0)
    shares[...] = jnp.zeros_like(shares)
    result[...] = jnp.zeros_like(result)

    point = lax.broadcasted_iota(jnp.int32, (tiles_local, LANES), 0) * LANES
    point = point + lax.broadcasted_iota(jnp.int32, (tiles_local, LANES), 1)

    tile_rows = tiles.reshape(scan_local * tiles_local * 8, LANES)

    def fill(b, _):
        valid = point < count[b] - group_index * tiles_local * LANES
        for c in range(6):
            values = samples[b, c]
            if c >= 3:
                values = jnp.where(valid, values, 0.0)
            tile_rows[pl.ds(b * tiles_local * 8 + c, tiles_local, stride=8), :] = values
        return 0

    lax.fori_loop(0, scan_local, fill, 0)
    lax.fori_loop(1, devices, wait_meta, 0)
    to_scalar = pltpu.make_async_copy(meta_in, codes, own.at[2])
    to_scalar.start()

    slot_lane = lax.broadcasted_iota(jnp.int32, (sources, LANES), 1) // cap
    slot_row = lax.broadcasted_iota(jnp.int32, (sources, LANES), 0)

    def decode(m, _):
        arrived = meta_in[pl.ds(m * sources, sources), 0, :]
        kinds = []
        for kind in (0, 2):
            moved = pltpu.roll(arrived, LANES - kind * cap, 1) if kind else arrived
            moved = pltpu.roll(moved, 0, 1, stride=cap, stride_axis=0)
            kinds.append(row_sum(jnp.where(slot_lane == slot_row, moved, 0)))
        partner, source = kinds
        ids[m, 0:1, :] = source.astype(jnp.float32)
        ids[m, 1:2, :] = jnp.where(partner < 0, -1, scan_index * scan_local + partner).astype(jnp.float32)
        return 0

    lax.fori_loop(0, blocks, decode, 0)
    to_scalar.wait()

    def one_block(k, _):
        m = exclusive(home, blocks - 1 - k, blocks)

        def gather(i, _):
            for j in range(cap):
                slot = i * cap + j
                row = codes[m * sources + i, 0, cap + j]
                comps[pl.ds(pl.multiple_of(slot * 8, 8), 8), :] = tiles[row]
            return 0

        lax.fori_loop(0, sources, gather, 0)
        for c in range(6):
            turned[4 + c] = comps[pl.ds(c, LANES, stride=8), :].T

        def arrive(i, _):
            source = m * sources + i
            group = lax.rem(i, n_grp)

            @pl.when((source != me) & (group < full_groups))
            def _():
                send_one(source, source, source, source, source, short).wait_recv()

            @pl.when((source != me) & (group >= full_groups))
            def _():
                send_one(source, source, source, source, source, rows).wait_recv()

            return 0

        lax.fori_loop(0, sources, arrive, 0)
        for c in range(4):
            pieces = [
                data_in[pl.ds((m * sources + i) * rows + c * cap, cap), :] for i in range(sources)
            ]
            turned[c] = jnp.concatenate(pieces, axis=0).T

        def step(kk, sums):
            at = pl.ds(pl.multiple_of(kk * 8, 8), 8)
            px, py, pz, mask, qx, qy, qz, nx, ny, nz = [turned[c, at, :] for c in range(10)]
            residual = nx * (px - qx) + ny * (py - qy) + nz * (pz - qz)
            weight = mask / (1.0 + residual * residual)
            jac = [py * nz - pz * ny, pz * nx - px * nz, px * ny - py * nx, nx, ny, nz]
            scaled = [weight * x for x in jac]
            products = [scaled[a] * jac[b] for a, b in PAIRS] + [x * residual for x in scaled]
            return tuple(s + p for s, p in zip(sums, products))

        zero = jnp.zeros((8, LANES), jnp.float32)
        sums = lax.fori_loop(0, LANES // 8, step, (zero,) * (len(PAIRS) + 6))
        for q, total in enumerate(sums):
            result[m, q : q + 1, :] = row_sum(total)
        result[m, 27:29, :] = ids[m, 0:2, :]
        values = result[m]
        lane = lax.broadcasted_iota(jnp.int32, (packed_rows, LANES), 1) // width
        chunks = [values[g * packed_rows : (g + 1) * packed_rows, :] for g in range(per_block)]
        for p in range(per_block):
            total = chunks[p]
            for g in range(per_block):
                if g != p:
                    total = jnp.where(lane == g, pltpu.roll(chunks[g], (g - p) * width % LANES, 1), total)
            row = m * per_block + p
            packed[row] = total
            holder = group_index * per_block + home_row

            @pl.when(row * n_grp + home == me)
            def _():
                by_source[holder] = total

            @pl.when(row * n_grp + home != me)
            def _():
                to_source(row, holder, holder).start()

        @pl.when(m == group_index)
        def _():
            by_partner[group_index] = values

        @pl.when(m != group_index)
        def _():
            to_partner(m, group_index).start()

        return 0

    lax.fori_loop(0, blocks, one_block, 0)

    for holder in range(sources):
        group, other = holder // per_block, holder % per_block
        peer = (group_index * per_block + other) * n_grp + group

        @pl.when(peer != me)
        def _():
            to_source(0, holder, holder).wait_recv()

    for g in range(n_grp):

        @pl.when(g != group_index)
        def _():
            to_partner(0, g).wait_recv()

    span = lax.broadcasted_iota(jnp.int32, (2 * scan_local, LANES), 0)
    values, chosen = [], []
    for g in range(n_grp):
        parts = [by_source[g * per_block + p] for p in range(per_block)]
        block = jnp.concatenate(regroup(parts, width), axis=0)
        values.append(block)
        at = block[27:28, :].astype(jnp.int32) - scan_index * scan_local
        chosen.append(jnp.where(span == at, 1.0, 0.0))
    for g in range(n_grp):
        block = by_partner[g]
        values.append(block)
        at = block[28:29, :].astype(jnp.int32) - scan_index * scan_local
        chosen.append(jnp.where((at >= 0) & (span - scan_local == at), 1.0, 0.0))
    high, low = split(jnp.concatenate(values, axis=1))
    matrix = jnp.concatenate(chosen, axis=1).astype(jnp.bfloat16)
    shares[group_index, :, 0 : 2 * scan_local] = contract(high, matrix) + contract(low, matrix)
    for g in range(n_grp):

        @pl.when(g != group_index)
        def _():
            to_share(g, group_index).start()

    def finish(k, _):
        peer = lax.rem(me + k, devices)

        @pl.when(group_index < full_groups)
        def _():
            send_one(peer, peer, peer, peer, peer, short).wait_send()

        @pl.when(group_index >= full_groups)
        def _():
            send_one(peer, peer, peer, peer, peer, rows).wait_send()

        return 0

    lax.fori_loop(1, devices, finish, 0)

    def finish_source(row, _):
        @pl.when(row * n_grp + home != me)
        def _():
            to_source(row, 0, 0).wait_send()

        return 0

    lax.fori_loop(0, n_scan, finish_source, 0)
    for g in range(n_grp):

        @pl.when(g != group_index)
        def _():
            to_partner(g, 0).wait_send()
            copy = to_share(g, g)
            copy.wait_send()
            copy.wait_recv()


def regroup(parts, width):
    groups = len(parts)
    lane = lax.broadcasted_iota(jnp.int32, parts[0].shape, 1) // width
    out = []
    for b in range(groups):
        total = parts[b]
        for g in range(groups):
            if g != b:
                total = jnp.where(lane == g, pltpu.roll(parts[g], (g - b) * width % LANES, 1), total)
        out.append(total)
    return out


def assemble_kernel(n_grp, width, by_source, by_partner, shares, hessian, gradient, spare):
    rows, columns = hessian.shape[2], hessian.shape[3]
    grad_rows = gradient.shape[0]
    per_block = LANES // width
    scan_index, group_index = lax.axis_index("scan"), lax.axis_index("grp")
    home, home_row = scan_index // per_block, lax.rem(scan_index, per_block)
    first_row, first_column = scan_index * rows, group_index * columns
    count = len(PAIRS)

    share = shares[0]
    for g in range(1, n_grp):
        share = share + shares[g]
    other = pltpu.roll(share, LANES - rows, 1)
    spare[...] = (share - other).T
    gradient[...] = spare[pl.ds(group_index * grad_rows, grad_rows), 21:27]

    pieces = []
    for g in range(n_grp):
        parts = [by_source[g * per_block + p] for p in range(per_block)]
        block = jnp.concatenate(regroup(parts, width), axis=0)
        source, partner = block[27:28, :].astype(jnp.int32), block[28:29, :].astype(jnp.int32)
        pieces.append((block, source - first_row, partner - first_column))
    for g in range(n_grp):
        block = by_partner[g]
        source, partner = block[27:28, :].astype(jnp.int32), block[28:29, :].astype(jnp.int32)
        pieces.append((block, partner - first_row, source - first_column))
    lane = lax.broadcasted_iota(jnp.int32, (1, LANES), 1)
    diagonal = jnp.where((lane < rows) & (group_index == home), lane, -1)
    pieces.append((share + other, diagonal, jnp.where(diagonal < 0, -1, lane + home_row * rows)))

    left, right = [], []
    row = lax.broadcasted_iota(jnp.int32, (rows, LANES), 0)
    column = lax.broadcasted_iota(jnp.int32, (columns, LANES), 0)
    for index, (block, at, to) in enumerate(pieces):
        hit = row == at
        left.append(jnp.concatenate([jnp.where(hit, block[q : q + 1, :], 0.0) for q in range(count)], axis=0))
        right.append(jnp.where(column == to, 1.0 if index == 2 * n_grp else -1.0, 0.0))
    matrix = jnp.concatenate(right, axis=1).astype(jnp.bfloat16)
    high, low = split(jnp.concatenate(left, axis=1))
    total = contract(high, matrix) + contract(low, matrix)
    where = {pair: q for q, pair in enumerate(PAIRS)}
    for i in range(6):
        for j in range(6):
            q = where[min(i, j), max(i, j)]
            hessian[i, j] = total[q * rows : (q + 1) * rows, :]


def local(samples, point_count, corr_scan, corr_tile, corr_src):
    f32, i32 = jnp.float32, jnp.int32
    scan_local, tiles_local = samples.shape[0], samples.shape[1]
    request_count = scan_local * corr_scan.shape[1]
    n_scan, n_grp = lax.axis_size("scan"), lax.axis_size("grp")
    devices = n_scan * n_grp
    cap = 2 * request_count // devices
    width = n_grp * cap
    packed_rows = VALUES * width // LANES
    per_block = LANES // width
    blocks = n_scan // per_block
    columns = scan_local * n_scan // n_grp
    grad_rows = scan_local // n_grp
    assert blocks == n_grp and blocks * per_block == n_scan and 2 * scan_local <= LANES
    shape = jax.ShapeDtypeStruct
    dma = pltpu.SemaphoreType.DMA

    tiles = samples.transpose(0, 2, 1, 3)
    per_scan = corr_scan.shape[1]
    assert request_count <= 256 and scan_local * tiles_local <= 256
    slots, meta = pl.pallas_call(
        functools.partial(route_kernel, cap, n_grp, scan_local, tiles_local),
        out_shape=(shape((devices * cap // LANES, LANES), i32), shape((devices, 1, LANES), i32)),
        in_specs=[VMEM, VMEM],
        out_specs=(VMEM, VMEM),
        scratch_shapes=[pltpu.VMEM((scan_local, LANES), i32)],
    )(corr_scan, corr_tile)

    by_source, by_partner, shares = pl.pallas_call(
        functools.partial(exchange_kernel, cap, n_grp),
        out_shape=(
            shape((n_grp * per_block, packed_rows, LANES), f32),
            shape((n_grp, VALUES, LANES), f32),
            shape((n_grp, VALUES, LANES), f32),
        ),
        in_specs=[ANY] * 5,
        out_specs=(VMEM, VMEM, VMEM),
        scratch_shapes=[
            pltpu.VMEM(tiles.shape, f32),
            pltpu.SMEM(point_count.shape, i32),
            pltpu.VMEM(corr_src.shape, i32),
            pltpu.SMEM(slots.shape, i32),
            pltpu.VMEM((request_count, 8, LANES), f32),
            pltpu.VMEM((devices * cap * 4, LANES), f32),
            pltpu.VMEM((devices * cap * 4, LANES), f32),
            pltpu.VMEM(meta.shape, i32),
            pltpu.SMEM(meta.shape, i32),
            pltpu.VMEM((scan_local * tiles_local, 8, LANES), f32),
            pltpu.VMEM((LANES * 8, LANES), f32),
            pltpu.VMEM((10, LANES, LANES), f32),
            pltpu.VMEM((blocks, 8, LANES), f32),
            pltpu.VMEM((blocks, VALUES, LANES), f32),
            pltpu.VMEM((n_scan, packed_rows, LANES), f32),
        ]
        + [dma((devices,))] * 4
        + [dma((n_scan,)), dma((n_grp * per_block,))]
        + [dma((n_grp,))] * 4
        + [dma((5,))],
        compiler_params=pltpu.CompilerParams(collective_id=0, has_side_effects=True),
    )(tiles, point_count, corr_src, slots, meta)

    hessian, gradient = pl.pallas_call(
        functools.partial(assemble_kernel, n_grp, width),
        out_shape=(shape((6, 6, scan_local, columns), f32), shape((grad_rows, 6), f32)),
        in_specs=[VMEM, VMEM, VMEM],
        out_specs=(VMEM, VMEM),
        scratch_shapes=[pltpu.VMEM((LANES, VALUES), f32)],
    )(by_source, by_partner, shares)
    return hessian.transpose(2, 0, 1, 3), gradient


def solution(mesh):
    placed = (
        P("scan", "grp", None, None),
        P("scan"),
        P("scan", "grp"),
        P("scan", "grp"),
        P("scan", "grp", None),
    )
    return jax.shard_map(
        local,
        mesh=mesh,
        in_specs=placed,
        out_specs=(P("scan", None, None, "grp"), P(("scan", "grp"), None)),
        check_vma=False,
    )
```

```python
import functools

import jax
import jax.numpy as jnp
from jax import lax
from jax.experimental import pallas as pl
from jax.experimental.pallas import tpu as pltpu
from jax.sharding import PartitionSpec as P

LANES = 128
VALUES = 32
LEAST_POINTS = 4096
PAIRS = [(i, j) for i in range(6) for j in range(i, 6)]
VMEM = pl.BlockSpec(memory_space=pltpu.VMEM)
SMEM = pl.BlockSpec(memory_space=pltpu.SMEM)
ANY = pl.BlockSpec(memory_space=pl.ANY)


def halves(value, size):
    if size & (size - 1):
        return value // size, value % size
    return value >> (size.bit_length() - 1), value & (size - 1)


def lane_take(table, index):
    return jnp.take_along_axis(table, index, axis=1, mode="promise_in_bounds")


def route_kernel(cap, n_grp, scan_local, tiles_local, corr_scan, corr_tile, slots, meta, wide):
    per_scan = corr_scan.shape[1]
    scan_index = lax.axis_index("scan")
    requests = scan_local * per_scan
    chunks, together = requests // LANES, LANES // per_scan
    f32 = jnp.float32

    def flat(ref):
        wide[...] = jnp.zeros_like(wide)
        wide[:, 0:per_scan] = ref[...]
        out = []
        for h in range(chunks):
            moved = pltpu.roll(wide[h * together : (h + 1) * together, :], 0, 1, stride=per_scan, stride_axis=0)
            out.append(row_sum(moved))
        return out

    def column(row):
        return jnp.broadcast_to(row, (LANES, LANES)).T

    scans, tiles = flat(corr_scan), flat(corr_tile)
    sublane = lax.broadcasted_iota(jnp.int32, (LANES, LANES), 0)
    lane = lax.broadcasted_iota(jnp.int32, (LANES, LANES), 1)
    targets, locals_, flats = [], [], []
    for b, t in zip(scans, tiles):
        (b_dev, b_loc), (t_dev, t_loc) = halves(b, scan_local), halves(t, tiles_local)
        targets.append((b_dev * n_grp + t_dev).astype(f32))
        locals_.append(b_loc.astype(f32))
        flats.append((b_loc * tiles_local + t_loc).astype(f32))
    target_columns = [column(x) for x in targets]
    places = []
    for h in range(chunks):
        rank = jnp.zeros((1, LANES), f32)
        for e in range(h + 1):
            same = target_columns[e] == targets[h]
            if e == h:
                same = same & (sublane < lane)
            rank = rank + row_sum(jnp.where(same, 1.0, 0.0))
        places.append(column(targets[h] * cap + rank))
    blank = jnp.zeros((4, LANES), f32)
    one = jnp.ones((1, LANES), f32)
    index = lax.broadcasted_iota(jnp.int32, (1, LANES), 1).astype(f32)
    left = jnp.concatenate(
        [
            jnp.concatenate([one, index + h * LANES, locals_[h], flats[h], blank], axis=0) for h in range(chunks)
        ],
        axis=1,
    ).astype(jnp.bfloat16)
    served = LANES // cap
    for a in range(slots.shape[0]):
        hits = [jnp.where(places[h] == (lane + a * LANES).astype(f32), 1.0, 0.0) for h in range(chunks)]
        table = lax.dot_general(
            left, jnp.concatenate(hits, axis=0).astype(jnp.bfloat16), (((1,), (0,)), ((), ())),
            preferred_element_type=f32,
        ).astype(jnp.int32)
        used, request = table[0:1, :] > 0, table[1:2, :]
        slots[a : a + 1, :] = request
        source = scan_index * scan_local + halves(request, per_scan)[0]
        kinds = [jnp.where(used, table[2:3, :], -1), table[3:4, :], jnp.where(used, source, -1)]
        total = jnp.zeros((served, LANES), jnp.int32)
        part = lax.broadcasted_iota(jnp.int32, (served, LANES), 1) // cap
        for kind, row in enumerate(kinds):
            moved = pltpu.roll(jnp.broadcast_to(row, (served, LANES)), cap, 1, stride=cap, stride_axis=0)
            if kind:
                moved = pltpu.roll(moved, kind * cap, 1)
            total = jnp.where(part == kind, moved, total)
        for i in range(served):
            meta[a * served + i] = total[served - 1 - i : served - i, :]


def greet_all(n_grp, devices, me):
    barrier = pltpu.get_barrier_semaphore()

    def hello(k, _):
        peer = lax.rem(me + k, devices)
        pl.semaphore_signal(
            barrier, inc=1, device_id=(peer // n_grp, peer % n_grp), device_id_type=pl.DeviceIdType.MESH
        )
        return 0

    lax.fori_loop(1, devices, hello, 0)


def await_all(devices):
    pl.semaphore_wait(pltpu.get_barrier_semaphore(), devices - 1)


def remote(src, dst, send, recv, peer, n_grp):
    return pltpu.make_async_remote_copy(
        src_ref=src, dst_ref=dst, send_sem=send, recv_sem=recv,
        device_id=(peer // n_grp, peer % n_grp), device_id_type=pl.DeviceIdType.MESH,
    )


def exclusive(a, b, size):
    if size & (size - 1):
        return lax.rem(a + b, size)
    total = 0
    for bit in range(size.bit_length() - 1):
        total = total + ((((a >> bit) + (b >> bit)) & 1) << bit)
    return total


def split(values):
    high = values.astype(jnp.bfloat16)
    return high, (values - high.astype(jnp.float32)).astype(jnp.bfloat16)


def contract(a, b):
    return lax.dot_general(a, b, (((1,), (1,)), ((), ())), preferred_element_type=jnp.float32)


def row_sum(products):
    return jnp.sum(products, axis=0, keepdims=True)


def exchange_kernel(
    cap, n_grp, samples_hbm, count_hbm, wanted_hbm, slots_hbm, meta, by_source, by_partner, shares,
    samples, count, wanted, slots, picks, data, data_in, meta_in, codes, tiles, comps, turned, ids, result, packed,
    send_data, recv_data, send_meta, recv_meta, send_src, recv_src, send_part, recv_part,
    send_share, recv_share, own,
):
    scan_local, tiles_local = samples.shape[0], samples.shape[2]
    per_scan = wanted.shape[1]
    n_scan = send_src.shape[0]
    devices = n_scan * n_grp
    rows = cap * 4
    width = n_grp * cap
    per_block = LANES // width
    blocks = n_scan // per_block
    sources = per_block * n_grp
    packed_rows = packed.shape[1]
    scan_index, group_index = lax.axis_index("scan"), lax.axis_index("grp")
    me = scan_index * n_grp + group_index
    home, home_row = scan_index // per_block, lax.rem(scan_index, per_block)
    full_groups = min(LEAST_POINTS // (tiles_local * LANES), n_grp) if 3 * cap % 8 == 0 else 0
    short = rows - cap

    def send_one(src, dst_index, send_index, recv_index, peer, size):
        return remote(
            data.at[pl.ds(pl.multiple_of(src * rows, 8), size)],
            data_in.at[pl.ds(pl.multiple_of(dst_index * rows, 8), size)],
            send_data.at[send_index], recv_data.at[recv_index], peer, n_grp,
        )

    def send_code(src, dst_index, send_index, recv_index, peer):
        return remote(
            meta.at[src], meta_in.at[dst_index], send_meta.at[send_index], recv_meta.at[recv_index], peer, n_grp
        )

    def to_source(row, holder, index):
        peer = row * n_grp + home
        return remote(packed.at[row], by_source.at[holder], send_src.at[row], recv_src.at[index], peer, n_grp)

    def to_partner(block, at):
        peer = scan_index * n_grp + block
        return remote(result.at[block], by_partner.at[at], send_part.at[block], recv_part.at[at], peer, n_grp)

    def to_share(g, at):
        peer = scan_index * n_grp + g
        return remote(shares.at[group_index], shares.at[at], send_share.at[g], recv_share.at[at], peer, n_grp)

    greet_all(n_grp, devices, me)
    fetch = pltpu.make_async_copy(samples_hbm, samples, own.at[3])
    fetch_count = pltpu.make_async_copy(count_hbm, count, own.at[4])
    fetch_wanted = pltpu.make_async_copy(wanted_hbm, wanted, own.at[0])
    fetch_slots = pltpu.make_async_copy(slots_hbm, slots, own.at[2])
    fetch_count.start()
    fetch_slots.start()
    fetch_wanted.start()
    fetch.start()
    fetch_count.wait()
    fetch_wanted.wait()
    fetch.wait()
    pick_rows = picks.reshape(scan_local * per_scan * 8, LANES)
    first_point = group_index * tiles_local * LANES

    def pick(s, _):
        point = wanted[s]
        tile, place = point >> 7, point & (LANES - 1)
        picked = [jnp.zeros((per_scan, LANES), jnp.float32)] * 3
        for t in range(tiles_local):
            hit = tile == t
            for c in range(3):
                row = jnp.broadcast_to(samples[s, c, pl.ds(t, 1), :], (per_scan, LANES))
                picked[c] = jnp.where(hit, lane_take(row, place), picked[c])
        picked.append(jnp.where(first_point + point < count[s], 1.0, 0.0).astype(jnp.float32))
        for c in range(4):
            pick_rows[pl.ds(s * per_scan * 8 + c, per_scan, stride=8), :] = picked[c]
        return 0

    lax.fori_loop(0, scan_local, pick, 0)
    fetch_slots.wait()

    def collect(peer, into):
        first = lax.rem(peer, LANES // cap) * cap
        for j in range(cap):
            request = slots[peer // (LANES // cap), first + j]
            into[pl.ds(peer * rows + j, 4, stride=cap), :] = picks[request, 0:4, :]

    await_all(devices)

    def start_meta(k, _):
        peer = lax.rem(me + k, devices)
        send_code(peer, me, peer, me, peer).start()
        return 0

    def wait_meta(k, _):
        peer = lax.rem(me + k, devices)
        copy = send_code(peer, peer, peer, peer, peer)
        copy.wait_send()
        copy.wait_recv()
        return 0

    def start_data(k, _):
        row = exclusive(scan_index, k + 1 - 2 * (k & 1), n_scan)
        for g in reversed(range(n_grp)):
            collect(row * n_grp + exclusive(group_index, g, n_grp), data)
        for g in reversed(range(n_grp)):
            peer = row * n_grp + exclusive(group_index, g, n_grp)

            @pl.when((peer != me) & (group_index < full_groups))
            def _():
                send_one(peer, me, peer, me, peer, short).start()

            @pl.when((peer != me) & (group_index >= full_groups))
            def _():
                send_one(peer, me, peer, me, peer, rows).start()

        return 0

    lax.fori_loop(1, devices, start_meta, 0)
    lax.fori_loop(0, n_scan, start_data, 0)
    own_meta = pltpu.make_async_copy(meta.at[me], meta_in.at[me], own.at[1])
    own_meta.start()
    collect(me, data_in)
    own_meta.wait()

    def no_mask(row, _):
        for g in range(full_groups):
            first = pl.multiple_of((row * n_grp + g) * rows + short, 8)
            data_in[pl.ds(first, cap), :] = jnp.ones((cap, LANES), jnp.float32)
        return 0

    lax.fori_loop(0, n_scan, no_mask, 0)
    shares[...] = jnp.zeros_like(shares)
    result[...] = jnp.zeros_like(result)

    point = lax.broadcasted_iota(jnp.int32, (tiles_local, LANES), 0) * LANES
    point = point + lax.broadcasted_iota(jnp.int32, (tiles_local, LANES), 1)

    tile_rows = tiles.reshape(scan_local * tiles_local * 8, LANES)

    def fill(b, _):
        valid = point < count[b] - group_index * tiles_local * LANES
        for c in range(6):
            values = samples[b, c]
            if c >= 3:
                values = jnp.where(valid, values, 0.0)
            tile_rows[pl.ds(b * tiles_local * 8 + c, tiles_local, stride=8), :] = values
        return 0

    lax.fori_loop(0, scan_local, fill, 0)
    lax.fori_loop(1, devices, wait_meta, 0)
    to_scalar = pltpu.make_async_copy(meta_in, codes, own.at[2])
    to_scalar.start()

    slot_lane = lax.broadcasted_iota(jnp.int32, (sources, LANES), 1) // cap
    slot_row = lax.broadcasted_iota(jnp.int32, (sources, LANES), 0)

    def decode(m, _):
        arrived = meta_in[pl.ds(m * sources, sources), 0, :]
        kinds = []
        for kind in (0, 2):
            moved = pltpu.roll(arrived, LANES - kind * cap, 1) if kind else arrived
            moved = pltpu.roll(moved, 0, 1, stride=cap, stride_axis=0)
            kinds.append(row_sum(jnp.where(slot_lane == slot_row, moved, 0)))
        partner, source = kinds
        ids[m, 0:1, :] = source.astype(jnp.float32)
        ids[m, 1:2, :] = jnp.where(partner < 0, -1, scan_index * scan_local + partner).astype(jnp.float32)
        return 0

    lax.fori_loop(0, blocks, decode, 0)
    to_scalar.wait()

    def one_block(k, _):
        m = exclusive(home, k, blocks)

        def gather(i, _):
            for j in range(cap):
                slot = i * cap + j
                row = codes[m * sources + i, 0, cap + j]
                comps[pl.ds(pl.multiple_of(slot * 8, 8), 8), :] = tiles[row]
            return 0

        lax.fori_loop(0, sources, gather, 0)
        for c in range(6):
            turned[4 + c] = comps[pl.ds(c, LANES, stride=8), :].T

        def arrive(i, _):
            source = m * sources + i
            group = lax.rem(i, n_grp)

            @pl.when((source != me) & (group < full_groups))
            def _():
                send_one(source, source, source, source, source, short).wait_recv()

            @pl.when((source != me) & (group >= full_groups))
            def _():
                send_one(source, source, source, source, source, rows).wait_recv()

            return 0

        lax.fori_loop(0, sources, arrive, 0)
        for c in range(4):
            pieces = [
                data_in[pl.ds((m * sources + i) * rows + c * cap, cap), :] for i in range(sources)
            ]
            turned[c] = jnp.concatenate(pieces, axis=0).T

        def step(kk, sums):
            at = pl.ds(pl.multiple_of(kk * 8, 8), 8)
            px, py, pz, mask, qx, qy, qz, nx, ny, nz = [turned[c, at, :] for c in range(10)]
            residual = nx * (px - qx) + ny * (py - qy) + nz * (pz - qz)
            weight = mask / (1.0 + residual * residual)
            jac = [py * nz - pz * ny, pz * nx - px * nz, px * ny - py * nx, nx, ny, nz]
            scaled = [weight * x for x in jac]
            products = [scaled[a] * jac[b] for a, b in PAIRS] + [x * residual for x in scaled]
            return tuple(s + p for s, p in zip(sums, products))

        zero = jnp.zeros((8, LANES), jnp.float32)
        sums = lax.fori_loop(0, LANES // 8, step, (zero,) * (len(PAIRS) + 6))
        for q, total in enumerate(sums):
            result[m, q : q + 1, :] = row_sum(total)
        result[m, 27:29, :] = ids[m, 0:2, :]
        values = result[m]
        lane = lax.broadcasted_iota(jnp.int32, (packed_rows, LANES), 1) // width
        chunks = [values[g * packed_rows : (g + 1) * packed_rows, :] for g in range(per_block)]
        for p in range(per_block):
            total = chunks[p]
            for g in range(per_block):
                if g != p:
                    total = jnp.where(lane == g, pltpu.roll(chunks[g], (g - p) * width % LANES, 1), total)
            row = m * per_block + p
            packed[row] = total
            holder = group_index * per_block + home_row

            @pl.when(row * n_grp + home == me)
            def _():
                by_source[holder] = total

            @pl.when(row * n_grp + home != me)
            def _():
                to_source(row, holder, holder).start()

        @pl.when(m == group_index)
        def _():
            by_partner[group_index] = values

        @pl.when(m != group_index)
        def _():
            to_partner(m, group_index).start()

        return 0

    lax.fori_loop(0, blocks, one_block, 0)

    for holder in range(sources):
        group, other = holder // per_block, holder % per_block
        peer = (group_index * per_block + other) * n_grp + group

        @pl.when(peer != me)
        def _():
            to_source(0, holder, holder).wait_recv()

    for g in range(n_grp):

        @pl.when(g != group_index)
        def _():
            to_partner(0, g).wait_recv()

    span = lax.broadcasted_iota(jnp.int32, (2 * scan_local, LANES), 0)
    values, chosen = [], []
    for g in range(n_grp):
        parts = [by_source[g * per_block + p] for p in range(per_block)]
        block = jnp.concatenate(regroup(parts, width), axis=0)
        values.append(block)
        at = block[27:28, :].astype(jnp.int32) - scan_index * scan_local
        chosen.append(jnp.where(span == at, 1.0, 0.0))
    for g in range(n_grp):
        block = by_partner[g]
        values.append(block)
        at = block[28:29, :].astype(jnp.int32) - scan_index * scan_local
        chosen.append(jnp.where((at >= 0) & (span - scan_local == at), 1.0, 0.0))
    high, low = split(jnp.concatenate(values, axis=1))
    matrix = jnp.concatenate(chosen, axis=1).astype(jnp.bfloat16)
    shares[group_index, :, 0 : 2 * scan_local] = contract(high, matrix) + contract(low, matrix)
    for g in range(n_grp):

        @pl.when(g != group_index)
        def _():
            to_share(g, group_index).start()

    def finish(k, _):
        peer = lax.rem(me + k, devices)

        @pl.when(group_index < full_groups)
        def _():
            send_one(peer, peer, peer, peer, peer, short).wait_send()

        @pl.when(group_index >= full_groups)
        def _():
            send_one(peer, peer, peer, peer, peer, rows).wait_send()

        return 0

    lax.fori_loop(1, devices, finish, 0)

    def finish_source(row, _):
        @pl.when(row * n_grp + home != me)
        def _():
            to_source(row, 0, 0).wait_send()

        return 0

    lax.fori_loop(0, n_scan, finish_source, 0)
    for g in range(n_grp):

        @pl.when(g != group_index)
        def _():
            to_partner(g, 0).wait_send()
            copy = to_share(g, g)
            copy.wait_send()
            copy.wait_recv()


def regroup(parts, width):
    groups = len(parts)
    lane = lax.broadcasted_iota(jnp.int32, parts[0].shape, 1) // width
    out = []
    for b in range(groups):
        total = parts[b]
        for g in range(groups):
            if g != b:
                total = jnp.where(lane == g, pltpu.roll(parts[g], (g - b) * width % LANES, 1), total)
        out.append(total)
    return out


def assemble_kernel(n_grp, width, by_source, by_partner, shares, hessian, gradient, spare):
    rows, columns = hessian.shape[2], hessian.shape[3]
    grad_rows = gradient.shape[0]
    per_block = LANES // width
    scan_index, group_index = lax.axis_index("scan"), lax.axis_index("grp")
    home, home_row = scan_index // per_block, lax.rem(scan_index, per_block)
    first_row, first_column = scan_index * rows, group_index * columns
    count = len(PAIRS)

    share = shares[0]
    for g in range(1, n_grp):
        share = share + shares[g]
    other = pltpu.roll(share, LANES - rows, 1)
    spare[...] = (share - other).T
    gradient[...] = spare[pl.ds(group_index * grad_rows, grad_rows), 21:27]

    pieces = []
    for g in range(n_grp):
        parts = [by_source[g * per_block + p] for p in range(per_block)]
        block = jnp.concatenate(regroup(parts, width), axis=0)
        source, partner = block[27:28, :].astype(jnp.int32), block[28:29, :].astype(jnp.int32)
        pieces.append((block, source - first_row, partner - first_column))
    for g in range(n_grp):
        block = by_partner[g]
        source, partner = block[27:28, :].astype(jnp.int32), block[28:29, :].astype(jnp.int32)
        pieces.append((block, partner - first_row, source - first_column))
    lane = lax.broadcasted_iota(jnp.int32, (1, LANES), 1)
    diagonal = jnp.where((lane < rows) & (group_index == home), lane, -1)
    pieces.append((share + other, diagonal, jnp.where(diagonal < 0, -1, lane + home_row * rows)))

    left, right = [], []
    row = lax.broadcasted_iota(jnp.int32, (rows, LANES), 0)
    column = lax.broadcasted_iota(jnp.int32, (columns, LANES), 0)
    for index, (block, at, to) in enumerate(pieces):
        hit = row == at
        left.append(jnp.concatenate([jnp.where(hit, block[q : q + 1, :], 0.0) for q in range(count)], axis=0))
        right.append(jnp.where(column == to, 1.0 if index == 2 * n_grp else -1.0, 0.0))
    matrix = jnp.concatenate(right, axis=1).astype(jnp.bfloat16)
    high, low = split(jnp.concatenate(left, axis=1))
    total = contract(high, matrix) + contract(low, matrix)
    where = {pair: q for q, pair in enumerate(PAIRS)}
    for i in range(6):
        for j in range(6):
            q = where[min(i, j), max(i, j)]
            hessian[i, j] = total[q * rows : (q + 1) * rows, :]


def local(samples, point_count, corr_scan, corr_tile, corr_src):
    f32, i32 = jnp.float32, jnp.int32
    scan_local, tiles_local = samples.shape[0], samples.shape[1]
    request_count = scan_local * corr_scan.shape[1]
    n_scan, n_grp = lax.axis_size("scan"), lax.axis_size("grp")
    devices = n_scan * n_grp
    cap = 2 * request_count // devices
    width = n_grp * cap
    packed_rows = VALUES * width // LANES
    per_block = LANES // width
    blocks = n_scan // per_block
    columns = scan_local * n_scan // n_grp
    grad_rows = scan_local // n_grp
    assert blocks == n_grp and blocks * per_block == n_scan and 2 * scan_local <= LANES
    shape = jax.ShapeDtypeStruct
    dma = pltpu.SemaphoreType.DMA

    tiles = samples.transpose(0, 2, 1, 3)
    per_scan = corr_scan.shape[1]
    assert request_count <= 256 and scan_local * tiles_local <= 256
    slots, meta = pl.pallas_call(
        functools.partial(route_kernel, cap, n_grp, scan_local, tiles_local),
        out_shape=(shape((devices * cap // LANES, LANES), i32), shape((devices, 1, LANES), i32)),
        in_specs=[VMEM, VMEM],
        out_specs=(VMEM, VMEM),
        scratch_shapes=[pltpu.VMEM((scan_local, LANES), i32)],
    )(corr_scan, corr_tile)

    by_source, by_partner, shares = pl.pallas_call(
        functools.partial(exchange_kernel, cap, n_grp),
        out_shape=(
            shape((n_grp * per_block, packed_rows, LANES), f32),
            shape((n_grp, VALUES, LANES), f32),
            shape((n_grp, VALUES, LANES), f32),
        ),
        in_specs=[ANY] * 5,
        out_specs=(VMEM, VMEM, VMEM),
        scratch_shapes=[
            pltpu.VMEM(tiles.shape, f32),
            pltpu.SMEM(point_count.shape, i32),
            pltpu.VMEM(corr_src.shape, i32),
            pltpu.SMEM(slots.shape, i32),
            pltpu.VMEM((request_count, 8, LANES), f32),
            pltpu.VMEM((devices * cap * 4, LANES), f32),
            pltpu.VMEM((devices * cap * 4, LANES), f32),
            pltpu.VMEM(meta.shape, i32),
            pltpu.SMEM(meta.shape, i32),
            pltpu.VMEM((scan_local * tiles_local, 8, LANES), f32),
            pltpu.VMEM((LANES * 8, LANES), f32),
            pltpu.VMEM((10, LANES, LANES), f32),
            pltpu.VMEM((blocks, 8, LANES), f32),
            pltpu.VMEM((blocks, VALUES, LANES), f32),
            pltpu.VMEM((n_scan, packed_rows, LANES), f32),
        ]
        + [dma((devices,))] * 4
        + [dma((n_scan,)), dma((n_grp * per_block,))]
        + [dma((n_grp,))] * 4
        + [dma((5,))],
        compiler_params=pltpu.CompilerParams(collective_id=0, has_side_effects=True),
    )(tiles, point_count, corr_src, slots, meta)

    hessian, gradient = pl.pallas_call(
        functools.partial(assemble_kernel, n_grp, width),
        out_shape=(shape((6, 6, scan_local, columns), f32), shape((grad_rows, 6), f32)),
        in_specs=[VMEM, VMEM, VMEM],
        out_specs=(VMEM, VMEM),
        scratch_shapes=[pltpu.VMEM((LANES, VALUES), f32)],
    )(by_source, by_partner, shares)
    return hessian.transpose(2, 0, 1, 3), gradient


def solution(mesh):
    placed = (
        P("scan", "grp", None, None),
        P("scan"),
        P("scan", "grp"),
        P("scan", "grp"),
        P("scan", "grp", None),
    )
    return jax.shard_map(
        local,
        mesh=mesh,
        in_specs=placed,
        out_specs=(P("scan", None, None, "grp"), P(("scan", "grp"), None)),
        check_vma=False,
    )
```

```python
import functools

import jax
import jax.numpy as jnp
from jax import lax
from jax.experimental import pallas as pl
from jax.experimental.pallas import tpu as pltpu
from jax.sharding import PartitionSpec as P

LANES = 128
VALUES = 32
LEAST_POINTS = 4096
SUMS = VALUES // 8
IDS, VECTOR = 21, 24
PAIRS = [(i, j) for i in range(6) for j in range(i, 6)]
VMEM = pl.BlockSpec(memory_space=pltpu.VMEM)
SMEM = pl.BlockSpec(memory_space=pltpu.SMEM)
ANY = pl.BlockSpec(memory_space=pl.ANY)


def halves(value, size):
    if size & (size - 1):
        return value // size, value % size
    return value >> (size.bit_length() - 1), value & (size - 1)


def lane_take(table, index):
    return jnp.take_along_axis(table, index, axis=1, mode="promise_in_bounds")


def route_kernel(cap, n_grp, scan_local, tiles_local, corr_scan, corr_tile, slots, meta, wide):
    per_scan = corr_scan.shape[1]
    scan_index = lax.axis_index("scan")
    requests = scan_local * per_scan
    chunks, together = requests // LANES, LANES // per_scan
    f32 = jnp.float32

    def flat(ref):
        wide[...] = jnp.zeros_like(wide)
        wide[:, 0:per_scan] = ref[...]
        out = []
        for h in range(chunks):
            moved = pltpu.roll(wide[h * together : (h + 1) * together, :], 0, 1, stride=per_scan, stride_axis=0)
            out.append(row_sum(moved))
        return out

    def column(row):
        return jnp.broadcast_to(row, (LANES, LANES)).T

    scans, tiles = flat(corr_scan), flat(corr_tile)
    sublane = lax.broadcasted_iota(jnp.int32, (LANES, LANES), 0)
    lane = lax.broadcasted_iota(jnp.int32, (LANES, LANES), 1)
    targets, locals_, flats = [], [], []
    for b, t in zip(scans, tiles):
        (b_dev, b_loc), (t_dev, t_loc) = halves(b, scan_local), halves(t, tiles_local)
        targets.append((b_dev * n_grp + t_dev).astype(f32))
        locals_.append(b_loc.astype(f32))
        flats.append((b_loc * tiles_local + t_loc).astype(f32))
    target_columns = [column(x) for x in targets]
    places = []
    for h in range(chunks):
        rank = jnp.zeros((1, LANES), f32)
        for e in range(h + 1):
            same = target_columns[e] == targets[h]
            if e == h:
                same = same & (sublane < lane)
            rank = rank + row_sum(jnp.where(same, 1.0, 0.0))
        places.append(column(targets[h] * cap + rank))
    blank = jnp.zeros((4, LANES), f32)
    one = jnp.ones((1, LANES), f32)
    index = lax.broadcasted_iota(jnp.int32, (1, LANES), 1).astype(f32)
    left = jnp.concatenate(
        [
            jnp.concatenate([one, index + h * LANES, locals_[h], flats[h], blank], axis=0) for h in range(chunks)
        ],
        axis=1,
    ).astype(jnp.bfloat16)
    served = LANES // cap
    for a in range(slots.shape[0]):
        hits = [jnp.where(places[h] == (lane + a * LANES).astype(f32), 1.0, 0.0) for h in range(chunks)]
        table = lax.dot_general(
            left, jnp.concatenate(hits, axis=0).astype(jnp.bfloat16), (((1,), (0,)), ((), ())),
            preferred_element_type=f32,
        ).astype(jnp.int32)
        used, request = table[0:1, :] > 0, table[1:2, :]
        slots[a : a + 1, :] = request
        source = scan_index * scan_local + halves(request, per_scan)[0]
        kinds = [jnp.where(used, table[2:3, :], -1), table[3:4, :], jnp.where(used, source, -1)]
        total = jnp.zeros((served, LANES), jnp.int32)
        part = lax.broadcasted_iota(jnp.int32, (served, LANES), 1) // cap
        for kind, row in enumerate(kinds):
            moved = pltpu.roll(jnp.broadcast_to(row, (served, LANES)), cap, 1, stride=cap, stride_axis=0)
            if kind:
                moved = pltpu.roll(moved, kind * cap, 1)
            total = jnp.where(part == kind, moved, total)
        for i in range(served):
            meta[a * served + i] = total[served - 1 - i : served - i, :]


def greet_all(n_grp, devices, me):
    barrier = pltpu.get_barrier_semaphore()

    def hello(k, _):
        peer = lax.rem(me + k, devices)
        pl.semaphore_signal(
            barrier, inc=1, device_id=(peer // n_grp, peer % n_grp), device_id_type=pl.DeviceIdType.MESH
        )
        return 0

    lax.fori_loop(1, devices, hello, 0)


def await_all(devices):
    pl.semaphore_wait(pltpu.get_barrier_semaphore(), devices - 1)


def remote(src, dst, send, recv, peer, n_grp):
    return pltpu.make_async_remote_copy(
        src_ref=src, dst_ref=dst, send_sem=send, recv_sem=recv,
        device_id=(peer // n_grp, peer % n_grp), device_id_type=pl.DeviceIdType.MESH,
    )


def exclusive(a, b, size):
    if size & (size - 1):
        return lax.rem(a + b, size)
    total = 0
    for bit in range(size.bit_length() - 1):
        total = total + ((((a >> bit) + (b >> bit)) & 1) << bit)
    return total


def split(values):
    high = values.astype(jnp.bfloat16)
    return high, (values - high.astype(jnp.float32)).astype(jnp.bfloat16)


def contract(a, b):
    return lax.dot_general(a, b, (((1,), (1,)), ((), ())), preferred_element_type=jnp.float32)


def row_sum(products):
    return jnp.sum(products, axis=0, keepdims=True)


def wait_for(ref, count, semaphore):
    part = ref.at[pl.ds(0, count)]
    pltpu.make_async_copy(part, part, semaphore).wait()


def compact(sums, place, rows):
    lane = lax.broadcasted_iota(jnp.int32, (8, LANES), 1)
    out = []
    for a in range(SUMS):
        part = sums[a * 8 : (a + 1) * 8, :]
        if place:
            part = pltpu.roll(part, LANES - place * rows, 1)
        part = jnp.where(lane < rows, part, 0.0)
        out.append(row_sum(pltpu.roll(part, 0, 1, stride=rows, stride_axis=0)))
    return out


def exchange_kernel(
    cap, n_grp, samples_hbm, count_hbm, wanted_hbm, slots_hbm, meta, by_source, by_partner, shares, parts,
    samples, count, wanted, slots, picks, data, data_in, meta_in, codes, tiles, comps, turned, ids, result, packed,
    tally, share_out, part_out,
    sent, received, recv_data, own,
):
    scan_local, tiles_local = samples.shape[0], samples.shape[2]
    per_scan = wanted.shape[1]
    n_scan = packed.shape[0]
    devices = n_scan * n_grp
    rows = cap * 4
    width = n_grp * cap
    per_block = LANES // width
    blocks = n_scan // per_block
    sources = per_block * n_grp
    packed_rows = packed.shape[1]
    scan_index, group_index = lax.axis_index("scan"), lax.axis_index("grp")
    me = scan_index * n_grp + group_index
    home, home_row = scan_index // per_block, lax.rem(scan_index, per_block)
    full_groups = min(LEAST_POINTS // (tiles_local * LANES), n_grp) if 3 * cap % 8 == 0 else 0
    short = rows - cap

    def send_one(peer, size):
        return remote(
            data.at[pl.ds(pl.multiple_of(peer * rows, 8), size)],
            data_in.at[pl.ds(pl.multiple_of(me * rows, 8), size)],
            sent.at[0], recv_data.at[home], peer, n_grp,
        )

    def send_code(peer):
        return remote(meta.at[peer], meta_in.at[me], sent.at[1], received.at[1], peer, n_grp)

    def to_source(row, holder):
        peer = row * n_grp + home
        return remote(packed.at[row], by_source.at[holder], sent.at[2], received.at[2], peer, n_grp)

    def to_partner(block):
        peer = scan_index * n_grp + block
        return remote(result.at[block], by_partner.at[group_index], sent.at[3], received.at[3], peer, n_grp)

    def to_share(peer, row, first):
        size = SUMS - first
        return remote(
            share_out.at[pl.ds(row * SUMS + first, size)], shares.at[pl.ds(me * SUMS + first, size)],
            sent.at[4], received.at[4], peer, n_grp,
        )

    def to_part(g, first):
        size = SUMS - first
        return remote(
            part_out.at[pl.ds(first, size)], parts.at[pl.ds(group_index * SUMS + first, size)],
            sent.at[5], received.at[5], scan_index * n_grp + g, n_grp,
        )

    fetch = pltpu.make_async_copy(samples_hbm, samples, own.at[3])
    fetch_count = pltpu.make_async_copy(count_hbm, count, own.at[4])
    fetch_wanted = pltpu.make_async_copy(wanted_hbm, wanted, own.at[0])
    fetch_slots = pltpu.make_async_copy(slots_hbm, slots, own.at[2])
    fetch_count.start()
    fetch_slots.start()
    fetch_wanted.start()
    fetch.start()
    greet_all(n_grp, devices, me)
    fetch_count.wait()
    fetch_wanted.wait()
    fetch.wait()
    pick_rows = picks.reshape(scan_local * per_scan * 8, LANES)
    first_point = group_index * tiles_local * LANES

    def pick(s, _):
        point = wanted[s]
        tile, place = point >> 7, point & (LANES - 1)
        picked = [jnp.zeros((per_scan, LANES), jnp.float32)] * 3
        for t in range(tiles_local):
            hit = tile == t
            for c in range(3):
                row = jnp.broadcast_to(samples[s, c, pl.ds(t, 1), :], (per_scan, LANES))
                picked[c] = jnp.where(hit, lane_take(row, place), picked[c])
        picked.append(jnp.where(first_point + point < count[s], 1.0, 0.0).astype(jnp.float32))
        for c in range(4):
            pick_rows[pl.ds(s * per_scan * 8 + c, per_scan, stride=8), :] = picked[c]
        return 0

    lax.fori_loop(0, scan_local, pick, 0, unroll=2)
    fetch_slots.wait()

    def collect(peer, into):
        first = lax.rem(peer, LANES // cap) * cap
        for j in range(cap):
            request = slots[peer // (LANES // cap), first + j]
            into[pl.ds(peer * rows + j, 4, stride=cap), :] = picks[request, 0:4, :]

    await_all(devices)

    def start_meta(k, _):
        peer = lax.rem(me + k, devices)
        send_code(peer).start()
        return 0

    def start_data(k, _):
        row = exclusive(scan_index, k + 1 - 2 * (k & 1), n_scan)
        for g in reversed(range(n_grp)):
            collect(row * n_grp + exclusive(group_index, g, n_grp), data)
        for g in reversed(range(n_grp)):
            peer = row * n_grp + exclusive(group_index, g, n_grp)

            @pl.when((peer != me) & (group_index < full_groups))
            def _():
                send_one(peer, short).start()

            @pl.when((peer != me) & (group_index >= full_groups))
            def _():
                send_one(peer, rows).start()

        return 0

    lax.fori_loop(1, devices, start_meta, 0)
    lax.fori_loop(0, n_scan, start_data, 0)
    own_meta = pltpu.make_async_copy(meta.at[me], meta_in.at[me], own.at[1])
    own_meta.start()
    collect(me, data_in)
    own_meta.wait()

    def no_mask(row, _):
        for g in range(full_groups):
            first = pl.multiple_of((row * n_grp + g) * rows + short, 8)
            data_in[pl.ds(first, cap), :] = jnp.ones((cap, LANES), jnp.float32)
        return 0

    lax.fori_loop(0, n_scan, no_mask, 0)
    tally[...] = jnp.zeros_like(tally)
    result[...] = jnp.zeros_like(result)

    point = lax.broadcasted_iota(jnp.int32, (tiles_local, LANES), 0) * LANES
    point = point + lax.broadcasted_iota(jnp.int32, (tiles_local, LANES), 1)

    tile_rows = tiles.reshape(scan_local * tiles_local * 8, LANES)

    def fill(b, _):
        valid = point < count[b] - group_index * tiles_local * LANES
        for c in range(6):
            values = samples[b, c]
            if c >= 3:
                values = jnp.where(valid, values, 0.0)
            tile_rows[pl.ds(b * tiles_local * 8 + c, tiles_local, stride=8), :] = values
        return 0

    lax.fori_loop(0, scan_local, fill, 0)
    wait_for(meta_in, devices - 1, received.at[1])
    to_scalar = pltpu.make_async_copy(meta_in, codes, own.at[2])
    to_scalar.start()

    slot_lane = lax.broadcasted_iota(jnp.int32, (sources, LANES), 1) // cap
    slot_row = lax.broadcasted_iota(jnp.int32, (sources, LANES), 0)

    def decode(m, _):
        arrived = meta_in[pl.ds(m * sources, sources), 0, :]
        kinds = []
        for kind in (0, 2):
            moved = pltpu.roll(arrived, LANES - kind * cap, 1) if kind else arrived
            moved = pltpu.roll(moved, 0, 1, stride=cap, stride_axis=0)
            kinds.append(row_sum(jnp.where(slot_lane == slot_row, moved, 0)))
        partner, source = kinds
        ids[m, 0:1, :] = source.astype(jnp.float32)
        ids[m, 1:2, :] = jnp.where(partner < 0, -1, scan_index * scan_local + partner).astype(jnp.float32)
        return 0

    lax.fori_loop(0, blocks, decode, 0)
    to_scalar.wait()

    def one_block(k, _):
        m = exclusive(home, k, blocks)

        def gather(i, _):
            for j in range(cap):
                slot = i * cap + j
                row = codes[m * sources + i, 0, cap + j]
                comps[pl.ds(pl.multiple_of(slot * 8, 8), 8), :] = tiles[row]
            return 0

        lax.fori_loop(0, sources, gather, 0)
        for c in range(6):
            turned[4 + c] = comps[pl.ds(c, LANES, stride=8), :].T

        whole = per_block * (n_grp * rows - full_groups * cap)

        @pl.when(m != home)
        def _():
            wait_for(data_in, whole, recv_data.at[m])

        @pl.when((m == home) & (group_index < full_groups))
        def _():
            wait_for(data_in, whole - short, recv_data.at[m])

        @pl.when((m == home) & (group_index >= full_groups))
        def _():
            wait_for(data_in, whole - rows, recv_data.at[m])

        for c in range(4):
            pieces = [
                data_in[pl.ds((m * sources + i) * rows + c * cap, cap), :] for i in range(sources)
            ]
            turned[c] = jnp.concatenate(pieces, axis=0).T

        def step(kk, sums):
            at = pl.ds(pl.multiple_of(kk * 8, 8), 8)
            px, py, pz, mask, qx, qy, qz, nx, ny, nz = [turned[c, at, :] for c in range(10)]
            residual = nx * (px - qx) + ny * (py - qy) + nz * (pz - qz)
            weight = mask / (1.0 + residual * residual)
            jac = [py * nz - pz * ny, pz * nx - px * nz, px * ny - py * nx, nx, ny, nz]
            scaled = [weight * x for x in jac]
            products = [scaled[a] * jac[b] for a, b in PAIRS] + [x * residual for x in scaled]
            return tuple(s + p for s, p in zip(sums, products))

        zero = jnp.zeros((8, LANES), jnp.float32)
        sums = lax.fori_loop(0, LANES // 8, step, (zero,) * (len(PAIRS) + 6))
        for q, total in enumerate(sums):
            q = q if q < len(PAIRS) else q - len(PAIRS) + VECTOR
            result[m, q : q + 1, :] = row_sum(total)
        result[m, IDS : IDS + 2, :] = ids[m, 0:2, :]
        values = result[m]
        lane = lax.broadcasted_iota(jnp.int32, (packed_rows, LANES), 1) // width
        chunks = [values[g * packed_rows : (g + 1) * packed_rows, :] for g in range(per_block)]
        for p in range(per_block):
            total = chunks[p]
            for g in range(per_block):
                if g != p:
                    total = jnp.where(lane == g, pltpu.roll(chunks[g], (g - p) * width % LANES, 1), total)
            row = m * per_block + p
            packed[row] = total
            holder = group_index * per_block + home_row

            @pl.when(row * n_grp + home == me)
            def _():
                pltpu.make_async_copy(packed.at[row], by_source.at[holder], own.at[3]).start()

            @pl.when(row * n_grp + home != me)
            def _():
                to_source(row, holder).start()

        @pl.when(m == group_index)
        def _():
            pltpu.make_async_copy(result.at[group_index], by_partner.at[group_index], own.at[4]).start()

        @pl.when(m != group_index)
        def _():
            to_partner(m).start()

        high, low = split(values)
        source = ids[m, 0:1, :].astype(jnp.int32) - m * per_block * scan_local
        partner = ids[m, 1:2, :].astype(jnp.int32) - scan_index * scan_local
        span = lax.broadcasted_iota(jnp.int32, (LANES, LANES), 0)
        chosen = jnp.where(span == source, 1.0, 0.0).astype(jnp.bfloat16)
        sums = contract(high, chosen) + contract(low, chosen)
        chosen = jnp.where(span == partner, 1.0, 0.0).astype(jnp.bfloat16)
        tally[...] += contract(high, chosen) + contract(low, chosen)
        for p in range(per_block):
            row = m * per_block + p
            for a, line in enumerate(compact(sums, p, scan_local)):
                share_out[row * SUMS + a] = line
            for g in range(n_grp):
                peer = row * n_grp + g

                @pl.when((peer != me) & (m == g))
                def _():
                    to_share(peer, row, 0).start()

                @pl.when((peer != me) & (m != g))
                def _():
                    to_share(peer, row, SUMS - 1).start()

        return 0

    lax.fori_loop(0, blocks, one_block, 0)
    for a, line in enumerate(compact(tally[...], 0, scan_local)):
        part_out[a] = line
    own_share = pltpu.make_async_copy(
        share_out.at[pl.ds(scan_index * SUMS, SUMS)], shares.at[pl.ds(me * SUMS, SUMS)], own.at[0]
    )
    own_part = pltpu.make_async_copy(part_out, parts.at[pl.ds(group_index * SUMS, SUMS)], own.at[1])
    own_share.start()
    own_part.start()
    for g in range(n_grp):

        @pl.when((g != group_index) & (home == g))
        def _():
            to_part(g, 0).start()

        @pl.when((g != group_index) & (home != g))
        def _():
            to_part(g, SUMS - 1).start()

    others = n_grp - 1
    wait_for(by_partner, others, received.at[3])
    wait_for(result, others, sent.at[3])
    wait_for(meta_in, devices - 1, sent.at[1])

    @pl.when(home == group_index)
    def _():
        pltpu.make_async_copy(packed.at[0], by_source.at[0], own.at[3]).wait()
        wait_for(by_source, sources - 1, received.at[2])
        wait_for(packed, n_scan - 1, sent.at[2])
        wait_for(shares, (devices - 1) * SUMS, received.at[4])
        wait_for(shares, n_scan * (SUMS + others) - SUMS, sent.at[4])
        wait_for(parts, others * SUMS, received.at[5])
        wait_for(parts, others, sent.at[5])

    @pl.when(home != group_index)
    def _():
        wait_for(by_source, sources, received.at[2])
        wait_for(packed, n_scan, sent.at[2])
        wait_for(shares, devices - 1, received.at[4])
        wait_for(shares, n_scan * (SUMS + others) - 1, sent.at[4])
        wait_for(parts, others, received.at[5])
        wait_for(parts, others - 1 + SUMS, sent.at[5])

    pltpu.make_async_copy(result.at[0], by_partner.at[group_index], own.at[4]).wait()
    own_share.wait()
    own_part.wait()

    @pl.when(group_index < full_groups)
    def _():
        wait_for(data, (devices - 1) * short, sent.at[0])

    @pl.when(group_index >= full_groups)
    def _():
        wait_for(data, (devices - 1) * rows, sent.at[0])


def regroup(parts, width):
    groups = len(parts)
    lane = lax.broadcasted_iota(jnp.int32, parts[0].shape, 1) // width
    out = []
    for b in range(groups):
        total = parts[b]
        for g in range(groups):
            if g != b:
                total = jnp.where(lane == g, pltpu.roll(parts[g], (g - b) * width % LANES, 1), total)
        out.append(total)
    return out


def assemble_kernel(n_grp, width, by_source, by_partner, shares, parts, hessian, gradient, spare):
    rows, columns = hessian.shape[2], hessian.shape[3]
    grad_rows = gradient.shape[0]
    per_block = LANES // width
    scan_index, group_index = lax.axis_index("scan"), lax.axis_index("grp")
    home, home_row = scan_index // per_block, lax.rem(scan_index, per_block)
    first_row, first_column = scan_index * rows, group_index * columns
    count = len(PAIRS)

    def total_of(ref):
        total = ref[0:SUMS, 0, :]
        for d in range(1, ref.shape[0] // SUMS):
            total = total + ref[d * SUMS : (d + 1) * SUMS, 0, :]
        return total

    def spread(line):
        return pltpu.roll(jnp.broadcast_to(line, (8, LANES)), rows, 1, stride=rows, stride_axis=0)

    outgoing, incoming = total_of(shares), total_of(parts)
    vector = spread(outgoing[SUMS - 1 :, :] - incoming[SUMS - 1 :, :])
    spare[...] = jnp.concatenate([vector[7 - i : 8 - i, :] for i in range(8)], axis=0).T
    gradient[...] = spare[pl.ds(group_index * grad_rows, grad_rows), 0:6]
    both = [spread(outgoing[a : a + 1, :] + incoming[a : a + 1, :]) for a in range(SUMS - 1)]
    lines = [both[q // 8][7 - q % 8 : 8 - q % 8, :] for q in range(count)]

    pieces = []
    for g in range(n_grp):
        halves_ = [by_source[g * per_block + p] for p in range(per_block)]
        block = jnp.concatenate(regroup(halves_, width), axis=0)
        source, partner = [block[r : r + 1, :].astype(jnp.int32) for r in (IDS, IDS + 1)]
        pieces.append((block, source - first_row, partner - first_column))
    for g in range(n_grp):
        block = by_partner[g]
        source, partner = [block[r : r + 1, :].astype(jnp.int32) for r in (IDS, IDS + 1)]
        pieces.append((block, partner - first_row, source - first_column))
    pieces = [([block[q : q + 1, :] for q in range(count)], at, to) for block, at, to in pieces]
    lane = lax.broadcasted_iota(jnp.int32, (1, LANES), 1)
    diagonal = jnp.where((lane < rows) & (group_index == home), lane, -1)
    pieces.append((lines, diagonal, jnp.where(diagonal < 0, -1, lane + home_row * rows)))

    left, right = [], []
    row = lax.broadcasted_iota(jnp.int32, (rows, LANES), 0)
    column = lax.broadcasted_iota(jnp.int32, (columns, LANES), 0)
    for index, (block, at, to) in enumerate(pieces):
        hit = row == at
        left.append(jnp.concatenate([jnp.where(hit, block[q], 0.0) for q in range(count)], axis=0))
        right.append(jnp.where(column == to, 1.0 if index == 2 * n_grp else -1.0, 0.0))
    matrix = jnp.concatenate(right, axis=1).astype(jnp.bfloat16)
    high, low = split(jnp.concatenate(left, axis=1))
    total = contract(high, matrix) + contract(low, matrix)
    where = {pair: q for q, pair in enumerate(PAIRS)}
    for i in range(6):
        for j in range(6):
            q = where[min(i, j), max(i, j)]
            hessian[i, j] = total[q * rows : (q + 1) * rows, :]


def local(samples, point_count, corr_scan, corr_tile, corr_src):
    f32, i32 = jnp.float32, jnp.int32
    scan_local, tiles_local = samples.shape[0], samples.shape[1]
    request_count = scan_local * corr_scan.shape[1]
    n_scan, n_grp = lax.axis_size("scan"), lax.axis_size("grp")
    devices = n_scan * n_grp
    cap = 2 * request_count // devices
    width = n_grp * cap
    packed_rows = VALUES * width // LANES
    per_block = LANES // width
    blocks = n_scan // per_block
    columns = scan_local * n_scan // n_grp
    grad_rows = scan_local // n_grp
    assert blocks == n_grp and blocks * per_block == n_scan and 8 * scan_local == LANES
    shape = jax.ShapeDtypeStruct
    dma = pltpu.SemaphoreType.DMA

    tiles = samples.transpose(0, 2, 1, 3)
    per_scan = corr_scan.shape[1]
    assert request_count <= 256 and scan_local * tiles_local <= 256
    slots, meta = pl.pallas_call(
        functools.partial(route_kernel, cap, n_grp, scan_local, tiles_local),
        out_shape=(shape((devices * cap // LANES, LANES), i32), shape((devices, 1, LANES), i32)),
        in_specs=[VMEM, VMEM],
        out_specs=(VMEM, VMEM),
        scratch_shapes=[pltpu.VMEM((scan_local, LANES), i32)],
    )(corr_scan, corr_tile)

    by_source, by_partner, shares, parts = pl.pallas_call(
        functools.partial(exchange_kernel, cap, n_grp),
        out_shape=(
            shape((n_grp * per_block, packed_rows, LANES), f32),
            shape((n_grp, VALUES, LANES), f32),
            shape((devices * SUMS, 1, LANES), f32),
            shape((n_grp * SUMS, 1, LANES), f32),
        ),
        in_specs=[ANY] * 5,
        out_specs=(ANY,) * 4,
        scratch_shapes=[
            pltpu.VMEM(tiles.shape, f32),
            pltpu.SMEM(point_count.shape, i32),
            pltpu.VMEM(corr_src.shape, i32),
            pltpu.SMEM(slots.shape, i32),
            pltpu.VMEM((request_count, 8, LANES), f32),
            pltpu.VMEM((devices * cap * 4, LANES), f32),
            pltpu.VMEM((devices * cap * 4, LANES), f32),
            pltpu.VMEM(meta.shape, i32),
            pltpu.SMEM(meta.shape, i32),
            pltpu.VMEM((scan_local * tiles_local, 8, LANES), f32),
            pltpu.VMEM((LANES * 8, LANES), f32),
            pltpu.VMEM((10, LANES, LANES), f32),
            pltpu.VMEM((blocks, 8, LANES), f32),
            pltpu.VMEM((blocks, VALUES, LANES), f32),
            pltpu.VMEM((n_scan, packed_rows, LANES), f32),
            pltpu.VMEM((VALUES, LANES), f32),
            pltpu.VMEM((n_scan * SUMS, 1, LANES), f32),
            pltpu.VMEM((SUMS, 1, LANES), f32),
        ]
        + [dma((6,)), dma((6,)), dma((blocks,)), dma((5,))],
        compiler_params=pltpu.CompilerParams(collective_id=0, has_side_effects=True),
    )(tiles, point_count, corr_src, slots, meta)

    hessian, gradient = pl.pallas_call(
        functools.partial(assemble_kernel, n_grp, width),
        out_shape=(shape((6, 6, scan_local, columns), f32), shape((grad_rows, 6), f32)),
        in_specs=[VMEM] * 4,
        out_specs=(VMEM, VMEM),
        scratch_shapes=[pltpu.VMEM((LANES, 8), f32)],
    )(by_source, by_partner, shares, parts)
    return hessian.transpose(2, 0, 1, 3), gradient


def solution(mesh):
    placed = (
        P("scan", "grp", None, None),
        P("scan"),
        P("scan", "grp"),
        P("scan", "grp"),
        P("scan", "grp", None),
    )
    return jax.shard_map(
        local,
        mesh=mesh,
        in_specs=placed,
        out_specs=(P("scan", None, None, "grp"), P(("scan", "grp"), None)),
        check_vma=False,
    )
```

```python
import functools

import jax
import jax.numpy as jnp
from jax import lax
from jax.experimental import pallas as pl
from jax.experimental.pallas import tpu as pltpu
from jax.sharding import PartitionSpec as P

LANES = 128
VALUES = 32
LEAST_POINTS = 4096
SUMS = VALUES // 8
IDS, VECTOR = 21, 24
PAIRS = [(i, j) for i in range(6) for j in range(i, 6)]
VMEM = pl.BlockSpec(memory_space=pltpu.VMEM)
SMEM = pl.BlockSpec(memory_space=pltpu.SMEM)
ANY = pl.BlockSpec(memory_space=pl.ANY)


def halves(value, size):
    if size & (size - 1):
        return value // size, value % size
    return value >> (size.bit_length() - 1), value & (size - 1)


def lane_take(table, index):
    return jnp.take_along_axis(table, index, axis=1, mode="promise_in_bounds")


def route_kernel(cap, n_grp, scan_local, tiles_local, corr_scan, corr_tile, slots, meta, wide):
    per_scan = corr_scan.shape[1]
    scan_index = lax.axis_index("scan")
    requests = scan_local * per_scan
    chunks, together = requests // LANES, LANES // per_scan
    f32 = jnp.float32

    def flat(ref):
        wide[...] = jnp.zeros_like(wide)
        wide[:, 0:per_scan] = ref[...]
        out = []
        for h in range(chunks):
            moved = pltpu.roll(wide[h * together : (h + 1) * together, :], 0, 1, stride=per_scan, stride_axis=0)
            out.append(row_sum(moved))
        return out

    def column(row):
        return jnp.broadcast_to(row, (LANES, LANES)).T

    scans, tiles = flat(corr_scan), flat(corr_tile)
    sublane = lax.broadcasted_iota(jnp.int32, (LANES, LANES), 0)
    lane = lax.broadcasted_iota(jnp.int32, (LANES, LANES), 1)
    targets, locals_, flats = [], [], []
    for b, t in zip(scans, tiles):
        (b_dev, b_loc), (t_dev, t_loc) = halves(b, scan_local), halves(t, tiles_local)
        targets.append((b_dev * n_grp + t_dev).astype(f32))
        locals_.append(b_loc.astype(f32))
        flats.append((b_loc * tiles_local + t_loc).astype(f32))
    target_columns = [column(x) for x in targets]
    places = []
    for h in range(chunks):
        rank = jnp.zeros((1, LANES), f32)
        for e in range(h + 1):
            same = target_columns[e] == targets[h]
            if e == h:
                same = same & (sublane < lane)
            rank = rank + row_sum(jnp.where(same, 1.0, 0.0))
        places.append(column(targets[h] * cap + rank))
    blank = jnp.zeros((4, LANES), f32)
    one = jnp.ones((1, LANES), f32)
    index = lax.broadcasted_iota(jnp.int32, (1, LANES), 1).astype(f32)
    left = jnp.concatenate(
        [
            jnp.concatenate([one, index + h * LANES, locals_[h], flats[h], blank], axis=0) for h in range(chunks)
        ],
        axis=1,
    ).astype(jnp.bfloat16)
    served = LANES // cap
    for a in range(slots.shape[0]):
        hits = [jnp.where(places[h] == (lane + a * LANES).astype(f32), 1.0, 0.0) for h in range(chunks)]
        table = lax.dot_general(
            left, jnp.concatenate(hits, axis=0).astype(jnp.bfloat16), (((1,), (0,)), ((), ())),
            preferred_element_type=f32,
        ).astype(jnp.int32)
        used, request = table[0:1, :] > 0, table[1:2, :]
        slots[a : a + 1, :] = request
        source = scan_index * scan_local + halves(request, per_scan)[0]
        kinds = [jnp.where(used, table[2:3, :], -1), table[3:4, :], jnp.where(used, source, -1)]
        total = jnp.zeros((served, LANES), jnp.int32)
        part = lax.broadcasted_iota(jnp.int32, (served, LANES), 1) // cap
        for kind, row in enumerate(kinds):
            moved = pltpu.roll(jnp.broadcast_to(row, (served, LANES)), cap, 1, stride=cap, stride_axis=0)
            if kind:
                moved = pltpu.roll(moved, kind * cap, 1)
            total = jnp.where(part == kind, moved, total)
        for i in range(served):
            meta[a * served + i] = total[served - 1 - i : served - i, :]


def greet_all(n_grp, devices, me):
    barrier = pltpu.get_barrier_semaphore()

    def hello(k, _):
        peer = lax.rem(me + k, devices)
        pl.semaphore_signal(
            barrier, inc=1, device_id=(peer // n_grp, peer % n_grp), device_id_type=pl.DeviceIdType.MESH
        )
        return 0

    lax.fori_loop(1, devices, hello, 0)


def await_all(devices):
    pl.semaphore_wait(pltpu.get_barrier_semaphore(), devices - 1)


def remote(src, dst, send, recv, peer, n_grp):
    return pltpu.make_async_remote_copy(
        src_ref=src, dst_ref=dst, send_sem=send, recv_sem=recv,
        device_id=(peer // n_grp, peer % n_grp), device_id_type=pl.DeviceIdType.MESH,
    )


def exclusive(a, b, size):
    if size & (size - 1):
        return lax.rem(a + b, size)
    total = 0
    for bit in range(size.bit_length() - 1):
        total = total + ((((a >> bit) + (b >> bit)) & 1) << bit)
    return total


def split(values):
    high = values.astype(jnp.bfloat16)
    return high, (values - high.astype(jnp.float32)).astype(jnp.bfloat16)


def contract(a, b):
    return lax.dot_general(a, b, (((1,), (1,)), ((), ())), preferred_element_type=jnp.float32)


def row_sum(products):
    return jnp.sum(products, axis=0, keepdims=True)


def wait_for(ref, count, semaphore):
    part = ref.at[pl.ds(0, count)]
    pltpu.make_async_copy(part, part, semaphore).wait()


def compact(sums, place, rows):
    lane = lax.broadcasted_iota(jnp.int32, (8, LANES), 1)
    out = []
    for a in range(SUMS):
        part = sums[a * 8 : (a + 1) * 8, :]
        if place:
            part = pltpu.roll(part, LANES - place * rows, 1)
        part = jnp.where(lane < rows, part, 0.0)
        out.append(row_sum(pltpu.roll(part, 0, 1, stride=rows, stride_axis=0)))
    return out


def exchange_kernel(
    cap, n_grp, samples_hbm, count_hbm, wanted_hbm, slots_hbm, meta, by_source, by_partner, shares, parts,
    samples, count, wanted, slots, data, data_in, meta_in, codes, tiles, comps, turned, ids, result, packed,
    tally, share_out, part_out,
    sent, received, recv_data, own,
):
    scan_local, tiles_local = samples.shape[0], samples.shape[2]
    per_scan = wanted.shape[1]
    n_scan = packed.shape[0]
    devices = n_scan * n_grp
    rows = cap * 4
    width = n_grp * cap
    per_block = LANES // width
    blocks = n_scan // per_block
    sources = per_block * n_grp
    packed_rows = packed.shape[1]
    scan_index, group_index = lax.axis_index("scan"), lax.axis_index("grp")
    me = scan_index * n_grp + group_index
    home, home_row = scan_index // per_block, lax.rem(scan_index, per_block)
    full_groups = min(LEAST_POINTS // (tiles_local * LANES), n_grp) if 3 * cap % 8 == 0 else 0
    short = rows - cap

    def send_one(peer, size):
        return remote(
            data.at[pl.ds(pl.multiple_of(peer * rows, 8), size)],
            data_in.at[pl.ds(pl.multiple_of(me * rows, 8), size)],
            sent.at[0], recv_data.at[home], peer, n_grp,
        )

    def send_code(peer):
        return remote(meta.at[peer], meta_in.at[me], sent.at[1], received.at[1], peer, n_grp)

    def to_source(row, holder):
        peer = row * n_grp + home
        return remote(packed.at[row], by_source.at[holder], sent.at[2], received.at[2], peer, n_grp)

    def to_partner(block):
        peer = scan_index * n_grp + block
        return remote(result.at[block], by_partner.at[group_index], sent.at[3], received.at[3], peer, n_grp)

    def to_share(peer, row, first):
        size = SUMS - first
        return remote(
            share_out.at[pl.ds(row * SUMS + first, size)], shares.at[pl.ds(me * SUMS + first, size)],
            sent.at[4], received.at[4], peer, n_grp,
        )

    def to_part(g, first):
        size = SUMS - first
        return remote(
            part_out.at[pl.ds(first, size)], parts.at[pl.ds(group_index * SUMS + first, size)],
            sent.at[5], received.at[5], scan_index * n_grp + g, n_grp,
        )

    fetch = pltpu.make_async_copy(samples_hbm, samples, own.at[3])
    fetch_count = pltpu.make_async_copy(count_hbm, count, own.at[4])
    fetch_wanted = pltpu.make_async_copy(wanted_hbm, wanted, own.at[0])
    fetch_slots = pltpu.make_async_copy(slots_hbm, slots, own.at[2])
    fetch_count.start()
    fetch_slots.start()
    fetch_wanted.start()
    fetch.start()
    greet_all(n_grp, devices, me)
    fetch_count.wait()
    fetch_wanted.wait()
    fetch.wait()
    fetch_slots.wait()
    first_point = group_index * tiles_local * LANES
    wanted_rows = wanted.reshape(scan_local * per_scan, LANES)
    tile_row = lax.broadcasted_iota(jnp.int32, (tiles_local, LANES), 0)

    def collect(peer, into):
        first = lax.rem(peer, LANES // cap) * cap
        for j in range(cap):
            request = slots[peer // (LANES // cap), first + j]
            s = halves(request, per_scan)[0]
            point = wanted_rows[pl.ds(request, 1), :]
            spread = jnp.broadcast_to(point, (tiles_local, LANES))
            hit, place = spread >> 7 == tile_row, spread & (LANES - 1)
            for c in range(3):
                found = jnp.where(hit, lane_take(samples[s, c], place), 0.0)
                into[pl.ds(peer * rows + c * cap + j, 1), :] = row_sum(found)
            mask = jnp.where(first_point + point < count[s], 1.0, 0.0).astype(jnp.float32)
            into[pl.ds(peer * rows + 3 * cap + j, 1), :] = mask

    await_all(devices)

    def start_meta(k, _):
        peer = lax.rem(me + k, devices)
        send_code(peer).start()
        return 0

    def start_data(k, _):
        peer = exclusive(me, k, devices)
        collect(peer, data)

        @pl.when((peer != me) & (group_index < full_groups))
        def _():
            send_one(peer, short).start()

        @pl.when((peer != me) & (group_index >= full_groups))
        def _():
            send_one(peer, rows).start()

        return 0

    lax.fori_loop(1, devices, start_meta, 0)
    share = devices // 4
    for quarter in (2, 1, 3, 0):
        lax.fori_loop(quarter * share, (quarter + 1) * share, start_data, 0)
    own_meta = pltpu.make_async_copy(meta.at[me], meta_in.at[me], own.at[1])
    own_meta.start()
    collect(me, data_in)
    own_meta.wait()

    def no_mask(row, _):
        for g in range(full_groups):
            first = pl.multiple_of((row * n_grp + g) * rows + short, 8)
            data_in[pl.ds(first, cap), :] = jnp.ones((cap, LANES), jnp.float32)
        return 0

    lax.fori_loop(0, n_scan, no_mask, 0)
    tally[...] = jnp.zeros_like(tally)
    result[...] = jnp.zeros_like(result)

    point = lax.broadcasted_iota(jnp.int32, (tiles_local, LANES), 0) * LANES
    point = point + lax.broadcasted_iota(jnp.int32, (tiles_local, LANES), 1)

    tile_rows = tiles.reshape(scan_local * tiles_local * 8, LANES)

    def fill(b, _):
        valid = point < count[b] - group_index * tiles_local * LANES
        for c in range(6):
            values = samples[b, c]
            if c >= 3:
                values = jnp.where(valid, values, 0.0)
            tile_rows[pl.ds(b * tiles_local * 8 + c, tiles_local, stride=8), :] = values
        return 0

    lax.fori_loop(0, scan_local, fill, 0)
    wait_for(meta_in, devices - 1, received.at[1])
    to_scalar = pltpu.make_async_copy(meta_in, codes, own.at[2])
    to_scalar.start()

    slot_lane = lax.broadcasted_iota(jnp.int32, (sources, LANES), 1) // cap
    slot_row = lax.broadcasted_iota(jnp.int32, (sources, LANES), 0)

    def decode(m, _):
        arrived = meta_in[pl.ds(m * sources, sources), 0, :]
        kinds = []
        for kind in (0, 2):
            moved = pltpu.roll(arrived, LANES - kind * cap, 1) if kind else arrived
            moved = pltpu.roll(moved, 0, 1, stride=cap, stride_axis=0)
            kinds.append(row_sum(jnp.where(slot_lane == slot_row, moved, 0)))
        partner, source = kinds
        ids[m, 0:1, :] = source.astype(jnp.float32)
        ids[m, 1:2, :] = jnp.where(partner < 0, -1, scan_index * scan_local + partner).astype(jnp.float32)
        return 0

    lax.fori_loop(0, blocks, decode, 0)
    to_scalar.wait()

    def one_block(k, _):
        m = exclusive(home, k, blocks)

        def gather(i, _):
            for j in range(cap):
                slot = i * cap + j
                row = codes[m * sources + i, 0, cap + j]
                comps[pl.ds(pl.multiple_of(slot * 8, 8), 8), :] = tiles[row]
            return 0

        lax.fori_loop(0, sources, gather, 0)
        for c in range(6):
            turned[4 + c] = comps[pl.ds(c, LANES, stride=8), :].T

        whole = per_block * (n_grp * rows - full_groups * cap)

        @pl.when(m != home)
        def _():
            wait_for(data_in, whole, recv_data.at[m])

        @pl.when((m == home) & (group_index < full_groups))
        def _():
            wait_for(data_in, whole - short, recv_data.at[m])

        @pl.when((m == home) & (group_index >= full_groups))
        def _():
            wait_for(data_in, whole - rows, recv_data.at[m])

        for c in range(4):
            pieces = [
                data_in[pl.ds((m * sources + i) * rows + c * cap, cap), :] for i in range(sources)
            ]
            turned[c] = jnp.concatenate(pieces, axis=0).T

        def step(kk, sums):
            at = pl.ds(pl.multiple_of(kk * 8, 8), 8)
            px, py, pz, mask, qx, qy, qz, nx, ny, nz = [turned[c, at, :] for c in range(10)]
            residual = nx * (px - qx) + ny * (py - qy) + nz * (pz - qz)
            weight = mask / (1.0 + residual * residual)
            jac = [py * nz - pz * ny, pz * nx - px * nz, px * ny - py * nx, nx, ny, nz]
            scaled = [weight * x for x in jac]
            products = [scaled[a] * jac[b] for a, b in PAIRS] + [x * residual for x in scaled]
            return tuple(s + p for s, p in zip(sums, products))

        zero = jnp.zeros((8, LANES), jnp.float32)
        sums = lax.fori_loop(0, LANES // 8, step, (zero,) * (len(PAIRS) + 6), unroll=True)
        for q, total in enumerate(sums):
            q = q if q < len(PAIRS) else q - len(PAIRS) + VECTOR
            result[m, q : q + 1, :] = row_sum(total)
        result[m, IDS : IDS + 2, :] = ids[m, 0:2, :]
        values = result[m]
        lane = lax.broadcasted_iota(jnp.int32, (packed_rows, LANES), 1) // width
        chunks = [values[g * packed_rows : (g + 1) * packed_rows, :] for g in range(per_block)]
        for p in range(per_block):
            total = chunks[p]
            for g in range(per_block):
                if g != p:
                    total = jnp.where(lane == g, pltpu.roll(chunks[g], (g - p) * width % LANES, 1), total)
            row = m * per_block + p
            packed[row] = total
            holder = group_index * per_block + home_row

            @pl.when(row * n_grp + home == me)
            def _():
                pltpu.make_async_copy(packed.at[row], by_source.at[holder], own.at[3]).start()

            @pl.when(row * n_grp + home != me)
            def _():
                to_source(row, holder).start()

        @pl.when(m == group_index)
        def _():
            pltpu.make_async_copy(result.at[group_index], by_partner.at[group_index], own.at[4]).start()

        @pl.when(m != group_index)
        def _():
            to_partner(m).start()

        high, low = split(values)
        source = ids[m, 0:1, :].astype(jnp.int32) - m * per_block * scan_local
        partner = ids[m, 1:2, :].astype(jnp.int32) - scan_index * scan_local
        span = lax.broadcasted_iota(jnp.int32, (LANES, LANES), 0)
        chosen = jnp.where(span == source, 1.0, 0.0).astype(jnp.bfloat16)
        sums = contract(high, chosen) + contract(low, chosen)
        chosen = jnp.where(span == partner, 1.0, 0.0).astype(jnp.bfloat16)
        tally[...] += contract(high, chosen) + contract(low, chosen)
        for p in range(per_block):
            row = m * per_block + p
            for a, line in enumerate(compact(sums, p, scan_local)):
                share_out[row * SUMS + a] = line
            for g in range(n_grp):
                peer = row * n_grp + g

                @pl.when((peer != me) & (m == g))
                def _():
                    to_share(peer, row, 0).start()

                @pl.when((peer != me) & (m != g))
                def _():
                    to_share(peer, row, SUMS - 1).start()

        return 0

    lax.fori_loop(0, blocks, one_block, 0)
    for a, line in enumerate(compact(tally[...], 0, scan_local)):
        part_out[a] = line
    own_share = pltpu.make_async_copy(
        share_out.at[pl.ds(scan_index * SUMS, SUMS)], shares.at[pl.ds(me * SUMS, SUMS)], own.at[0]
    )
    own_part = pltpu.make_async_copy(part_out, parts.at[pl.ds(group_index * SUMS, SUMS)], own.at[1])
    own_share.start()
    own_part.start()
    for g in range(n_grp):

        @pl.when((g != group_index) & (home == g))
        def _():
            to_part(g, 0).start()

        @pl.when((g != group_index) & (home != g))
        def _():
            to_part(g, SUMS - 1).start()

    others = n_grp - 1
    wait_for(by_partner, others, received.at[3])
    wait_for(result, others, sent.at[3])
    wait_for(meta_in, devices - 1, sent.at[1])

    @pl.when(home == group_index)
    def _():
        pltpu.make_async_copy(packed.at[0], by_source.at[0], own.at[3]).wait()
        wait_for(by_source, sources - 1, received.at[2])
        wait_for(packed, n_scan - 1, sent.at[2])
        wait_for(shares, (devices - 1) * SUMS, received.at[4])
        wait_for(shares, n_scan * (SUMS + others) - SUMS, sent.at[4])
        wait_for(parts, others * SUMS, received.at[5])
        wait_for(parts, others, sent.at[5])

    @pl.when(home != group_index)
    def _():
        wait_for(by_source, sources, received.at[2])
        wait_for(packed, n_scan, sent.at[2])
        wait_for(shares, devices - 1, received.at[4])
        wait_for(shares, n_scan * (SUMS + others) - 1, sent.at[4])
        wait_for(parts, others, received.at[5])
        wait_for(parts, others - 1 + SUMS, sent.at[5])

    pltpu.make_async_copy(result.at[0], by_partner.at[group_index], own.at[4]).wait()
    own_share.wait()
    own_part.wait()

    @pl.when(group_index < full_groups)
    def _():
        wait_for(data, (devices - 1) * short, sent.at[0])

    @pl.when(group_index >= full_groups)
    def _():
        wait_for(data, (devices - 1) * rows, sent.at[0])


def regroup(parts, width):
    groups = len(parts)
    lane = lax.broadcasted_iota(jnp.int32, parts[0].shape, 1) // width
    out = []
    for b in range(groups):
        total = parts[b]
        for g in range(groups):
            if g != b:
                total = jnp.where(lane == g, pltpu.roll(parts[g], (g - b) * width % LANES, 1), total)
        out.append(total)
    return out


def assemble_kernel(n_grp, width, by_source, by_partner, shares, parts, hessian, gradient, spare):
    rows, columns = hessian.shape[2], hessian.shape[3]
    grad_rows = gradient.shape[0]
    per_block = LANES // width
    scan_index, group_index = lax.axis_index("scan"), lax.axis_index("grp")
    home, home_row = scan_index // per_block, lax.rem(scan_index, per_block)
    first_row, first_column = scan_index * rows, group_index * columns
    count = len(PAIRS)

    def total_of(ref):
        total = ref[0:SUMS, 0, :]
        for d in range(1, ref.shape[0] // SUMS):
            total = total + ref[d * SUMS : (d + 1) * SUMS, 0, :]
        return total

    def spread(line):
        return pltpu.roll(jnp.broadcast_to(line, (8, LANES)), rows, 1, stride=rows, stride_axis=0)

    outgoing, incoming = total_of(shares), total_of(parts)
    vector = spread(outgoing[SUMS - 1 :, :] - incoming[SUMS - 1 :, :])
    spare[...] = jnp.concatenate([vector[7 - i : 8 - i, :] for i in range(8)], axis=0).T
    gradient[...] = spare[pl.ds(group_index * grad_rows, grad_rows), 0:6]
    both = [spread(outgoing[a : a + 1, :] + incoming[a : a + 1, :]) for a in range(SUMS - 1)]
    lines = [both[q // 8][7 - q % 8 : 8 - q % 8, :] for q in range(count)]

    pieces = []
    for g in range(n_grp):
        halves_ = [by_source[g * per_block + p] for p in range(per_block)]
        block = jnp.concatenate(regroup(halves_, width), axis=0)
        source, partner = [block[r : r + 1, :].astype(jnp.int32) for r in (IDS, IDS + 1)]
        pieces.append((block, source - first_row, partner - first_column))
    for g in range(n_grp):
        block = by_partner[g]
        source, partner = [block[r : r + 1, :].astype(jnp.int32) for r in (IDS, IDS + 1)]
        pieces.append((block, partner - first_row, source - first_column))
    pieces = [([block[q : q + 1, :] for q in range(count)], at, to) for block, at, to in pieces]
    lane = lax.broadcasted_iota(jnp.int32, (1, LANES), 1)
    diagonal = jnp.where((lane < rows) & (group_index == home), lane, -1)
    pieces.append((lines, diagonal, jnp.where(diagonal < 0, -1, lane + home_row * rows)))

    left, right = [], []
    row = lax.broadcasted_iota(jnp.int32, (rows, LANES), 0)
    column = lax.broadcasted_iota(jnp.int32, (columns, LANES), 0)
    for index, (block, at, to) in enumerate(pieces):
        hit = row == at
        left.append(jnp.concatenate([jnp.where(hit, block[q], 0.0) for q in range(count)], axis=0))
        right.append(jnp.where(column == to, 1.0 if index == 2 * n_grp else -1.0, 0.0))
    matrix = jnp.concatenate(right, axis=1).astype(jnp.bfloat16)
    high, low = split(jnp.concatenate(left, axis=1))
    total = contract(high, matrix) + contract(low, matrix)
    where = {pair: q for q, pair in enumerate(PAIRS)}
    for i in range(6):
        for j in range(6):
            q = where[min(i, j), max(i, j)]
            hessian[i, j] = total[q * rows : (q + 1) * rows, :]


def local(samples, point_count, corr_scan, corr_tile, corr_src):
    f32, i32 = jnp.float32, jnp.int32
    scan_local, tiles_local = samples.shape[0], samples.shape[1]
    request_count = scan_local * corr_scan.shape[1]
    n_scan, n_grp = lax.axis_size("scan"), lax.axis_size("grp")
    devices = n_scan * n_grp
    cap = 2 * request_count // devices
    width = n_grp * cap
    packed_rows = VALUES * width // LANES
    per_block = LANES // width
    blocks = n_scan // per_block
    columns = scan_local * n_scan // n_grp
    grad_rows = scan_local // n_grp
    assert blocks == n_grp and blocks * per_block == n_scan and 8 * scan_local == LANES
    shape = jax.ShapeDtypeStruct
    dma = pltpu.SemaphoreType.DMA

    tiles = samples.transpose(0, 2, 1, 3)
    per_scan = corr_scan.shape[1]
    assert request_count <= 256 and scan_local * tiles_local <= 256
    slots, meta = pl.pallas_call(
        functools.partial(route_kernel, cap, n_grp, scan_local, tiles_local),
        out_shape=(shape((devices * cap // LANES, LANES), i32), shape((devices, 1, LANES), i32)),
        in_specs=[VMEM, VMEM],
        out_specs=(VMEM, VMEM),
        scratch_shapes=[pltpu.VMEM((scan_local, LANES), i32)],
    )(corr_scan, corr_tile)

    by_source, by_partner, shares, parts = pl.pallas_call(
        functools.partial(exchange_kernel, cap, n_grp),
        out_shape=(
            shape((n_grp * per_block, packed_rows, LANES), f32),
            shape((n_grp, VALUES, LANES), f32),
            shape((devices * SUMS, 1, LANES), f32),
            shape((n_grp * SUMS, 1, LANES), f32),
        ),
        in_specs=[ANY] * 5,
        out_specs=(ANY,) * 4,
        scratch_shapes=[
            pltpu.VMEM(tiles.shape, f32),
            pltpu.SMEM(point_count.shape, i32),
            pltpu.VMEM(corr_src.shape, i32),
            pltpu.SMEM(slots.shape, i32),
            pltpu.VMEM((devices * cap * 4, LANES), f32),
            pltpu.VMEM((devices * cap * 4, LANES), f32),
            pltpu.VMEM(meta.shape, i32),
            pltpu.SMEM(meta.shape, i32),
            pltpu.VMEM((scan_local * tiles_local, 8, LANES), f32),
            pltpu.VMEM((LANES * 8, LANES), f32),
            pltpu.VMEM((10, LANES, LANES), f32),
            pltpu.VMEM((blocks, 8, LANES), f32),
            pltpu.VMEM((blocks, VALUES, LANES), f32),
            pltpu.VMEM((n_scan, packed_rows, LANES), f32),
            pltpu.VMEM((VALUES, LANES), f32),
            pltpu.VMEM((n_scan * SUMS, 1, LANES), f32),
            pltpu.VMEM((SUMS, 1, LANES), f32),
        ]
        + [dma((6,)), dma((6,)), dma((blocks,)), dma((5,))],
        compiler_params=pltpu.CompilerParams(collective_id=0, has_side_effects=True),
    )(tiles, point_count, corr_src, slots, meta)

    hessian, gradient = pl.pallas_call(
        functools.partial(assemble_kernel, n_grp, width),
        out_shape=(shape((6, 6, scan_local, columns), f32), shape((grad_rows, 6), f32)),
        in_specs=[VMEM] * 4,
        out_specs=(VMEM, VMEM),
        scratch_shapes=[pltpu.VMEM((LANES, 8), f32)],
    )(by_source, by_partner, shares, parts)
    return hessian.transpose(2, 0, 1, 3), gradient


def solution(mesh):
    placed = (
        P("scan", "grp", None, None),
        P("scan"),
        P("scan", "grp"),
        P("scan", "grp"),
        P("scan", "grp", None),
    )
    return jax.shard_map(
        local,
        mesh=mesh,
        in_specs=placed,
        out_specs=(P("scan", None, None, "grp"), P(("scan", "grp"), None)),
        check_vma=False,
    )
```

```python
import functools

import jax
import jax.numpy as jnp
from jax import lax
from jax.experimental import pallas as pl
from jax.experimental.pallas import tpu as pltpu
from jax.sharding import PartitionSpec as P

LANES = 128
VALUES = 32
LEAST_POINTS = 4096
SUMS = VALUES // 8
IDS, VECTOR = 21, 24
FLAT, USED = 512, 1 << 20
PAIRS = [(i, j) for i in range(6) for j in range(i, 6)]
VMEM = pl.BlockSpec(memory_space=pltpu.VMEM)
SMEM = pl.BlockSpec(memory_space=pltpu.SMEM)
ANY = pl.BlockSpec(memory_space=pl.ANY)


def halves(value, size):
    if size & (size - 1):
        return value // size, value % size
    return value >> (size.bit_length() - 1), value & (size - 1)


def lane_take(table, index):
    return jnp.take_along_axis(table, index, axis=1, mode="promise_in_bounds")


def route(cap, n_grp, tiles_local, first_scan, scans, tiles, wide, slots, meta):
    scan_local, per_scan = scans.shape
    chunks, together = scan_local * per_scan // LANES, LANES // per_scan

    def flat(ref):
        wide[...] = jnp.zeros_like(wide)
        wide[:, 0:per_scan] = ref[...]
        out = []
        for h in range(chunks):
            moved = pltpu.roll(wide[h * together : (h + 1) * together, :], 0, 1, stride=per_scan, stride_axis=0)
            out.append(row_sum(moved))
        return out

    def column(row):
        return jnp.broadcast_to(row, (LANES, LANES)).T

    sublane = lax.broadcasted_iota(jnp.int32, (LANES, LANES), 0)
    lane = lax.broadcasted_iota(jnp.int32, (LANES, LANES), 1)
    index = lax.broadcasted_iota(jnp.int32, (1, LANES), 1)
    targets, codes = [], []
    for h, (b, t) in enumerate(zip(flat(scans), flat(tiles))):
        (b_dev, b_loc), (t_dev, t_loc) = halves(b, scan_local), halves(t, tiles_local)
        targets.append(b_dev * n_grp + t_dev)
        codes.append(column(USED + (b_loc * tiles_local + t_loc) * FLAT + index + h * LANES))
    target_columns = [column(x) for x in targets]
    places = []
    for h in range(chunks):
        rank = jnp.zeros((1, LANES), jnp.int32)
        for e in range(h + 1):
            same = target_columns[e] == targets[h]
            if e == h:
                same = same & (sublane < lane)
            rank = rank + row_sum(jnp.where(same, 1, 0))
        places.append(column(targets[h] * cap + rank))
    served = LANES // cap
    part = lax.broadcasted_iota(jnp.int32, (served, LANES), 1) // cap
    for a in range(slots.shape[0]):
        table = jnp.zeros((1, LANES), jnp.int32)
        for h in range(chunks):
            table = table + row_sum(jnp.where(places[h] == lane + a * LANES, codes[h], 0))
        used, request, tile = table >= USED, table & (FLAT - 1), (table & (USED - 1)) >> (FLAT.bit_length() - 1)
        slots[a : a + 1, :] = request
        source = first_scan + halves(request, per_scan)[0]
        kinds = [jnp.where(used, halves(tile, tiles_local)[0], -1), tile, jnp.where(used, source, -1)]
        total = jnp.zeros((served, LANES), jnp.int32)
        for kind, row in enumerate(kinds):
            moved = pltpu.roll(jnp.broadcast_to(row, (served, LANES)), cap, 1, stride=cap, stride_axis=0)
            if kind:
                moved = pltpu.roll(moved, kind * cap, 1)
            total = jnp.where(part == kind, moved, total)
        for i in range(served):
            meta[a * served + i] = total[served - 1 - i : served - i, :]


def greet_all(n_grp, devices, me):
    barrier = pltpu.get_barrier_semaphore()

    def hello(k, _):
        peer = lax.rem(me + k, devices)
        pl.semaphore_signal(
            barrier, inc=1, device_id=(peer // n_grp, peer % n_grp), device_id_type=pl.DeviceIdType.MESH
        )
        return 0

    lax.fori_loop(1, devices, hello, 0)


def await_all(devices):
    pl.semaphore_wait(pltpu.get_barrier_semaphore(), devices - 1)


def remote(src, dst, send, recv, peer, n_grp):
    return pltpu.make_async_remote_copy(
        src_ref=src, dst_ref=dst, send_sem=send, recv_sem=recv,
        device_id=(peer // n_grp, peer % n_grp), device_id_type=pl.DeviceIdType.MESH,
    )


def exclusive(a, b, size):
    if size & (size - 1):
        return lax.rem(a + b, size)
    total = 0
    for bit in range(size.bit_length() - 1):
        total = total + ((((a >> bit) + (b >> bit)) & 1) << bit)
    return total


def split(values):
    high = values.astype(jnp.bfloat16)
    return high, (values - high.astype(jnp.float32)).astype(jnp.bfloat16)


def contract(a, b):
    return lax.dot_general(a, b, (((1,), (1,)), ((), ())), preferred_element_type=jnp.float32)


def row_sum(products):
    return jnp.sum(products, axis=0, keepdims=True)


def within(index, size):
    return jnp.maximum(jnp.minimum(index, size - 1), 0)


def wait_for(ref, count, semaphore):
    part = ref.at[pl.ds(0, count)]
    pltpu.make_async_copy(part, part, semaphore).wait()


def compact(sums, place, rows):
    lane = lax.broadcasted_iota(jnp.int32, (8, LANES), 1)
    out = []
    for a in range(SUMS):
        part = sums[a * 8 : (a + 1) * 8, :]
        if place:
            part = pltpu.roll(part, LANES - place * rows, 1)
        part = jnp.where(lane < rows, part, 0.0)
        out.append(row_sum(pltpu.roll(part, 0, 1, stride=rows, stride_axis=0)))
    return out


def exchange_kernel(
    cap, n_grp, samples_hbm, count_hbm, wanted_hbm, scans_hbm, tiles_hbm, by_source, by_partner, shares, parts,
    samples, count, wanted, scans, partner_tiles, wide, routed, slots, meta, data, data_in, meta_in, codes, tiles, comps, turned, ids, result, packed,
    tally, share_out, part_out,
    sent, received, recv_data, own,
):
    scan_local, tiles_local = samples.shape[0], samples.shape[2]
    per_scan = wanted.shape[1]
    n_scan = packed.shape[0]
    devices = n_scan * n_grp
    rows = cap * 4
    width = n_grp * cap
    per_block = LANES // width
    blocks = n_scan // per_block
    sources = per_block * n_grp
    packed_rows = packed.shape[1]
    scan_index, group_index = lax.axis_index("scan"), lax.axis_index("grp")
    me = scan_index * n_grp + group_index
    home, home_row = scan_index // per_block, lax.rem(scan_index, per_block)
    full_groups = min(LEAST_POINTS // (tiles_local * LANES), n_grp) if 3 * cap % 8 == 0 else 0
    short = rows - cap

    def send_one(peer, size):
        return remote(
            data.at[pl.ds(pl.multiple_of(peer * rows, 8), size)],
            data_in.at[pl.ds(pl.multiple_of(me * rows, 8), size)],
            sent.at[0], recv_data.at[home], peer, n_grp,
        )

    def send_code(peer):
        return remote(meta.at[peer], meta_in.at[me], sent.at[1], received.at[1], peer, n_grp)

    def to_source(row, holder):
        peer = row * n_grp + home
        return remote(packed.at[row], by_source.at[holder], sent.at[2], received.at[2], peer, n_grp)

    def to_partner(block):
        peer = scan_index * n_grp + block
        return remote(result.at[block], by_partner.at[group_index], sent.at[3], received.at[3], peer, n_grp)

    def to_share(peer, row, first):
        size = SUMS - first
        return remote(
            share_out.at[pl.ds(row * SUMS + first, size)], shares.at[pl.ds(me * SUMS + first, size)],
            sent.at[4], received.at[4], peer, n_grp,
        )

    def to_part(g, first):
        size = SUMS - first
        return remote(
            part_out.at[pl.ds(first, size)], parts.at[pl.ds(group_index * SUMS + first, size)],
            sent.at[5], received.at[5], scan_index * n_grp + g, n_grp,
        )

    fetch = pltpu.make_async_copy(samples_hbm, samples, own.at[3])
    fetch_count = pltpu.make_async_copy(count_hbm, count, own.at[4])
    fetch_wanted = pltpu.make_async_copy(wanted_hbm, wanted, own.at[0])
    fetch_scans = pltpu.make_async_copy(scans_hbm, scans, own.at[1])
    fetch_tiles = pltpu.make_async_copy(tiles_hbm, partner_tiles, own.at[2])
    fetch_scans.start()
    fetch_tiles.start()
    fetch_count.start()
    fetch_wanted.start()
    fetch.start()
    greet_all(n_grp, devices, me)
    fetch_scans.wait()
    fetch_tiles.wait()
    route(cap, n_grp, tiles_local, scan_index * scan_local, scans, partner_tiles, wide, routed, meta)
    fetch_slots = pltpu.make_async_copy(routed, slots, own.at[1])
    fetch_slots.start()
    fetch_count.wait()
    fetch_wanted.wait()
    fetch.wait()
    fetch_slots.wait()
    first_point = group_index * tiles_local * LANES
    wanted_rows = wanted.reshape(scan_local * per_scan, LANES)
    tile_row = lax.broadcasted_iota(jnp.int32, (tiles_local, LANES), 0)

    def collect(peer, into):
        first = lax.rem(peer, LANES // cap) * cap
        for j in range(cap):
            request = within(slots[peer // (LANES // cap), first + j], scan_local * per_scan)
            s = halves(request, per_scan)[0]
            point = wanted_rows[pl.ds(request, 1), :]
            spread = jnp.broadcast_to(point, (tiles_local, LANES))
            hit, place = spread >> 7 == tile_row, spread & (LANES - 1)
            for c in range(3):
                found = jnp.where(hit, lane_take(samples[s, c], place), 0.0)
                into[pl.ds(peer * rows + c * cap + j, 1), :] = row_sum(found)
            mask = jnp.where(first_point + point < count[s], 1.0, 0.0).astype(jnp.float32)
            into[pl.ds(peer * rows + 3 * cap + j, 1), :] = mask

    await_all(devices)

    def start_meta(k, _):
        peer = lax.rem(me + k, devices)
        send_code(peer).start()
        return 0

    def start_data(k, _):
        peer = exclusive(me, k, devices)
        collect(peer, data)

        @pl.when((peer != me) & (group_index < full_groups))
        def _():
            send_one(peer, short).start()

        @pl.when((peer != me) & (group_index >= full_groups))
        def _():
            send_one(peer, rows).start()

        return 0

    lax.fori_loop(1, devices, start_meta, 0)
    share = devices // 4
    for quarter in (2, 1, 3, 0):
        lax.fori_loop(quarter * share, (quarter + 1) * share, start_data, 0)
    own_meta = pltpu.make_async_copy(meta.at[me], meta_in.at[me], own.at[1])
    own_meta.start()
    collect(me, data_in)
    own_meta.wait()

    def no_mask(row, _):
        for g in range(full_groups):
            first = pl.multiple_of((row * n_grp + g) * rows + short, 8)
            data_in[pl.ds(first, cap), :] = jnp.ones((cap, LANES), jnp.float32)
        return 0

    lax.fori_loop(0, n_scan, no_mask, 0)
    tally[...] = jnp.zeros_like(tally)
    result[...] = jnp.zeros_like(result)

    point = lax.broadcasted_iota(jnp.int32, (tiles_local, LANES), 0) * LANES
    point = point + lax.broadcasted_iota(jnp.int32, (tiles_local, LANES), 1)

    tile_rows = tiles.reshape(scan_local * tiles_local * 8, LANES)

    def fill(b, _):
        valid = point < count[b] - group_index * tiles_local * LANES
        for c in range(6):
            values = samples[b, c]
            if c >= 3:
                values = jnp.where(valid, values, 0.0)
            tile_rows[pl.ds(b * tiles_local * 8 + c, tiles_local, stride=8), :] = values
        return 0

    lax.fori_loop(0, scan_local, fill, 0)
    wait_for(meta_in, devices - 1, received.at[1])
    to_scalar = pltpu.make_async_copy(meta_in, codes, own.at[2])
    to_scalar.start()

    slot_lane = lax.broadcasted_iota(jnp.int32, (sources, LANES), 1) // cap
    slot_row = lax.broadcasted_iota(jnp.int32, (sources, LANES), 0)

    def decode(m, _):
        arrived = meta_in[pl.ds(m * sources, sources), 0, :]
        kinds = []
        for kind in (0, 2):
            moved = pltpu.roll(arrived, LANES - kind * cap, 1) if kind else arrived
            moved = pltpu.roll(moved, 0, 1, stride=cap, stride_axis=0)
            kinds.append(row_sum(jnp.where(slot_lane == slot_row, moved, 0)))
        partner, source = kinds
        ids[m, 0:1, :] = source.astype(jnp.float32)
        ids[m, 1:2, :] = jnp.where(partner < 0, -1, scan_index * scan_local + partner).astype(jnp.float32)
        return 0

    lax.fori_loop(0, blocks, decode, 0)
    to_scalar.wait()

    def one_block(k, _):
        m = exclusive(home, k, blocks)

        def gather(i, _):
            for j in range(cap):
                slot = i * cap + j
                row = within(codes[m * sources + i, 0, cap + j], scan_local * tiles_local)
                comps[pl.ds(pl.multiple_of(slot * 8, 8), 8), :] = tiles[row]
            return 0

        lax.fori_loop(0, sources, gather, 0)
        for c in range(6):
            turned[4 + c] = comps[pl.ds(c, LANES, stride=8), :].T

        whole = per_block * (n_grp * rows - full_groups * cap)

        @pl.when(m != home)
        def _():
            wait_for(data_in, whole, recv_data.at[m])

        @pl.when((m == home) & (group_index < full_groups))
        def _():
            wait_for(data_in, whole - short, recv_data.at[m])

        @pl.when((m == home) & (group_index >= full_groups))
        def _():
            wait_for(data_in, whole - rows, recv_data.at[m])

        for c in range(4):
            pieces = [
                data_in[pl.ds((m * sources + i) * rows + c * cap, cap), :] for i in range(sources)
            ]
            turned[c] = jnp.concatenate(pieces, axis=0).T

        def step(kk, sums):
            at = pl.ds(pl.multiple_of(kk * 8, 8), 8)
            px, py, pz, mask, qx, qy, qz, nx, ny, nz = [turned[c, at, :] for c in range(10)]
            residual = nx * (px - qx) + ny * (py - qy) + nz * (pz - qz)
            weight = mask / (1.0 + residual * residual)
            jac = [py * nz - pz * ny, pz * nx - px * nz, px * ny - py * nx, nx, ny, nz]
            scaled = [weight * x for x in jac]
            products = [scaled[a] * jac[b] for a, b in PAIRS] + [x * residual for x in scaled]
            return tuple(s + p for s, p in zip(sums, products))

        zero = jnp.zeros((8, LANES), jnp.float32)
        sums = lax.fori_loop(0, LANES // 8, step, (zero,) * (len(PAIRS) + 6), unroll=True)
        for q, total in enumerate(sums):
            q = q if q < len(PAIRS) else q - len(PAIRS) + VECTOR
            result[m, q : q + 1, :] = row_sum(total)
        result[m, IDS : IDS + 2, :] = ids[m, 0:2, :]
        values = result[m]
        lane = lax.broadcasted_iota(jnp.int32, (packed_rows, LANES), 1) // width
        chunks = [values[g * packed_rows : (g + 1) * packed_rows, :] for g in range(per_block)]
        for p in range(per_block):
            total = chunks[p]
            for g in range(per_block):
                if g != p:
                    total = jnp.where(lane == g, pltpu.roll(chunks[g], (g - p) * width % LANES, 1), total)
            row = m * per_block + p
            packed[row] = total
            holder = group_index * per_block + home_row

            @pl.when(row * n_grp + home == me)
            def _():
                pltpu.make_async_copy(packed.at[row], by_source.at[holder], own.at[3]).start()

            @pl.when(row * n_grp + home != me)
            def _():
                to_source(row, holder).start()

        @pl.when(m == group_index)
        def _():
            pltpu.make_async_copy(result.at[group_index], by_partner.at[group_index], own.at[4]).start()

        @pl.when(m != group_index)
        def _():
            to_partner(m).start()

        high, low = split(values)
        source = ids[m, 0:1, :].astype(jnp.int32) - m * per_block * scan_local
        partner = ids[m, 1:2, :].astype(jnp.int32) - scan_index * scan_local
        span = lax.broadcasted_iota(jnp.int32, (LANES, LANES), 0)
        chosen = jnp.where(span == source, 1.0, 0.0).astype(jnp.bfloat16)
        sums = contract(high, chosen) + contract(low, chosen)
        chosen = jnp.where(span == partner, 1.0, 0.0).astype(jnp.bfloat16)
        tally[...] += contract(high, chosen) + contract(low, chosen)
        for p in range(per_block):
            row = m * per_block + p
            for a, line in enumerate(compact(sums, p, scan_local)):
                share_out[row * SUMS + a] = line
            for g in range(n_grp):
                peer = row * n_grp + g

                @pl.when((peer != me) & (m == g))
                def _():
                    to_share(peer, row, 0).start()

                @pl.when((peer != me) & (m != g))
                def _():
                    to_share(peer, row, SUMS - 1).start()

        return 0

    lax.fori_loop(0, blocks, one_block, 0)
    for a, line in enumerate(compact(tally[...], 0, scan_local)):
        part_out[a] = line
    own_share = pltpu.make_async_copy(
        share_out.at[pl.ds(scan_index * SUMS, SUMS)], shares.at[pl.ds(me * SUMS, SUMS)], own.at[0]
    )
    own_part = pltpu.make_async_copy(part_out, parts.at[pl.ds(group_index * SUMS, SUMS)], own.at[1])
    own_share.start()
    own_part.start()
    for g in range(n_grp):

        @pl.when((g != group_index) & (home == g))
        def _():
            to_part(g, 0).start()

        @pl.when((g != group_index) & (home != g))
        def _():
            to_part(g, SUMS - 1).start()

    others = n_grp - 1
    wait_for(by_partner, others, received.at[3])
    wait_for(result, others, sent.at[3])
    wait_for(meta_in, devices - 1, sent.at[1])

    @pl.when(home == group_index)
    def _():
        pltpu.make_async_copy(packed.at[0], by_source.at[0], own.at[3]).wait()
        wait_for(by_source, sources - 1, received.at[2])
        wait_for(packed, n_scan - 1, sent.at[2])
        wait_for(shares, (devices - 1) * SUMS, received.at[4])
        wait_for(shares, n_scan * (SUMS + others) - SUMS, sent.at[4])
        wait_for(parts, others * SUMS, received.at[5])
        wait_for(parts, others, sent.at[5])

    @pl.when(home != group_index)
    def _():
        wait_for(by_source, sources, received.at[2])
        wait_for(packed, n_scan, sent.at[2])
        wait_for(shares, devices - 1, received.at[4])
        wait_for(shares, n_scan * (SUMS + others) - 1, sent.at[4])
        wait_for(parts, others, received.at[5])
        wait_for(parts, others - 1 + SUMS, sent.at[5])

    pltpu.make_async_copy(result.at[0], by_partner.at[group_index], own.at[4]).wait()
    own_share.wait()
    own_part.wait()

    @pl.when(group_index < full_groups)
    def _():
        wait_for(data, (devices - 1) * short, sent.at[0])

    @pl.when(group_index >= full_groups)
    def _():
        wait_for(data, (devices - 1) * rows, sent.at[0])


def regroup(parts, width):
    groups = len(parts)
    lane = lax.broadcasted_iota(jnp.int32, parts[0].shape, 1) // width
    out = []
    for b in range(groups):
        total = parts[b]
        for g in range(groups):
            if g != b:
                total = jnp.where(lane == g, pltpu.roll(parts[g], (g - b) * width % LANES, 1), total)
        out.append(total)
    return out


def assemble_kernel(n_grp, width, by_source, by_partner, shares, parts, hessian, gradient, spare):
    rows, columns = hessian.shape[2], hessian.shape[3]
    grad_rows = gradient.shape[0]
    per_block = LANES // width
    scan_index, group_index = lax.axis_index("scan"), lax.axis_index("grp")
    home, home_row = scan_index // per_block, lax.rem(scan_index, per_block)
    first_row, first_column = scan_index * rows, group_index * columns
    count = len(PAIRS)

    def total_of(ref):
        total = ref[0:SUMS, 0, :]
        for d in range(1, ref.shape[0] // SUMS):
            total = total + ref[d * SUMS : (d + 1) * SUMS, 0, :]
        return total

    def spread(line):
        return pltpu.roll(jnp.broadcast_to(line, (8, LANES)), rows, 1, stride=rows, stride_axis=0)

    outgoing, incoming = total_of(shares), total_of(parts)
    vector = spread(outgoing[SUMS - 1 :, :] - incoming[SUMS - 1 :, :])
    spare[...] = jnp.concatenate([vector[7 - i : 8 - i, :] for i in range(8)], axis=0).T
    gradient[...] = spare[pl.ds(group_index * grad_rows, grad_rows), 0:6]
    both = [spread(outgoing[a : a + 1, :] + incoming[a : a + 1, :]) for a in range(SUMS - 1)]
    lines = [both[q // 8][7 - q % 8 : 8 - q % 8, :] for q in range(count)]

    pieces = []
    for g in range(n_grp):
        halves_ = [by_source[g * per_block + p] for p in range(per_block)]
        block = jnp.concatenate(regroup(halves_, width), axis=0)
        source, partner = [block[r : r + 1, :].astype(jnp.int32) for r in (IDS, IDS + 1)]
        pieces.append((block, source - first_row, partner - first_column))
    for g in range(n_grp):
        block = by_partner[g]
        source, partner = [block[r : r + 1, :].astype(jnp.int32) for r in (IDS, IDS + 1)]
        pieces.append((block, partner - first_row, source - first_column))
    pieces = [([block[q : q + 1, :] for q in range(count)], at, to) for block, at, to in pieces]
    lane = lax.broadcasted_iota(jnp.int32, (1, LANES), 1)
    diagonal = jnp.where((lane < rows) & (group_index == home), lane, -1)
    pieces.append((lines, diagonal, jnp.where(diagonal < 0, -1, lane + home_row * rows)))

    left, right = [], []
    row = lax.broadcasted_iota(jnp.int32, (rows, LANES), 0)
    column = lax.broadcasted_iota(jnp.int32, (columns, LANES), 0)
    for index, (block, at, to) in enumerate(pieces):
        hit = row == at
        left.append(jnp.concatenate([jnp.where(hit, block[q], 0.0) for q in range(count)], axis=0))
        right.append(jnp.where(column == to, 1.0 if index == 2 * n_grp else -1.0, 0.0))
    matrix = jnp.concatenate(right, axis=1).astype(jnp.bfloat16)
    high, low = split(jnp.concatenate(left, axis=1))
    total = contract(high, matrix) + contract(low, matrix)
    where = {pair: q for q, pair in enumerate(PAIRS)}
    for i in range(6):
        for j in range(6):
            q = where[min(i, j), max(i, j)]
            hessian[i, j] = total[q * rows : (q + 1) * rows, :]


def local(samples, point_count, corr_scan, corr_tile, corr_src):
    f32, i32 = jnp.float32, jnp.int32
    scan_local, tiles_local = samples.shape[0], samples.shape[1]
    request_count = scan_local * corr_scan.shape[1]
    n_scan, n_grp = lax.axis_size("scan"), lax.axis_size("grp")
    devices = n_scan * n_grp
    cap = 2 * request_count // devices
    width = n_grp * cap
    packed_rows = VALUES * width // LANES
    per_block = LANES // width
    blocks = n_scan // per_block
    columns = scan_local * n_scan // n_grp
    grad_rows = scan_local // n_grp
    assert blocks == n_grp and blocks * per_block == n_scan and 8 * scan_local == LANES
    shape = jax.ShapeDtypeStruct
    dma = pltpu.SemaphoreType.DMA

    tiles = samples.transpose(0, 2, 1, 3)
    per_scan = corr_scan.shape[1]
    assert request_count <= FLAT and scan_local * tiles_local * FLAT <= USED
    table = (devices * cap // LANES, LANES)

    by_source, by_partner, shares, parts = pl.pallas_call(
        functools.partial(exchange_kernel, cap, n_grp),
        out_shape=(
            shape((n_grp * per_block, packed_rows, LANES), f32),
            shape((n_grp, VALUES, LANES), f32),
            shape((devices * SUMS, 1, LANES), f32),
            shape((n_grp * SUMS, 1, LANES), f32),
        ),
        in_specs=[ANY] * 5,
        out_specs=(ANY,) * 4,
        scratch_shapes=[
            pltpu.VMEM(tiles.shape, f32),
            pltpu.SMEM(point_count.shape, i32),
            pltpu.VMEM(corr_src.shape, i32),
            pltpu.VMEM(corr_scan.shape, i32),
            pltpu.VMEM(corr_tile.shape, i32),
            pltpu.VMEM((scan_local, LANES), i32),
            pltpu.VMEM(table, i32),
            pltpu.SMEM(table, i32),
            pltpu.VMEM((devices, 1, LANES), i32),
            pltpu.VMEM((devices * cap * 4, LANES), f32),
            pltpu.VMEM((devices * cap * 4, LANES), f32),
            pltpu.VMEM((devices, 1, LANES), i32),
            pltpu.SMEM((devices, 1, LANES), i32),
            pltpu.VMEM((scan_local * tiles_local, 8, LANES), f32),
            pltpu.VMEM((LANES * 8, LANES), f32),
            pltpu.VMEM((10, LANES, LANES), f32),
            pltpu.VMEM((blocks, 8, LANES), f32),
            pltpu.VMEM((blocks, VALUES, LANES), f32),
            pltpu.VMEM((n_scan, packed_rows, LANES), f32),
            pltpu.VMEM((VALUES, LANES), f32),
            pltpu.VMEM((n_scan * SUMS, 1, LANES), f32),
            pltpu.VMEM((SUMS, 1, LANES), f32),
        ]
        + [dma((6,)), dma((6,)), dma((blocks,)), dma((5,))],
        compiler_params=pltpu.CompilerParams(collective_id=0, has_side_effects=True),
    )(tiles, point_count, corr_src, corr_scan, corr_tile)

    hessian, gradient = pl.pallas_call(
        functools.partial(assemble_kernel, n_grp, width),
        out_shape=(shape((6, 6, scan_local, columns), f32), shape((grad_rows, 6), f32)),
        in_specs=[VMEM] * 4,
        out_specs=(VMEM, VMEM),
        scratch_shapes=[pltpu.VMEM((LANES, 8), f32)],
    )(by_source, by_partner, shares, parts)
    return hessian.transpose(2, 0, 1, 3), gradient


def solution(mesh):
    placed = (
        P("scan", "grp", None, None),
        P("scan"),
        P("scan", "grp"),
        P("scan", "grp"),
        P("scan", "grp", None),
    )
    return jax.shard_map(
        local,
        mesh=mesh,
        in_specs=placed,
        out_specs=(P("scan", None, None, "grp"), P(("scan", "grp"), None)),
        check_vma=False,
    )
```

```python
import functools

import jax
import jax.numpy as jnp
from jax import lax
from jax.experimental import pallas as pl
from jax.experimental.pallas import tpu as pltpu
from jax.sharding import PartitionSpec as P

LANES = 128
VALUES = 32
LEAST_POINTS = 4096
SUMS = VALUES // 8
IDS, VECTOR, REPLY = 21, 24, 24
FLAT, USED = 512, 1 << 20
PAIRS = [(i, j) for i in range(6) for j in range(i, 6)]
VMEM = pl.BlockSpec(memory_space=pltpu.VMEM)
SMEM = pl.BlockSpec(memory_space=pltpu.SMEM)
ANY = pl.BlockSpec(memory_space=pl.ANY)


def halves(value, size):
    if size & (size - 1):
        return value // size, value % size
    return value >> (size.bit_length() - 1), value & (size - 1)


def lane_take(table, index):
    return jnp.take_along_axis(table, index, axis=1, mode="promise_in_bounds")


def route(cap, n_grp, tiles_local, first_scan, scans, tiles, wide, slots, meta):
    scan_local, per_scan = scans.shape
    chunks, together = scan_local * per_scan // LANES, LANES // per_scan

    def flat(ref):
        wide[...] = jnp.zeros_like(wide)
        wide[:, 0:per_scan] = ref[...]
        out = []
        for h in range(chunks):
            moved = pltpu.roll(wide[h * together : (h + 1) * together, :], 0, 1, stride=per_scan, stride_axis=0)
            out.append(row_sum(moved))
        return out

    def column(row):
        return jnp.broadcast_to(row, (LANES, LANES)).T

    sublane = lax.broadcasted_iota(jnp.int32, (LANES, LANES), 0)
    lane = lax.broadcasted_iota(jnp.int32, (LANES, LANES), 1)
    index = lax.broadcasted_iota(jnp.int32, (1, LANES), 1)
    targets, codes = [], []
    for h, (b, t) in enumerate(zip(flat(scans), flat(tiles))):
        (b_dev, b_loc), (t_dev, t_loc) = halves(b, scan_local), halves(t, tiles_local)
        targets.append(b_dev * n_grp + t_dev)
        codes.append(column(USED + (b_loc * tiles_local + t_loc) * FLAT + index + h * LANES))
    target_columns = [column(x) for x in targets]
    places = []
    for h in range(chunks):
        rank = jnp.zeros((1, LANES), jnp.int32)
        for e in range(h + 1):
            same = target_columns[e] == targets[h]
            if e == h:
                same = same & (sublane < lane)
            rank = rank + row_sum(jnp.where(same, 1, 0))
        places.append(column(targets[h] * cap + rank))
    served = LANES // cap
    part = lax.broadcasted_iota(jnp.int32, (served, LANES), 1) // cap
    for a in range(slots.shape[0]):
        table = jnp.zeros((1, LANES), jnp.int32)
        for h in range(chunks):
            table = table + row_sum(jnp.where(places[h] == lane + a * LANES, codes[h], 0))
        used, request, tile = table >= USED, table & (FLAT - 1), (table & (USED - 1)) >> (FLAT.bit_length() - 1)
        slots[a : a + 1, :] = request
        source = first_scan + halves(request, per_scan)[0]
        kinds = [jnp.where(used, halves(tile, tiles_local)[0], -1), tile, jnp.where(used, source, -1)]
        total = jnp.zeros((served, LANES), jnp.int32)
        for kind, row in enumerate(kinds):
            moved = pltpu.roll(jnp.broadcast_to(row, (served, LANES)), cap, 1, stride=cap, stride_axis=0)
            if kind:
                moved = pltpu.roll(moved, kind * cap, 1)
            total = jnp.where(part == kind, moved, total)
        for i in range(served):
            meta[a * served + i] = total[served - 1 - i : served - i, :]


def greet_all(n_grp, devices, me):
    barrier = pltpu.get_barrier_semaphore()

    def hello(k, _):
        peer = lax.rem(me + k, devices)
        pl.semaphore_signal(
            barrier, inc=1, device_id=(peer // n_grp, peer % n_grp), device_id_type=pl.DeviceIdType.MESH
        )
        return 0

    lax.fori_loop(1, devices, hello, 0)


def await_all(devices):
    pl.semaphore_wait(pltpu.get_barrier_semaphore(), devices - 1)


def remote(src, dst, send, recv, peer, n_grp):
    return pltpu.make_async_remote_copy(
        src_ref=src, dst_ref=dst, send_sem=send, recv_sem=recv,
        device_id=(peer // n_grp, peer % n_grp), device_id_type=pl.DeviceIdType.MESH,
    )


def exclusive(a, b, size):
    if size & (size - 1):
        return lax.rem(a + b, size)
    total = 0
    for bit in range(size.bit_length() - 1):
        total = total + ((((a >> bit) + (b >> bit)) & 1) << bit)
    return total


def split(values):
    high = values.astype(jnp.bfloat16)
    return high, (values - high.astype(jnp.float32)).astype(jnp.bfloat16)


def contract(a, b):
    return lax.dot_general(a, b, (((1,), (1,)), ((), ())), preferred_element_type=jnp.float32)


def row_sum(products):
    return jnp.sum(products, axis=0, keepdims=True)


def within(index, size):
    return jnp.maximum(jnp.minimum(index, size - 1), 0)


def wait_for(ref, count, semaphore):
    part = ref.at[pl.ds(0, count)]
    pltpu.make_async_copy(part, part, semaphore).wait()


def compact(sums, place, rows):
    lane = lax.broadcasted_iota(jnp.int32, (8, LANES), 1)
    out = []
    for a in range(SUMS):
        part = sums[a * 8 : (a + 1) * 8, :]
        if place:
            part = pltpu.roll(part, LANES - place * rows, 1)
        part = jnp.where(lane < rows, part, 0.0)
        out.append(row_sum(pltpu.roll(part, 0, 1, stride=rows, stride_axis=0)))
    return out


def exchange_kernel(
    cap, n_grp, samples_hbm, count_hbm, wanted_hbm, scans_hbm, tiles_hbm, by_source, by_partner, shares, parts,
    samples, count, wanted, scans, partner_tiles, wide, routed, slots, meta, data, data_in, meta_in, codes, tiles, comps, turned, ids, result, packed,
    tally, share_out, part_out,
    sent, received, recv_data, own,
):
    scan_local, tiles_local = samples.shape[0], samples.shape[2]
    per_scan = wanted.shape[1]
    n_scan = packed.shape[0]
    devices = n_scan * n_grp
    rows = cap * 4
    width = n_grp * cap
    per_block = LANES // width
    blocks = n_scan // per_block
    sources = per_block * n_grp
    packed_rows = packed.shape[1]
    scan_index, group_index = lax.axis_index("scan"), lax.axis_index("grp")
    me = scan_index * n_grp + group_index
    home, home_row = scan_index // per_block, lax.rem(scan_index, per_block)
    full_groups = min(LEAST_POINTS // (tiles_local * LANES), n_grp) if 3 * cap % 8 == 0 else 0
    short = rows - cap

    def send_one(peer, size):
        return remote(
            data.at[pl.ds(pl.multiple_of(peer * rows, 8), size)],
            data_in.at[pl.ds(pl.multiple_of(me * rows, 8), size)],
            sent.at[0], recv_data.at[home], peer, n_grp,
        )

    def send_code(peer):
        return remote(meta.at[peer], meta_in.at[me], sent.at[1], received.at[1], peer, n_grp)

    def to_source(row, holder):
        peer = row * n_grp + home
        return remote(packed.at[row], by_source.at[holder], sent.at[2], received.at[2], peer, n_grp)

    def to_partner(block):
        peer = scan_index * n_grp + block
        return remote(result.at[block], by_partner.at[group_index], sent.at[3], received.at[3], peer, n_grp)

    def to_share(peer, row, first):
        size = SUMS - first
        return remote(
            share_out.at[pl.ds(row * SUMS + first, size)], shares.at[pl.ds(me * SUMS + first, size)],
            sent.at[4], received.at[4], peer, n_grp,
        )

    def to_part(g, first):
        size = SUMS - first
        return remote(
            part_out.at[pl.ds(first, size)], parts.at[pl.ds(group_index * SUMS + first, size)],
            sent.at[5], received.at[5], scan_index * n_grp + g, n_grp,
        )

    fetch = pltpu.make_async_copy(samples_hbm, samples, own.at[3])
    fetch_count = pltpu.make_async_copy(count_hbm, count, own.at[4])
    fetch_wanted = pltpu.make_async_copy(wanted_hbm, wanted, own.at[0])
    fetch_scans = pltpu.make_async_copy(scans_hbm, scans, own.at[1])
    fetch_tiles = pltpu.make_async_copy(tiles_hbm, partner_tiles, own.at[2])
    fetch_scans.start()
    fetch_tiles.start()
    fetch_count.start()
    fetch_wanted.start()
    fetch.start()
    greet_all(n_grp, devices, me)
    fetch_scans.wait()
    fetch_tiles.wait()
    route(cap, n_grp, tiles_local, scan_index * scan_local, scans, partner_tiles, wide, routed, meta)
    fetch_slots = pltpu.make_async_copy(routed, slots, own.at[1])
    fetch_slots.start()
    fetch_count.wait()
    fetch_wanted.wait()
    fetch.wait()
    fetch_slots.wait()
    first_point = group_index * tiles_local * LANES
    wanted_rows = wanted.reshape(scan_local * per_scan, LANES)
    tile_row = lax.broadcasted_iota(jnp.int32, (tiles_local, LANES), 0)

    def collect(peer, into):
        first = lax.rem(peer, LANES // cap) * cap
        for j in range(cap):
            request = within(slots[peer // (LANES // cap), first + j], scan_local * per_scan)
            s = halves(request, per_scan)[0]
            point = wanted_rows[pl.ds(request, 1), :]
            spread = jnp.broadcast_to(point, (tiles_local, LANES))
            hit, place = spread >> 7 == tile_row, spread & (LANES - 1)
            for c in range(3):
                found = jnp.where(hit, lane_take(samples[s, c], place), 0.0)
                into[pl.ds(peer * rows + c * cap + j, 1), :] = row_sum(found)
            mask = jnp.where(first_point + point < count[s], 1.0, 0.0).astype(jnp.float32)
            into[pl.ds(peer * rows + 3 * cap + j, 1), :] = mask

    await_all(devices)

    def start_meta(k, _):
        peer = lax.rem(me + k, devices)
        send_code(peer).start()
        return 0

    def start_data(k, _):
        peer = exclusive(me, k, devices)
        collect(peer, data)

        @pl.when((peer != me) & (group_index < full_groups))
        def _():
            send_one(peer, short).start()

        @pl.when((peer != me) & (group_index >= full_groups))
        def _():
            send_one(peer, rows).start()

        return 0

    lax.fori_loop(1, devices, start_meta, 0)
    share = devices // 4
    for quarter in (2, 1, 3, 0):
        lax.fori_loop(quarter * share, (quarter + 1) * share, start_data, 0)
    own_meta = pltpu.make_async_copy(meta.at[me], meta_in.at[me], own.at[1])
    own_meta.start()
    collect(me, data_in)
    own_meta.wait()

    def no_mask(row, _):
        for g in range(full_groups):
            first = pl.multiple_of((row * n_grp + g) * rows + short, 8)
            data_in[pl.ds(first, cap), :] = jnp.ones((cap, LANES), jnp.float32)
        return 0

    lax.fori_loop(0, n_scan, no_mask, 0)
    tally[...] = jnp.zeros_like(tally)
    result[...] = jnp.zeros_like(result)

    point = lax.broadcasted_iota(jnp.int32, (tiles_local, LANES), 0) * LANES
    point = point + lax.broadcasted_iota(jnp.int32, (tiles_local, LANES), 1)

    tile_rows = tiles.reshape(scan_local * tiles_local * 8, LANES)

    def fill(b, _):
        valid = point < count[b] - group_index * tiles_local * LANES
        for c in range(6):
            values = samples[b, c]
            if c >= 3:
                values = jnp.where(valid, values, 0.0)
            tile_rows[pl.ds(b * tiles_local * 8 + c, tiles_local, stride=8), :] = values
        return 0

    lax.fori_loop(0, scan_local, fill, 0)
    wait_for(meta_in, devices - 1, received.at[1])
    to_scalar = pltpu.make_async_copy(meta_in, codes, own.at[2])
    to_scalar.start()

    slot_lane = lax.broadcasted_iota(jnp.int32, (sources, LANES), 1) // cap
    slot_row = lax.broadcasted_iota(jnp.int32, (sources, LANES), 0)

    def decode(m, _):
        arrived = meta_in[pl.ds(m * sources, sources), 0, :]
        kinds = []
        for kind in (0, 2):
            moved = pltpu.roll(arrived, LANES - kind * cap, 1) if kind else arrived
            moved = pltpu.roll(moved, 0, 1, stride=cap, stride_axis=0)
            kinds.append(row_sum(jnp.where(slot_lane == slot_row, moved, 0)))
        partner, source = kinds
        ids[m, 0:1, :] = source.astype(jnp.float32)
        ids[m, 1:2, :] = jnp.where(partner < 0, -1, scan_index * scan_local + partner).astype(jnp.float32)
        return 0

    lax.fori_loop(0, blocks, decode, 0)
    to_scalar.wait()

    def one_block(k, _):
        m = exclusive(home, k, blocks)

        def gather(i, _):
            for j in range(cap):
                slot = i * cap + j
                row = within(codes[m * sources + i, 0, cap + j], scan_local * tiles_local)
                comps[pl.ds(pl.multiple_of(slot * 8, 8), 8), :] = tiles[row]
            return 0

        lax.fori_loop(0, sources, gather, 0)
        for c in range(6):
            turned[4 + c] = comps[pl.ds(c, LANES, stride=8), :].T

        whole = per_block * (n_grp * rows - full_groups * cap)

        @pl.when(m != home)
        def _():
            wait_for(data_in, whole, recv_data.at[m])

        @pl.when((m == home) & (group_index < full_groups))
        def _():
            wait_for(data_in, whole - short, recv_data.at[m])

        @pl.when((m == home) & (group_index >= full_groups))
        def _():
            wait_for(data_in, whole - rows, recv_data.at[m])

        for c in range(4):
            pieces = [
                data_in[pl.ds((m * sources + i) * rows + c * cap, cap), :] for i in range(sources)
            ]
            turned[c] = jnp.concatenate(pieces, axis=0).T

        def step(kk, sums):
            at = pl.ds(pl.multiple_of(kk * 8, 8), 8)
            px, py, pz, mask, qx, qy, qz, nx, ny, nz = [turned[c, at, :] for c in range(10)]
            residual = nx * (px - qx) + ny * (py - qy) + nz * (pz - qz)
            weight = mask / (1.0 + residual * residual)
            jac = [py * nz - pz * ny, pz * nx - px * nz, px * ny - py * nx, nx, ny, nz]
            scaled = [weight * x for x in jac]
            products = [scaled[a] * jac[b] for a, b in PAIRS] + [x * residual for x in scaled]
            return tuple(s + p for s, p in zip(sums, products))

        zero = jnp.zeros((8, LANES), jnp.float32)
        sums = lax.fori_loop(0, LANES // 8, step, (zero,) * (len(PAIRS) + 6), unroll=True)
        for q, total in enumerate(sums):
            q = q if q < len(PAIRS) else q - len(PAIRS) + VECTOR
            result[m, q : q + 1, :] = row_sum(total)
        result[m, IDS : IDS + 2, :] = ids[m, 0:2, :]
        values = result[m]
        lane = lax.broadcasted_iota(jnp.int32, (packed_rows, LANES), 1) // width
        chunks = [values[g * packed_rows : (g + 1) * packed_rows, :] for g in range(per_block)]
        for p in range(per_block):
            total = chunks[p]
            for g in range(per_block):
                if g != p:
                    total = jnp.where(lane == g, pltpu.roll(chunks[g], (g - p) * width % LANES, 1), total)
            row = m * per_block + p
            packed[row] = total
            holder = group_index * per_block + home_row

            @pl.when(row * n_grp + home == me)
            def _():
                pltpu.make_async_copy(packed.at[row], by_source.at[holder], own.at[3]).start()

            @pl.when(row * n_grp + home != me)
            def _():
                to_source(row, holder).start()

        @pl.when(m == group_index)
        def _():
            pltpu.make_async_copy(result.at[group_index], by_partner.at[group_index], own.at[4]).start()

        @pl.when(m != group_index)
        def _():
            to_partner(m).start()

        high, low = split(values)
        source = ids[m, 0:1, :].astype(jnp.int32) - m * per_block * scan_local
        partner = ids[m, 1:2, :].astype(jnp.int32) - scan_index * scan_local
        span = lax.broadcasted_iota(jnp.int32, (LANES, LANES), 0)
        chosen = jnp.where(span == source, 1.0, 0.0).astype(jnp.bfloat16)
        sums = contract(high, chosen) + contract(low, chosen)
        chosen = jnp.where(span == partner, 1.0, 0.0).astype(jnp.bfloat16)
        tally[...] += contract(high, chosen) + contract(low, chosen)
        for p in range(per_block):
            row = m * per_block + p
            for a, line in enumerate(compact(sums, p, scan_local)):
                share_out[row * SUMS + a] = line
            for g in range(n_grp):
                peer = row * n_grp + g

                @pl.when((peer != me) & (m == g))
                def _():
                    to_share(peer, row, 0).start()

                @pl.when((peer != me) & (m != g))
                def _():
                    to_share(peer, row, SUMS - 1).start()

        return 0

    lax.fori_loop(0, blocks, one_block, 0)
    for a, line in enumerate(compact(tally[...], 0, scan_local)):
        part_out[a] = line
    own_share = pltpu.make_async_copy(
        share_out.at[pl.ds(scan_index * SUMS, SUMS)], shares.at[pl.ds(me * SUMS, SUMS)], own.at[0]
    )
    own_part = pltpu.make_async_copy(part_out, parts.at[pl.ds(group_index * SUMS, SUMS)], own.at[1])
    own_share.start()
    own_part.start()
    for g in range(n_grp):

        @pl.when((g != group_index) & (home == g))
        def _():
            to_part(g, 0).start()

        @pl.when((g != group_index) & (home != g))
        def _():
            to_part(g, SUMS - 1).start()

    others = n_grp - 1
    wait_for(by_partner, others, received.at[3])
    wait_for(result, others, sent.at[3])
    wait_for(meta_in, devices - 1, sent.at[1])

    @pl.when(home == group_index)
    def _():
        pltpu.make_async_copy(packed.at[0], by_source.at[0], own.at[3]).wait()
        wait_for(by_source, sources - 1, received.at[2])
        wait_for(packed, n_scan - 1, sent.at[2])
        wait_for(shares, (devices - 1) * SUMS, received.at[4])
        wait_for(shares, n_scan * (SUMS + others) - SUMS, sent.at[4])
        wait_for(parts, others * SUMS, received.at[5])
        wait_for(parts, others, sent.at[5])

    @pl.when(home != group_index)
    def _():
        wait_for(by_source, sources, received.at[2])
        wait_for(packed, n_scan, sent.at[2])
        wait_for(shares, devices - 1, received.at[4])
        wait_for(shares, n_scan * (SUMS + others) - 1, sent.at[4])
        wait_for(parts, others, received.at[5])
        wait_for(parts, others - 1 + SUMS, sent.at[5])

    pltpu.make_async_copy(result.at[0], by_partner.at[group_index], own.at[4]).wait()
    own_share.wait()
    own_part.wait()

    @pl.when(group_index < full_groups)
    def _():
        wait_for(data, (devices - 1) * short, sent.at[0])

    @pl.when(group_index >= full_groups)
    def _():
        wait_for(data, (devices - 1) * rows, sent.at[0])


def regroup(parts, width):
    groups = len(parts)
    lane = lax.broadcasted_iota(jnp.int32, parts[0].shape, 1) // width
    out = []
    for b in range(groups):
        total = parts[b]
        for g in range(groups):
            if g != b:
                total = jnp.where(lane == g, pltpu.roll(parts[g], (g - b) * width % LANES, 1), total)
        out.append(total)
    return out


def assemble_kernel(n_grp, width, by_source, by_partner, shares, parts, hessian, gradient, spare):
    rows, columns = hessian.shape[2], hessian.shape[3]
    grad_rows = gradient.shape[0]
    per_block = LANES // width
    scan_index, group_index = lax.axis_index("scan"), lax.axis_index("grp")
    home, home_row = scan_index // per_block, lax.rem(scan_index, per_block)
    first_row, first_column = scan_index * rows, group_index * columns
    count = len(PAIRS)

    def total_of(ref):
        total = ref[0:SUMS, 0, :]
        for d in range(1, ref.shape[0] // SUMS):
            total = total + ref[d * SUMS : (d + 1) * SUMS, 0, :]
        return total

    def spread(line):
        return pltpu.roll(jnp.broadcast_to(line, (8, LANES)), rows, 1, stride=rows, stride_axis=0)

    outgoing, incoming = total_of(shares), total_of(parts)
    vector = spread(outgoing[SUMS - 1 :, :] - incoming[SUMS - 1 :, :])
    spare[...] = jnp.concatenate([vector[7 - i : 8 - i, :] for i in range(8)], axis=0).T
    gradient[...] = spare[pl.ds(group_index * grad_rows, grad_rows), 0:6]
    both = [spread(outgoing[a : a + 1, :] + incoming[a : a + 1, :]) for a in range(SUMS - 1)]
    lines = [both[q // 8][7 - q % 8 : 8 - q % 8, :] for q in range(count)]

    pieces = []
    for g in range(n_grp):
        halves_ = [by_source[g * per_block + p] for p in range(per_block)]
        block = jnp.concatenate(regroup(halves_, width), axis=0)
        source, partner = [block[r : r + 1, :].astype(jnp.int32) for r in (IDS, IDS + 1)]
        pieces.append((block, source - first_row, partner - first_column))
    for g in range(n_grp):
        block = by_partner[g]
        source, partner = [block[r : r + 1, :].astype(jnp.int32) for r in (IDS, IDS + 1)]
        pieces.append((block, partner - first_row, source - first_column))
    pieces = [([block[q : q + 1, :] for q in range(count)], at, to) for block, at, to in pieces]
    lane = lax.broadcasted_iota(jnp.int32, (1, LANES), 1)
    diagonal = jnp.where((lane < rows) & (group_index == home), lane, -1)
    pieces.append((lines, diagonal, jnp.where(diagonal < 0, -1, lane + home_row * rows)))

    left, right = [], []
    row = lax.broadcasted_iota(jnp.int32, (rows, LANES), 0)
    column = lax.broadcasted_iota(jnp.int32, (columns, LANES), 0)
    for index, (block, at, to) in enumerate(pieces):
        hit = row == at
        left.append(jnp.concatenate([jnp.where(hit, block[q], 0.0) for q in range(count)], axis=0))
        right.append(jnp.where(column == to, 1.0 if index == 2 * n_grp else -1.0, 0.0))
    matrix = jnp.concatenate(right, axis=1).astype(jnp.bfloat16)
    high, low = split(jnp.concatenate(left, axis=1))
    total = contract(high, matrix) + contract(low, matrix)
    where = {pair: q for q, pair in enumerate(PAIRS)}
    for i in range(6):
        for j in range(6):
            q = where[min(i, j), max(i, j)]
            hessian[i, j] = total[q * rows : (q + 1) * rows, :]


def local(samples, point_count, corr_scan, corr_tile, corr_src):
    f32, i32 = jnp.float32, jnp.int32
    scan_local, tiles_local = samples.shape[0], samples.shape[1]
    request_count = scan_local * corr_scan.shape[1]
    n_scan, n_grp = lax.axis_size("scan"), lax.axis_size("grp")
    devices = n_scan * n_grp
    cap = 2 * request_count // devices
    width = n_grp * cap
    packed_rows = REPLY * width // LANES
    per_block = LANES // width
    blocks = n_scan // per_block
    columns = scan_local * n_scan // n_grp
    grad_rows = scan_local // n_grp
    assert blocks == n_grp and blocks * per_block == n_scan and 8 * scan_local == LANES
    shape = jax.ShapeDtypeStruct
    dma = pltpu.SemaphoreType.DMA

    tiles = samples.transpose(0, 2, 1, 3)
    per_scan = corr_scan.shape[1]
    assert request_count <= FLAT and scan_local * tiles_local * FLAT <= USED
    table = (devices * cap // LANES, LANES)

    by_source, by_partner, shares, parts = pl.pallas_call(
        functools.partial(exchange_kernel, cap, n_grp),
        out_shape=(
            shape((n_grp * per_block, packed_rows, LANES), f32),
            shape((n_grp, VALUES, LANES), f32),
            shape((devices * SUMS, 1, LANES), f32),
            shape((n_grp * SUMS, 1, LANES), f32),
        ),
        in_specs=[ANY] * 5,
        out_specs=(ANY,) * 4,
        scratch_shapes=[
            pltpu.VMEM(tiles.shape, f32),
            pltpu.SMEM(point_count.shape, i32),
            pltpu.VMEM(corr_src.shape, i32),
            pltpu.VMEM(corr_scan.shape, i32),
            pltpu.VMEM(corr_tile.shape, i32),
            pltpu.VMEM((scan_local, LANES), i32),
            pltpu.VMEM(table, i32),
            pltpu.SMEM(table, i32),
            pltpu.VMEM((devices, 1, LANES), i32),
            pltpu.VMEM((devices * cap * 4, LANES), f32),
            pltpu.VMEM((devices * cap * 4, LANES), f32),
            pltpu.VMEM((devices, 1, LANES), i32),
            pltpu.SMEM((devices, 1, LANES), i32),
            pltpu.VMEM((scan_local * tiles_local, 8, LANES), f32),
            pltpu.VMEM((LANES * 8, LANES), f32),
            pltpu.VMEM((10, LANES, LANES), f32),
            pltpu.VMEM((blocks, 8, LANES), f32),
            pltpu.VMEM((blocks, VALUES, LANES), f32),
            pltpu.VMEM((n_scan, packed_rows, LANES), f32),
            pltpu.VMEM((VALUES, LANES), f32),
            pltpu.VMEM((n_scan * SUMS, 1, LANES), f32),
            pltpu.VMEM((SUMS, 1, LANES), f32),
        ]
        + [dma((6,)), dma((6,)), dma((blocks,)), dma((5,))],
        compiler_params=pltpu.CompilerParams(collective_id=0, has_side_effects=True),
    )(tiles, point_count, corr_src, corr_scan, corr_tile)

    hessian, gradient = pl.pallas_call(
        functools.partial(assemble_kernel, n_grp, width),
        out_shape=(shape((6, 6, scan_local, columns), f32), shape((grad_rows, 6), f32)),
        in_specs=[VMEM] * 4,
        out_specs=(VMEM, VMEM),
        scratch_shapes=[pltpu.VMEM((LANES, 8), f32)],
    )(by_source, by_partner, shares, parts)
    return hessian.transpose(2, 0, 1, 3), gradient


def solution(mesh):
    placed = (
        P("scan", "grp", None, None),
        P("scan"),
        P("scan", "grp"),
        P("scan", "grp"),
        P("scan", "grp", None),
    )
    return jax.shard_map(
        local,
        mesh=mesh,
        in_specs=placed,
        out_specs=(P("scan", None, None, "grp"), P(("scan", "grp"), None)),
        check_vma=False,
    )
```

```python
import functools

import jax
import jax.numpy as jnp
from jax import lax
from jax.experimental import pallas as pl
from jax.experimental.pallas import tpu as pltpu
from jax.sharding import PartitionSpec as P

LANES = 128
VALUES = 32
LEAST_POINTS = 4096
SUMS = VALUES // 8
IDS, VECTOR, REPLY = 21, 24, 24
FLAT, USED = 512, 1 << 20
PAIRS = [(i, j) for i in range(6) for j in range(i, 6)]
VMEM = pl.BlockSpec(memory_space=pltpu.VMEM)
SMEM = pl.BlockSpec(memory_space=pltpu.SMEM)
ANY = pl.BlockSpec(memory_space=pl.ANY)


def halves(value, size):
    if size & (size - 1):
        return value // size, value % size
    return value >> (size.bit_length() - 1), value & (size - 1)


def lane_take(table, index):
    return jnp.take_along_axis(table, index, axis=1, mode="promise_in_bounds")


def route(cap, n_grp, tiles_local, first_scan, scans, tiles, wide, slots, meta):
    scan_local, per_scan = scans.shape
    chunks, together = scan_local * per_scan // LANES, LANES // per_scan

    def flat(ref):
        wide[...] = jnp.zeros_like(wide)
        wide[:, 0:per_scan] = ref[...]
        out = []
        for h in range(chunks):
            moved = pltpu.roll(wide[h * together : (h + 1) * together, :], 0, 1, stride=per_scan, stride_axis=0)
            out.append(row_sum(moved))
        return out

    def column(row):
        return jnp.broadcast_to(row, (LANES, LANES)).T

    sublane = lax.broadcasted_iota(jnp.int32, (LANES, LANES), 0)
    lane = lax.broadcasted_iota(jnp.int32, (LANES, LANES), 1)
    index = lax.broadcasted_iota(jnp.int32, (1, LANES), 1)
    targets, codes = [], []
    for h, (b, t) in enumerate(zip(flat(scans), flat(tiles))):
        (b_dev, b_loc), (t_dev, t_loc) = halves(b, scan_local), halves(t, tiles_local)
        targets.append(b_dev * n_grp + t_dev)
        codes.append(column(USED + (b_loc * tiles_local + t_loc) * FLAT + index + h * LANES))
    target_columns = [column(x) for x in targets]
    places = []
    for h in range(chunks):
        rank = jnp.zeros((1, LANES), jnp.int32)
        for e in range(h + 1):
            same = target_columns[e] == targets[h]
            if e == h:
                same = same & (sublane < lane)
            rank = rank + row_sum(jnp.where(same, 1, 0))
        places.append(column(targets[h] * cap + rank))
    served = LANES // cap
    part = lax.broadcasted_iota(jnp.int32, (served, LANES), 1) // cap
    for a in range(slots.shape[0]):
        table = jnp.zeros((1, LANES), jnp.int32)
        for h in range(chunks):
            table = table + row_sum(jnp.where(places[h] == lane + a * LANES, codes[h], 0))
        used, request, tile = table >= USED, table & (FLAT - 1), (table & (USED - 1)) >> (FLAT.bit_length() - 1)
        slots[a : a + 1, :] = request
        source = first_scan + halves(request, per_scan)[0]
        kinds = [jnp.where(used, halves(tile, tiles_local)[0], -1), tile, jnp.where(used, source, -1)]
        total = jnp.zeros((served, LANES), jnp.int32)
        for kind, row in enumerate(kinds):
            moved = pltpu.roll(jnp.broadcast_to(row, (served, LANES)), cap, 1, stride=cap, stride_axis=0)
            if kind:
                moved = pltpu.roll(moved, kind * cap, 1)
            total = jnp.where(part == kind, moved, total)
        for i in range(served):
            meta[a * served + i] = total[served - 1 - i : served - i, :]


def greet_all(n_grp, devices, me):
    barrier = pltpu.get_barrier_semaphore()

    def hello(k, _):
        peer = lax.rem(me + k, devices)
        pl.semaphore_signal(
            barrier, inc=1, device_id=(peer // n_grp, peer % n_grp), device_id_type=pl.DeviceIdType.MESH
        )
        return 0

    lax.fori_loop(1, devices, hello, 0)


def await_all(devices):
    pl.semaphore_wait(pltpu.get_barrier_semaphore(), devices - 1)


def remote(src, dst, send, recv, peer, n_grp):
    return pltpu.make_async_remote_copy(
        src_ref=src, dst_ref=dst, send_sem=send, recv_sem=recv,
        device_id=(peer // n_grp, peer % n_grp), device_id_type=pl.DeviceIdType.MESH,
    )


def exclusive(a, b, size):
    if size & (size - 1):
        return lax.rem(a + b, size)
    total = 0
    for bit in range(size.bit_length() - 1):
        total = total + ((((a >> bit) + (b >> bit)) & 1) << bit)
    return total


def split(values):
    high = values.astype(jnp.bfloat16)
    return high, (values - high.astype(jnp.float32)).astype(jnp.bfloat16)


def contract(a, b):
    return lax.dot_general(a, b, (((1,), (1,)), ((), ())), preferred_element_type=jnp.float32)


def row_sum(products):
    return jnp.sum(products, axis=0, keepdims=True)


def within(index, size):
    return jnp.maximum(jnp.minimum(index, size - 1), 0)


def wait_for(ref, count, semaphore):
    part = ref.at[pl.ds(0, count)]
    pltpu.make_async_copy(part, part, semaphore).wait()


def compact(sums, place, rows):
    lane = lax.broadcasted_iota(jnp.int32, (8, LANES), 1)
    out = []
    for a in range(SUMS):
        part = sums[a * 8 : (a + 1) * 8, :]
        if place:
            part = pltpu.roll(part, LANES - place * rows, 1)
        part = jnp.where(lane < rows, part, 0.0)
        out.append(row_sum(pltpu.roll(part, 0, 1, stride=rows, stride_axis=0)))
    return out


def exchange_kernel(
    cap, n_grp, samples_hbm, count_hbm, wanted_hbm, scans_hbm, tiles_hbm, by_source, by_partner, shares, parts,
    samples, count, wanted, scans, partner_tiles, wide, routed, slots, meta, data, data_in, meta_in, codes, tiles, comps, turned, ids, result, packed,
    tally, share_out, part_out,
    sent, received, recv_data, own,
):
    scan_local, tiles_local = samples.shape[0], samples.shape[2]
    per_scan = wanted.shape[1]
    n_scan = packed.shape[0]
    devices = n_scan * n_grp
    rows = cap * 4
    width = n_grp * cap
    per_block = LANES // width
    blocks = n_scan // per_block
    sources = per_block * n_grp
    packed_rows = packed.shape[1]
    scan_index, group_index = lax.axis_index("scan"), lax.axis_index("grp")
    me = scan_index * n_grp + group_index
    home, home_row = scan_index // per_block, lax.rem(scan_index, per_block)
    full_groups = min(LEAST_POINTS // (tiles_local * LANES), n_grp) if 3 * cap % 8 == 0 else 0
    short = rows - cap

    def send_one(peer, size):
        return remote(
            data.at[pl.ds(pl.multiple_of(peer * rows, 8), size)],
            data_in.at[pl.ds(pl.multiple_of(me * rows, 8), size)],
            sent.at[0], recv_data.at[home], peer, n_grp,
        )

    def send_code(peer):
        return remote(meta.at[peer], meta_in.at[me], sent.at[1], received.at[1], peer, n_grp)

    def to_source(row, holder):
        peer = row * n_grp + home
        return remote(packed.at[row], by_source.at[holder], sent.at[2], received.at[2], peer, n_grp)

    def to_partner(block):
        peer = scan_index * n_grp + block
        return remote(result.at[block], by_partner.at[group_index], sent.at[3], received.at[3], peer, n_grp)

    def to_share(peer, row, first):
        size = SUMS - first
        return remote(
            share_out.at[pl.ds(row * SUMS + first, size)], shares.at[pl.ds(me * SUMS + first, size)],
            sent.at[4], received.at[4], peer, n_grp,
        )

    def to_part(g, first):
        size = SUMS - first
        return remote(
            part_out.at[pl.ds(first, size)], parts.at[pl.ds(group_index * SUMS + first, size)],
            sent.at[5], received.at[5], scan_index * n_grp + g, n_grp,
        )

    fetch = pltpu.make_async_copy(samples_hbm, samples, own.at[3])
    fetch_count = pltpu.make_async_copy(count_hbm, count, own.at[4])
    fetch_wanted = pltpu.make_async_copy(wanted_hbm, wanted, own.at[0])
    fetch_scans = pltpu.make_async_copy(scans_hbm, scans, own.at[1])
    fetch_tiles = pltpu.make_async_copy(tiles_hbm, partner_tiles, own.at[2])
    fetch_scans.start()
    fetch_tiles.start()
    fetch_count.start()
    fetch_wanted.start()
    fetch.start()
    greet_all(n_grp, devices, me)
    fetch_scans.wait()
    fetch_tiles.wait()
    route(cap, n_grp, tiles_local, scan_index * scan_local, scans, partner_tiles, wide, routed, meta)
    fetch_slots = pltpu.make_async_copy(routed, slots, own.at[1])
    fetch_slots.start()
    fetch_count.wait()
    fetch_wanted.wait()
    fetch.wait()
    fetch_slots.wait()
    first_point = group_index * tiles_local * LANES
    wanted_rows = wanted.reshape(scan_local * per_scan, LANES)
    tile_row = lax.broadcasted_iota(jnp.int32, (tiles_local, LANES), 0)

    def collect(peer, into):
        first = lax.rem(peer, LANES // cap) * cap
        for j in range(cap):
            request = within(slots[peer // (LANES // cap), first + j], scan_local * per_scan)
            s = halves(request, per_scan)[0]
            point = wanted_rows[pl.ds(request, 1), :]
            spread = jnp.broadcast_to(point, (tiles_local, LANES))
            hit, place = spread >> 7 == tile_row, spread & (LANES - 1)
            for c in range(3):
                found = jnp.where(hit, lane_take(samples[s, c], place), 0.0)
                into[pl.ds(peer * rows + c * cap + j, 1), :] = row_sum(found)
            mask = jnp.where(first_point + point < count[s], 1.0, 0.0).astype(jnp.float32)
            into[pl.ds(peer * rows + 3 * cap + j, 1), :] = mask

    await_all(devices)

    def start_meta(k, _):
        peer = lax.rem(me + k, devices)
        send_code(peer).start()
        return 0

    def start_data(k, _):
        peer = exclusive(me, k, devices)
        collect(peer, data)

        @pl.when((peer != me) & (group_index < full_groups))
        def _():
            send_one(peer, short).start()

        @pl.when((peer != me) & (group_index >= full_groups))
        def _():
            send_one(peer, rows).start()

        return 0

    lax.fori_loop(1, devices, start_meta, 0)
    share = devices // 4
    for quarter in (2, 1, 0, 3):
        lax.fori_loop(quarter * share, (quarter + 1) * share, start_data, 0)
    own_meta = pltpu.make_async_copy(meta.at[me], meta_in.at[me], own.at[1])
    own_meta.start()
    collect(me, data_in)
    own_meta.wait()

    def no_mask(row, _):
        for g in range(full_groups):
            first = pl.multiple_of((row * n_grp + g) * rows + short, 8)
            data_in[pl.ds(first, cap), :] = jnp.ones((cap, LANES), jnp.float32)
        return 0

    lax.fori_loop(0, n_scan, no_mask, 0)
    tally[...] = jnp.zeros_like(tally)
    result[...] = jnp.zeros_like(result)

    point = lax.broadcasted_iota(jnp.int32, (tiles_local, LANES), 0) * LANES
    point = point + lax.broadcasted_iota(jnp.int32, (tiles_local, LANES), 1)

    tile_rows = tiles.reshape(scan_local * tiles_local * 8, LANES)

    def fill(b, _):
        valid = point < count[b] - group_index * tiles_local * LANES
        for c in range(6):
            values = samples[b, c]
            if c >= 3:
                values = jnp.where(valid, values, 0.0)
            tile_rows[pl.ds(b * tiles_local * 8 + c, tiles_local, stride=8), :] = values
        return 0

    lax.fori_loop(0, scan_local, fill, 0)
    wait_for(meta_in, devices - 1, received.at[1])
    to_scalar = pltpu.make_async_copy(meta_in, codes, own.at[2])
    to_scalar.start()

    slot_lane = lax.broadcasted_iota(jnp.int32, (sources, LANES), 1) // cap
    slot_row = lax.broadcasted_iota(jnp.int32, (sources, LANES), 0)

    def decode(m, _):
        arrived = meta_in[pl.ds(m * sources, sources), 0, :]
        kinds = []
        for kind in (0, 2):
            moved = pltpu.roll(arrived, LANES - kind * cap, 1) if kind else arrived
            moved = pltpu.roll(moved, 0, 1, stride=cap, stride_axis=0)
            kinds.append(row_sum(jnp.where(slot_lane == slot_row, moved, 0)))
        partner, source = kinds
        ids[m, 0:1, :] = source.astype(jnp.float32)
        ids[m, 1:2, :] = jnp.where(partner < 0, -1, scan_index * scan_local + partner).astype(jnp.float32)
        return 0

    lax.fori_loop(0, blocks, decode, 0)
    to_scalar.wait()

    def one_block(k, _):
        m = exclusive(home, k, blocks)

        def gather(i, _):
            for j in range(cap):
                slot = i * cap + j
                row = within(codes[m * sources + i, 0, cap + j], scan_local * tiles_local)
                comps[pl.ds(pl.multiple_of(slot * 8, 8), 8), :] = tiles[row]
            return 0

        lax.fori_loop(0, sources, gather, 0)
        for c in range(6):
            turned[4 + c] = comps[pl.ds(c, LANES, stride=8), :].T

        whole = per_block * (n_grp * rows - full_groups * cap)

        @pl.when(m != home)
        def _():
            wait_for(data_in, whole, recv_data.at[m])

        @pl.when((m == home) & (group_index < full_groups))
        def _():
            wait_for(data_in, whole - short, recv_data.at[m])

        @pl.when((m == home) & (group_index >= full_groups))
        def _():
            wait_for(data_in, whole - rows, recv_data.at[m])

        for c in range(4):
            pieces = [
                data_in[pl.ds((m * sources + i) * rows + c * cap, cap), :] for i in range(sources)
            ]
            turned[c] = jnp.concatenate(pieces, axis=0).T

        def step(kk, sums):
            at = pl.ds(pl.multiple_of(kk * 8, 8), 8)
            px, py, pz, mask, qx, qy, qz, nx, ny, nz = [turned[c, at, :] for c in range(10)]
            residual = nx * (px - qx) + ny * (py - qy) + nz * (pz - qz)
            weight = mask / (1.0 + residual * residual)
            jac = [py * nz - pz * ny, pz * nx - px * nz, px * ny - py * nx, nx, ny, nz]
            scaled = [weight * x for x in jac]
            products = [scaled[a] * jac[b] for a, b in PAIRS] + [x * residual for x in scaled]
            return tuple(s + p for s, p in zip(sums, products))

        zero = jnp.zeros((8, LANES), jnp.float32)
        sums = lax.fori_loop(0, LANES // 8, step, (zero,) * (len(PAIRS) + 6), unroll=True)
        for q, total in enumerate(sums):
            q = q if q < len(PAIRS) else q - len(PAIRS) + VECTOR
            result[m, q : q + 1, :] = row_sum(total)
        result[m, IDS : IDS + 2, :] = ids[m, 0:2, :]
        values = result[m]
        lane = lax.broadcasted_iota(jnp.int32, (packed_rows, LANES), 1) // width
        chunks = [values[g * packed_rows : (g + 1) * packed_rows, :] for g in range(per_block)]
        for p in range(per_block):
            total = chunks[p]
            for g in range(per_block):
                if g != p:
                    total = jnp.where(lane == g, pltpu.roll(chunks[g], (g - p) * width % LANES, 1), total)
            row = m * per_block + p
            packed[row] = total
            holder = group_index * per_block + home_row

            @pl.when(row * n_grp + home == me)
            def _():
                pltpu.make_async_copy(packed.at[row], by_source.at[holder], own.at[3]).start()

            @pl.when(row * n_grp + home != me)
            def _():
                to_source(row, holder).start()

        @pl.when(m == group_index)
        def _():
            pltpu.make_async_copy(result.at[group_index], by_partner.at[group_index], own.at[4]).start()

        @pl.when(m != group_index)
        def _():
            to_partner(m).start()

        high, low = split(values)
        source = ids[m, 0:1, :].astype(jnp.int32) - m * per_block * scan_local
        partner = ids[m, 1:2, :].astype(jnp.int32) - scan_index * scan_local
        span = lax.broadcasted_iota(jnp.int32, (LANES, LANES), 0)
        chosen = jnp.where(span == source, 1.0, 0.0).astype(jnp.bfloat16)
        sums = contract(high, chosen) + contract(low, chosen)
        chosen = jnp.where(span == partner, 1.0, 0.0).astype(jnp.bfloat16)
        tally[...] += contract(high, chosen) + contract(low, chosen)
        for p in range(per_block):
            row = m * per_block + p
            for a, line in enumerate(compact(sums, p, scan_local)):
                share_out[row * SUMS + a] = line
            for g in range(n_grp):
                peer = row * n_grp + g

                @pl.when((peer != me) & (m == g))
                def _():
                    to_share(peer, row, 0).start()

                @pl.when((peer != me) & (m != g))
                def _():
                    to_share(peer, row, SUMS - 1).start()

        return 0

    lax.fori_loop(0, blocks, one_block, 0)
    for a, line in enumerate(compact(tally[...], 0, scan_local)):
        part_out[a] = line
    own_share = pltpu.make_async_copy(
        share_out.at[pl.ds(scan_index * SUMS, SUMS)], shares.at[pl.ds(me * SUMS, SUMS)], own.at[0]
    )
    own_part = pltpu.make_async_copy(part_out, parts.at[pl.ds(group_index * SUMS, SUMS)], own.at[1])
    own_share.start()
    own_part.start()
    for g in range(n_grp):

        @pl.when((g != group_index) & (home == g))
        def _():
            to_part(g, 0).start()

        @pl.when((g != group_index) & (home != g))
        def _():
            to_part(g, SUMS - 1).start()

    others = n_grp - 1
    wait_for(by_partner, others, received.at[3])
    wait_for(result, others, sent.at[3])
    wait_for(meta_in, devices - 1, sent.at[1])

    @pl.when(home == group_index)
    def _():
        pltpu.make_async_copy(packed.at[0], by_source.at[0], own.at[3]).wait()
        wait_for(by_source, sources - 1, received.at[2])
        wait_for(packed, n_scan - 1, sent.at[2])
        wait_for(shares, (devices - 1) * SUMS, received.at[4])
        wait_for(shares, n_scan * (SUMS + others) - SUMS, sent.at[4])
        wait_for(parts, others * SUMS, received.at[5])
        wait_for(parts, others, sent.at[5])

    @pl.when(home != group_index)
    def _():
        wait_for(by_source, sources, received.at[2])
        wait_for(packed, n_scan, sent.at[2])
        wait_for(shares, devices - 1, received.at[4])
        wait_for(shares, n_scan * (SUMS + others) - 1, sent.at[4])
        wait_for(parts, others, received.at[5])
        wait_for(parts, others - 1 + SUMS, sent.at[5])

    pltpu.make_async_copy(result.at[0], by_partner.at[group_index], own.at[4]).wait()
    own_share.wait()
    own_part.wait()

    @pl.when(group_index < full_groups)
    def _():
        wait_for(data, (devices - 1) * short, sent.at[0])

    @pl.when(group_index >= full_groups)
    def _():
        wait_for(data, (devices - 1) * rows, sent.at[0])


def regroup(parts, width):
    groups = len(parts)
    lane = lax.broadcasted_iota(jnp.int32, parts[0].shape, 1) // width
    out = []
    for b in range(groups):
        total = parts[b]
        for g in range(groups):
            if g != b:
                total = jnp.where(lane == g, pltpu.roll(parts[g], (g - b) * width % LANES, 1), total)
        out.append(total)
    return out


def assemble_kernel(n_grp, width, by_source, by_partner, shares, parts, hessian, gradient, spare):
    rows, columns = hessian.shape[2], hessian.shape[3]
    grad_rows = gradient.shape[0]
    per_block = LANES // width
    scan_index, group_index = lax.axis_index("scan"), lax.axis_index("grp")
    home, home_row = scan_index // per_block, lax.rem(scan_index, per_block)
    first_row, first_column = scan_index * rows, group_index * columns
    count = len(PAIRS)

    def total_of(ref):
        total = ref[0:SUMS, 0, :]
        for d in range(1, ref.shape[0] // SUMS):
            total = total + ref[d * SUMS : (d + 1) * SUMS, 0, :]
        return total

    def spread(line):
        return pltpu.roll(jnp.broadcast_to(line, (8, LANES)), rows, 1, stride=rows, stride_axis=0)

    outgoing, incoming = total_of(shares), total_of(parts)
    vector = spread(outgoing[SUMS - 1 :, :] - incoming[SUMS - 1 :, :])
    spare[...] = jnp.concatenate([vector[7 - i : 8 - i, :] for i in range(8)], axis=0).T
    gradient[...] = spare[pl.ds(group_index * grad_rows, grad_rows), 0:6]
    both = [spread(outgoing[a : a + 1, :] + incoming[a : a + 1, :]) for a in range(SUMS - 1)]
    lines = [both[q // 8][7 - q % 8 : 8 - q % 8, :] for q in range(count)]

    pieces = []
    for g in range(n_grp):
        halves_ = [by_source[g * per_block + p] for p in range(per_block)]
        block = jnp.concatenate(regroup(halves_, width), axis=0)
        source, partner = [block[r : r + 1, :].astype(jnp.int32) for r in (IDS, IDS + 1)]
        pieces.append((block, source - first_row, partner - first_column))
    for g in range(n_grp):
        block = by_partner[g]
        source, partner = [block[r : r + 1, :].astype(jnp.int32) for r in (IDS, IDS + 1)]
        pieces.append((block, partner - first_row, source - first_column))
    pieces = [([block[q : q + 1, :] for q in range(count)], at, to) for block, at, to in pieces]
    lane = lax.broadcasted_iota(jnp.int32, (1, LANES), 1)
    diagonal = jnp.where((lane < rows) & (group_index == home), lane, -1)
    pieces.append((lines, diagonal, jnp.where(diagonal < 0, -1, lane + home_row * rows)))

    left, right = [], []
    row = lax.broadcasted_iota(jnp.int32, (rows, LANES), 0)
    column = lax.broadcasted_iota(jnp.int32, (columns, LANES), 0)
    for index, (block, at, to) in enumerate(pieces):
        hit = row == at
        left.append(jnp.concatenate([jnp.where(hit, block[q], 0.0) for q in range(count)], axis=0))
        right.append(jnp.where(column == to, 1.0 if index == 2 * n_grp else -1.0, 0.0))
    matrix = jnp.concatenate(right, axis=1).astype(jnp.bfloat16)
    high, low = split(jnp.concatenate(left, axis=1))
    total = contract(high, matrix) + contract(low, matrix)
    where = {pair: q for q, pair in enumerate(PAIRS)}
    for i in range(6):
        for j in range(6):
            q = where[min(i, j), max(i, j)]
            hessian[i, j] = total[q * rows : (q + 1) * rows, :]


def local(samples, point_count, corr_scan, corr_tile, corr_src):
    f32, i32 = jnp.float32, jnp.int32
    scan_local, tiles_local = samples.shape[0], samples.shape[1]
    request_count = scan_local * corr_scan.shape[1]
    n_scan, n_grp = lax.axis_size("scan"), lax.axis_size("grp")
    devices = n_scan * n_grp
    cap = 2 * request_count // devices
    width = n_grp * cap
    packed_rows = REPLY * width // LANES
    per_block = LANES // width
    blocks = n_scan // per_block
    columns = scan_local * n_scan // n_grp
    grad_rows = scan_local // n_grp
    assert blocks == n_grp and blocks * per_block == n_scan and 8 * scan_local == LANES
    shape = jax.ShapeDtypeStruct
    dma = pltpu.SemaphoreType.DMA

    tiles = samples.transpose(0, 2, 1, 3)
    per_scan = corr_scan.shape[1]
    assert request_count <= FLAT and scan_local * tiles_local * FLAT <= USED
    table = (devices * cap // LANES, LANES)

    by_source, by_partner, shares, parts = pl.pallas_call(
        functools.partial(exchange_kernel, cap, n_grp),
        out_shape=(
            shape((n_grp * per_block, packed_rows, LANES), f32),
            shape((n_grp, VALUES, LANES), f32),
            shape((devices * SUMS, 1, LANES), f32),
            shape((n_grp * SUMS, 1, LANES), f32),
        ),
        in_specs=[ANY] * 5,
        out_specs=(ANY,) * 4,
        scratch_shapes=[
            pltpu.VMEM(tiles.shape, f32),
            pltpu.SMEM(point_count.shape, i32),
            pltpu.VMEM(corr_src.shape, i32),
            pltpu.VMEM(corr_scan.shape, i32),
            pltpu.VMEM(corr_tile.shape, i32),
            pltpu.VMEM((scan_local, LANES), i32),
            pltpu.VMEM(table, i32),
            pltpu.SMEM(table, i32),
            pltpu.VMEM((devices, 1, LANES), i32),
            pltpu.VMEM((devices * cap * 4, LANES), f32),
            pltpu.VMEM((devices * cap * 4, LANES), f32),
            pltpu.VMEM((devices, 1, LANES), i32),
            pltpu.SMEM((devices, 1, LANES), i32),
            pltpu.VMEM((scan_local * tiles_local, 8, LANES), f32),
            pltpu.VMEM((LANES * 8, LANES), f32),
            pltpu.VMEM((10, LANES, LANES), f32),
            pltpu.VMEM((blocks, 8, LANES), f32),
            pltpu.VMEM((blocks, VALUES, LANES), f32),
            pltpu.VMEM((n_scan, packed_rows, LANES), f32),
            pltpu.VMEM((VALUES, LANES), f32),
            pltpu.VMEM((n_scan * SUMS, 1, LANES), f32),
            pltpu.VMEM((SUMS, 1, LANES), f32),
        ]
        + [dma((6,)), dma((6,)), dma((blocks,)), dma((5,))],
        compiler_params=pltpu.CompilerParams(collective_id=0, has_side_effects=True),
    )(tiles, point_count, corr_src, corr_scan, corr_tile)

    hessian, gradient = pl.pallas_call(
        functools.partial(assemble_kernel, n_grp, width),
        out_shape=(shape((6, 6, scan_local, columns), f32), shape((grad_rows, 6), f32)),
        in_specs=[VMEM] * 4,
        out_specs=(VMEM, VMEM),
        scratch_shapes=[pltpu.VMEM((LANES, 8), f32)],
    )(by_source, by_partner, shares, parts)
    return hessian.transpose(2, 0, 1, 3), gradient


def solution(mesh):
    placed = (
        P("scan", "grp", None, None),
        P("scan"),
        P("scan", "grp"),
        P("scan", "grp"),
        P("scan", "grp", None),
    )
    return jax.shard_map(
        local,
        mesh=mesh,
        in_specs=placed,
        out_specs=(P("scan", None, None, "grp"), P(("scan", "grp"), None)),
        check_vma=False,
    )
```
